8 devices in a mesh: dp: 4 (over z, y, x), sp: 2 (over core).
Axes of the slice: x: 2, y: 2, z: 1, core: 2. Of those that a mesh axis runs over, the one named last changes fastest.
Arguments:
- act_in: bfloat16 [4, 1024, 2048], P('dp', 'sp')
- positions: int32 [4, 1024], P('dp', 'sp')
- out_grad: bfloat16 [4, 1024, 2048], P('dp', 'sp')
- norm1_gain: bfloat16 [2048], P(('dp', 'sp'))
- norm2_gain: bfloat16 [2048], P(('dp', 'sp'))
- w_query: bfloat16 [2048, 32, 64], P(('dp', 'sp'))
- w_key: bfloat16 [2048, 8, 64], P(('dp', 'sp'))
- w_value: bfloat16 [2048, 8, 64], P(('dp', 'sp'))
- w_out: bfloat16 [2048, 2048], P(('dp', 'sp'))
- w_gate: bfloat16 [2048, 8192], P(('dp', 'sp'))
- w_up: bfloat16 [2048, 8192], P(('dp', 'sp'))
- w_down: bfloat16 [8192, 2048], P(('dp', 'sp'))
Outputs:
- output 1: bfloat16 [4, 1024, 2048], P('dp', 'sp')
- output 2: bfloat16 [4, 1024, 2048], P('dp', 'sp')
- output 3: float32 [2048], P(('dp', 'sp'))
- output 4: float32 [2048], P(('dp', 'sp'))
- output 5: float32 [2048, 32, 64], P(('dp', 'sp'))
- output 6: float32 [2048, 8, 64], P(('dp', 'sp'))
- output 7: float32 [2048, 8, 64], P(('dp', 'sp'))
- output 8: float32 [2048, 2048], P(('dp', 'sp'))
- output 9: float32 [2048, 8192], P(('dp', 'sp'))
- output 10: float32 [2048, 8192], P(('dp', 'sp'))
- output 11: float32 [8192, 2048], P(('dp', 'sp'))
All inputs are finite; a program needn't handle non-finite values.
Results may differ from the reference program's by a relative error of at most 0.016116.
Values are sent between devices in bfloat16 or wider.
A program may use at most 1 GiB of HBM per device.

```python
import math
import jax
import jax.numpy as jnp
from jax import lax

MODEL_DIM = 2048
Q_HEADS = 32
KV_HEADS = 8
HEAD_DIM = 64
FFN_DIM = 8192
TOKENS_DEV = 512
DP_SIZE = 4
SP_SIZE = 2

SEQ_LEN = TOKENS_DEV * SP_SIZE
HALF_DIM = HEAD_DIM // 2
N_GROUP = Q_HEADS // KV_HEADS
Q_BLOCK = math.gcd(SEQ_LEN, 256)
N_BLOCKS = SEQ_LEN // Q_BLOCK
ATTN_SCALE = HEAD_DIM ** -0.5
EPS = 1e-5
ROPE_BASE = 10000.0
QK_GAIN = 1.5
NEG_BIG = -1e30


def draw_weight(draw_key, shape, fan_in, gain_factor):
    return (jax.random.normal(draw_key, shape, jnp.float32) * (gain_factor * fan_in ** -0.5)).astype(jnp.bfloat16)


def setup_inputs(seed: int = 0) -> dict:
    key_list = jax.random.split(jax.random.key(seed), 12)
    row_shape = (DP_SIZE, SEQ_LEN, MODEL_DIM)
    q_width = Q_HEADS * HEAD_DIM
    pos_steps = jax.random.randint(key_list[1], (DP_SIZE, SEQ_LEN), 1, 3)
    return dict(
        act_in=jax.random.normal(key_list[0], row_shape, jnp.float32).astype(jnp.bfloat16),
        positions=(jnp.cumsum(pos_steps, axis=1) - 1).astype(jnp.int32),
        out_grad=jax.random.normal(key_list[2], row_shape, jnp.float32).astype(jnp.bfloat16),
        norm1_gain=jax.random.uniform(key_list[3], (MODEL_DIM,), jnp.float32, 0.5, 1.5).astype(jnp.bfloat16),
        norm2_gain=jax.random.uniform(key_list[4], (MODEL_DIM,), jnp.float32, 0.5, 1.5).astype(jnp.bfloat16),
        w_query=draw_weight(key_list[5], (MODEL_DIM, Q_HEADS, HEAD_DIM), MODEL_DIM, QK_GAIN),
        w_key=draw_weight(key_list[6], (MODEL_DIM, KV_HEADS, HEAD_DIM), MODEL_DIM, QK_GAIN),
        w_value=draw_weight(key_list[7], (MODEL_DIM, KV_HEADS, HEAD_DIM), MODEL_DIM, 1.0),
        w_out=draw_weight(key_list[8], (q_width, MODEL_DIM), q_width, 1.0),
        w_gate=draw_weight(key_list[9], (MODEL_DIM, FFN_DIM), MODEL_DIM, 1.0),
        w_up=draw_weight(key_list[10], (MODEL_DIM, FFN_DIM), MODEL_DIM, 1.0),
        w_down=draw_weight(key_list[11], (FFN_DIM, MODEL_DIM), FFN_DIM, 1.0),
    )


def rms_scale(rows_f32):
    return lax.rsqrt(jnp.mean(rows_f32 * rows_f32, axis=-1, keepdims=True) + EPS)


def to_bf(values):
    return values.astype(jnp.bfloat16).astype(jnp.float32)


def rope_apply(values, positions):
    inv_freq = ROPE_BASE ** (-(jnp.arange(HALF_DIM, dtype=jnp.float32) * (2.0 / HEAD_DIM)))
    angles = positions.astype(jnp.float32)[:, None] * inv_freq[None, :]
    cos_t = jnp.cos(angles)[:, None, :]
    sin_t = jnp.sin(angles)[:, None, :]
    first_half = values[..., :HALF_DIM]
    second_half = values[..., HALF_DIM:]
    return jnp.concatenate([first_half * cos_t - second_half * sin_t, second_half * cos_t + first_half * sin_t], axis=-1)


def layer_forward(weights, act_rows, positions):
    gain_a, gain_b, w_query, w_key, w_value, w_out, w_gate, w_up, w_down = weights
    act_f = act_rows.astype(jnp.float32)
    normed_a = to_bf(act_f * rms_scale(act_f) * gain_a)
    q_rot = to_bf(rope_apply(jnp.einsum("sd,dhe->she", normed_a, w_query), positions))
    k_rot = to_bf(rope_apply(jnp.einsum("sd,dhe->she", normed_a, w_key), positions))
    v_proj = to_bf(jnp.einsum("sd,dhe->she", normed_a, w_value))
    q_groups = q_rot.reshape(N_BLOCKS, Q_BLOCK, KV_HEADS, N_GROUP, HEAD_DIM)
    block_starts = jnp.arange(N_BLOCKS) * Q_BLOCK
    key_index = jnp.arange(SEQ_LEN)

    def one_block(block_item):
        q_blk, q_start = block_item
        scores = jnp.einsum("qkgd,skd->kgqs", q_blk, k_rot) * ATTN_SCALE
        allowed = (q_start + jnp.arange(Q_BLOCK))[:, None] >= key_index[None, :]
        scores = jnp.where(allowed, scores, NEG_BIG)
        prob_rows = to_bf(jax.nn.softmax(scores, axis=-1))
        return to_bf(jnp.einsum("kgqs,skd->qkgd", prob_rows, v_proj))

    attn_rows = lax.map(jax.checkpoint(one_block), (q_groups, block_starts)).reshape(SEQ_LEN, Q_HEADS * HEAD_DIM)
    hidden = to_bf(act_f + jnp.dot(attn_rows, w_out))
    normed_b = to_bf(hidden * rms_scale(hidden) * gain_b)
    mixed_act = to_bf(jax.nn.silu(jnp.dot(normed_b, w_gate)) * jnp.dot(normed_b, w_up))
    return (hidden + jnp.dot(mixed_act, w_down)).astype(jnp.bfloat16)


def reference(act_in, positions, out_grad, norm1_gain, norm2_gain, w_query, w_key, w_value, w_out, w_gate, w_up, w_down):
    weights = tuple(param.astype(jnp.float32) for param in (norm1_gain, norm2_gain, w_query, w_key, w_value, w_out, w_gate, w_up, w_down))
    zero_grads = tuple(jnp.zeros_like(param) for param in weights)

    def per_sequence(grad_sums, seq_item):
        act_row, pos_row, grad_row = seq_item

        def fwd_fn(params, act_rows):
            return layer_forward(params, act_rows, pos_row)

        act_out, pullback = jax.vjp(fwd_fn, weights, act_row)
        param_grads, act_grad = pullback(grad_row)
        new_sums = tuple(run_sum + seq_grad for run_sum, seq_grad in zip(grad_sums, param_grads))
        return new_sums, (act_out, act_grad)

    grad_sums, outs = lax.scan(per_sequence, zero_grads, (act_in, positions, out_grad))
    return (outs[0], outs[1], grad_sums[0], grad_sums[1], grad_sums[2], grad_sums[3], grad_sums[4], grad_sums[5], grad_sums[6], grad_sums[7], grad_sums[8])
```

```python
import math
import jax
import jax.numpy as jnp
from jax import lax
from jax.experimental import pallas as pl
from jax.experimental.pallas import tpu as pltpu
from jax.sharding import PartitionSpec as P


EPS = 1e-5
ROPE_BASE = 10000.0
NEG_BIG = -1e30
F32 = jnp.float32
BF16 = jnp.bfloat16


def dot(a, b):
    return lax.dot_general(a, b, (((1,), (0,)), ((), ())), preferred_element_type=F32)


def dot_nt(a, b):
    return lax.dot_general(a, b, (((1,), (1,)), ((), ())), preferred_element_type=F32)


def dot_tn(a, b):
    return lax.dot_general(a, b, (((0,), (0,)), ((), ())), preferred_element_type=F32)


def after(value, *deps):
    return lax.optimization_barrier((value,) + deps)[0]


def pick_blocks(table, values, width):
    rows, cols = values.shape
    n_out = table.shape[0]

    def body(table_ref, in_ref, out_ref):
        out_ref[...] = in_ref[...]

    return pl.pallas_call(
        body,
        out_shape=jax.ShapeDtypeStruct((rows, n_out * width), values.dtype),
        grid_spec=pltpu.PrefetchScalarGridSpec(
            num_scalar_prefetch=1,
            grid=(n_out,),
            in_specs=[pl.BlockSpec((rows, width), lambda j, t: (0, t[j]))],
            out_specs=pl.BlockSpec((rows, width), lambda j, t: (0, j)),
        ),
        cost_estimate=pl.CostEstimate(flops=rows * n_out * width, bytes_accessed=2 * rows * n_out * width * values.dtype.itemsize, transcendentals=0),
        name="pick_blocks",
    )(table, values)


def attn_forward(q_rot, k_rot, v_proj, q_block):
    n_batch, q_len, n_heads, head_dim = q_rot.shape
    k_len, n_kv = k_rot.shape[1], k_rot.shape[2]
    n_group = n_heads // n_kv
    attn_scale = head_dim ** -0.5
    key_index = jnp.arange(k_len)

    def block_step(block_idx, loop_state):
        out_buf, norm_buf = loop_state
        q_start = block_idx * q_block
        q_blk = lax.dynamic_slice_in_dim(q_rot, q_start, q_block, axis=1).reshape(n_batch, q_block, n_kv, n_group, head_dim)
        scores = jnp.einsum("bqkgd,bskd->bkgqs", q_blk, k_rot, preferred_element_type=F32) * attn_scale
        allowed = (q_start + jnp.arange(q_block))[:, None] >= key_index[None, :]
        scores = jnp.where(allowed, scores, NEG_BIG)
        row_max = jnp.max(scores, axis=-1, keepdims=True)
        exp_scores = jnp.exp(scores - row_max)
        row_sum = jnp.sum(exp_scores, axis=-1, keepdims=True)
        prob_bf = (exp_scores / row_sum).astype(BF16)
        out_blk = jnp.einsum("bkgqs,bskd->bqkgd", prob_bf, v_proj, preferred_element_type=F32)
        out_blk = out_blk.astype(BF16).reshape(n_batch, q_block, n_heads, head_dim)
        norm_blk = (row_max + jnp.log(row_sum))[..., 0]
        out_buf = lax.dynamic_update_slice_in_dim(out_buf, out_blk, q_start, axis=1)
        norm_buf = lax.dynamic_update_slice_in_dim(norm_buf, norm_blk, q_start, axis=3)
        return out_buf, norm_buf

    init_state = (jnp.zeros(q_rot.shape, BF16), jnp.zeros((n_batch, n_kv, n_group, q_len), F32))
    return lax.fori_loop(0, q_len // q_block, block_step, init_state)


def attn_backward(q_rot, k_rot, v_proj, grad_out, log_norm, q_block):
    n_batch, q_len, n_heads, head_dim = q_rot.shape
    k_len, n_kv = k_rot.shape[1], k_rot.shape[2]
    n_group = n_heads // n_kv
    attn_scale = head_dim ** -0.5
    key_index = jnp.arange(k_len)

    def block_step(block_idx, loop_state):
        dq_buf, dk_acc, dv_acc = loop_state
        q_start = block_idx * q_block
        q_blk = lax.dynamic_slice_in_dim(q_rot, q_start, q_block, axis=1).reshape(n_batch, q_block, n_kv, n_group, head_dim)
        do_blk = lax.dynamic_slice_in_dim(grad_out, q_start, q_block, axis=1).reshape(n_batch, q_block, n_kv, n_group, head_dim)
        norm_blk = lax.dynamic_slice_in_dim(log_norm, q_start, q_block, axis=3)
        scores = jnp.einsum("bqkgd,bskd->bkgqs", q_blk, k_rot, preferred_element_type=F32) * attn_scale
        allowed = (q_start + jnp.arange(q_block))[:, None] >= key_index[None, :]
        scores = jnp.where(allowed, scores, NEG_BIG)
        probs_f = jnp.exp(scores - norm_blk[..., None])
        grad_prob = jnp.einsum("bqkgd,bskd->bkgqs", do_blk, v_proj, preferred_element_type=F32)
        grad_scores = probs_f * (grad_prob - jnp.sum(probs_f * grad_prob, axis=-1, keepdims=True))
        grad_scores = (grad_scores * attn_scale).astype(BF16)
        dq_blk = jnp.einsum("bkgqs,bskd->bqkgd", grad_scores, k_rot, preferred_element_type=F32)
        dq_blk = dq_blk.astype(BF16).reshape(n_batch, q_block, n_heads, head_dim)
        dk_acc = dk_acc + jnp.einsum("bkgqs,bqkgd->bskd", grad_scores, q_blk, preferred_element_type=F32)
        dv_acc = dv_acc + jnp.einsum("bkgqs,bqkgd->bskd", probs_f.astype(BF16), do_blk, preferred_element_type=F32)
        dq_buf = lax.dynamic_update_slice_in_dim(dq_buf, dq_blk, q_start, axis=1)
        return dq_buf, dk_acc, dv_acc

    init_state = (jnp.zeros(q_rot.shape, BF16), jnp.zeros(k_rot.shape, F32), jnp.zeros(v_proj.shape, F32))
    return lax.fori_loop(0, q_len // q_block, block_step, init_state)


def rope_rotate(values, cos_t, sin_t, rot_sign):
    rows, cols = values.shape
    reps = cols // 128
    lane = lax.broadcasted_iota(jnp.int32, (rows, cols), 1)
    low = (lane & 63) < 32
    up_roll = jnp.roll(values, -32, axis=1)
    down_roll = jnp.roll(values, 32, axis=1)
    other = jnp.where(low, -up_roll, down_roll)
    return values * jnp.tile(cos_t, (1, reps)) + rot_sign * other * jnp.tile(sin_t, (1, reps))


def solution(mesh):
    flat_axes = ("dp", "sp")
    row_spec = P("dp", "sp", None)
    pos_spec = P("dp", "sp")
    vec_spec = P(flat_axes)
    mat_spec = P(flat_axes, None)
    cube_spec = P(flat_axes, None, None)
    x_pairs = [(i, i ^ 1) for i in range(4)]
    y_pairs = [(i, i ^ 2) for i in range(4)]
    d_pairs = [(i, i ^ 3) for i in range(4)]
    s_pairs = [(0, 1), (1, 0)]

    def send_x(v):
        return lax.ppermute(v, "dp", x_pairs)

    def send_y(v):
        return lax.ppermute(v, "dp", y_pairs)

    def send_d(v):
        return lax.ppermute(v, "dp", d_pairs)

    def send_s(v):
        return lax.ppermute(v, "sp", s_pairs)

    def spread(own):
        return own, send_x(own), send_y(own)

    def relay(parts):
        own, from_x, from_y = parts
        half = own.shape[0] // 2
        return own, from_x, from_y, jnp.concatenate([send_y(from_x[:half]), send_x(from_y[half:])], axis=0)

    def scatter4(chunks):
        c0, c1, c2, c3 = chunks
        half = c0.shape[0] // 2
        t1 = send_x(c3[:half])
        t2 = send_y(c3[half:])
        u1 = send_x(c1[:half])
        u2 = send_y(c2[half:])
        v1 = send_x(c1[half:] + t2)
        v2 = send_y(c2[:half] + t1)
        return jnp.concatenate([c0[:half] + u1 + v2, c0[half:] + v1 + u2], axis=0)

    def local_step(act_in, positions, out_grad, norm1_gain, norm2_gain, w_query, w_key, w_value, w_out, w_gate, w_up, w_down):
        dp = lax.axis_index("dp")
        sp = lax.axis_index("sp")
        first = sp == 0
        n_tok, d_model = act_in.shape[1], act_in.shape[2]
        d_shard = w_gate.shape[0]
        n_q, n_kv, hd = w_query.shape[1], w_key.shape[1], w_query.shape[2]
        q_cols, kv_cols = n_q * hd, n_kv * hd
        f_quarter = w_gate.shape[1] // 4
        place = jnp.arange(8, dtype=jnp.int32)
        rel_table = (((place & 3) ^ dp) * 2 + ((place >> 2) ^ sp)).astype(jnp.int32)
        block = jnp.arange(8, dtype=jnp.int32)
        abs_table = (((block & 1) ^ sp) * 4 + ((block >> 1) ^ dp)).astype(jnp.int32)
        quarter_table = (jnp.arange(4, dtype=jnp.int32) ^ dp).astype(jnp.int32)

        def to_rel(v):
            return pick_blocks(rel_table, v, d_shard)

        def to_abs(v):
            return pick_blocks(abs_table, v, d_shard)

        def pick_half(v):
            h = v.shape[1] // 2
            return jnp.where(first, v[:, :h], v[:, h:]), jnp.where(first, v[:, h:], v[:, :h])

        def in_order(mine, other, axis):
            return jnp.where(first, jnp.concatenate([mine, other], axis=axis), jnp.concatenate([other, mine], axis=axis))

        act = act_in[0]
        dy = out_grad[0]
        pos = positions[0]

        w_qkv = jnp.concatenate([w_query.reshape(d_shard, q_cols), w_key.reshape(d_shard, kv_cols), w_value.reshape(d_shard, kv_cols)], axis=1)
        qkv_parts = spread(w_qkv)
        wo_parts = spread(w_out)
        gains = jnp.stack([norm1_gain, norm2_gain])
        gain_list = [gains, send_x(gains), send_y(gains), send_d(gains)]
        gain_mine = jnp.concatenate(gain_list, axis=1)
        gain_rel = jnp.concatenate([gain_mine, send_s(gain_mine)], axis=1).astype(F32)
        gain1_rel, gain2_rel = gain_rel[0:1], gain_rel[1:2]

        act_f = act.astype(F32)
        scale_a = lax.rsqrt(jnp.mean(act_f * act_f, axis=-1, keepdims=True) + EPS)
        unit_a = to_rel(act).astype(F32) * scale_a
        normed_a = (unit_a * gain1_rel).astype(BF16)

        inv_freq = ROPE_BASE ** (-(jnp.arange(hd // 2, dtype=F32) * (2.0 / hd)))
        angles = pos.astype(F32)[:, None] * inv_freq
        cos_t = jnp.tile(jnp.cos(angles), (1, 4))
        sin_t = jnp.tile(jnp.sin(angles), (1, 4))

        qkv_list = relay(qkv_parts)
        qkv_mine = jnp.concatenate(qkv_list, axis=0)
        qkv_other = send_s(qkv_mine)
        wo_list = relay(wo_parts)
        wo_mine = jnp.concatenate(wo_list, axis=0)
        wo_other = send_s(wo_mine)
        half_d = d_model // 2

        w_pairs = jnp.concatenate([pick_blocks(quarter_table, w_gate, f_quarter), pick_blocks(quarter_table, w_up, f_quarter)], axis=0)
        w_pairs = after(w_pairs, qkv_parts[1], qkv_parts[2])
        pair_r = [w_pairs[:, r * f_quarter:(r + 1) * f_quarter] for r in range(4)]
        pair_got = [pair_r[0], send_x(pair_r[1]), send_y(pair_r[2]), send_d(pair_r[3])]
        w1_mine = jnp.concatenate([p[:d_shard] for p in pair_got], axis=0)
        w3_mine = jnp.concatenate([p[d_shard:] for p in pair_got], axis=0)
        w1_full = jnp.concatenate([w1_mine, send_s(w1_mine)], axis=0)
        w3_full = jnp.concatenate([w3_mine, send_s(w3_mine)], axis=0)
        w2_full = in_order(w_down, send_s(w_down), 0)

        qkv = dot(normed_a[:, :half_d], qkv_mine) + dot(normed_a[:, half_d:], qkv_other)
        q_rot = rope_rotate(qkv[:, :q_cols], cos_t, sin_t, 1.0).astype(BF16)
        k_rot = rope_rotate(qkv[:, q_cols:q_cols + kv_cols], cos_t, sin_t, 1.0).astype(BF16)
        v_proj = qkv[:, q_cols + kv_cols:].astype(BF16)

        q_keep, q_send = pick_half(q_rot)
        k_keep, k_send = pick_half(k_rot)
        v_keep, v_send = pick_half(v_proj)
        kept = jnp.concatenate([q_keep, k_keep, v_keep], axis=1)
        got = send_s(jnp.concatenate([q_send, k_send, v_send], axis=1))
        seq = in_order(kept, got, 0)
        seq_len = seq.shape[0]
        hq, hk = q_cols // 2, kv_cols // 2
        q_heads = seq[:, :hq].reshape(1, seq_len, n_q // 2, hd)
        k_heads = seq[:, hq:hq + hk].reshape(1, seq_len, n_kv // 2, hd)
        v_heads = seq[:, hq + hk:].reshape(1, seq_len, n_kv // 2, hd)
        q_block = math.gcd(seq_len, 256)
        attn_heads, log_norm = attn_forward(q_heads, k_heads, v_heads, q_block)
        attn_flat = attn_heads.reshape(seq_len, hq)
        own_rows = jnp.where(first, attn_flat[:n_tok], attn_flat[n_tok:])
        far_rows = jnp.where(first, attn_flat[n_tok:], attn_flat[:n_tok])
        attn_tok = in_order(own_rows, send_s(far_rows), 1)
        attn_rel = to_rel(attn_tok)
        proj = dot(attn_rel[:, :half_d], wo_mine) + dot(attn_rel[:, half_d:], wo_other)
        hidden = (act_f + proj).astype(BF16)
        hidden_f = hidden.astype(F32)
        scale_b = lax.rsqrt(jnp.mean(hidden_f * hidden_f, axis=-1, keepdims=True) + EPS)
        unit_b = to_rel(hidden).astype(F32) * scale_b
        normed_b = (unit_b * gain2_rel).astype(BF16)

        w_list = relay(spread(normed_b))
        dy_own = after(dy, wo_parts[1], wo_parts[2])
        dy_list = relay(spread(dy_own))
        quarter_d = d_model // 8

        def swap_blocks(v, r):
            if r == 0:
                return v
            return jnp.concatenate([v[:, (s * 4 + (b ^ r)) * quarter_d:(s * 4 + (b ^ r) + 1) * quarter_d] for s in range(2) for b in range(4)], axis=1)

        w_rows = [swap_blocks(w_list[r], r) for r in range(4)]
        gate_list, up_list, mixed_list, y_list = [], [], [], []
        for r in range(4):
            gate_pre = dot(w_rows[r], w1_full)
            up_pre = dot(w_rows[r], w3_full)
            mixed = (gate_pre * jax.nn.sigmoid(gate_pre) * up_pre).astype(BF16)
            gate_list.append(gate_pre)
            up_list.append(up_pre)
            mixed_list.append(mixed)
        dgate_list, dup_list, dw_list = [], [], []
        for r in (3, 1, 2, 0):
            grad_mixed = dot_nt(dy_list[r], w2_full).astype(BF16).astype(F32)
            sig = jax.nn.sigmoid(gate_list[r])
            dup = (grad_mixed * gate_list[r] * sig).astype(BF16)
            dgate = (grad_mixed * up_list[r] * sig * (1.0 + gate_list[r] * (1.0 - sig))).astype(BF16)
            dw = dot_nt(dgate, w1_full) + dot_nt(dup, w3_full)
            dgate_list.append((r, dgate))
            dup_list.append((r, dup))
            dw_list.append((r, swap_blocks(dw, r)))
        dgate_list = [v for _, v in sorted(dgate_list, key=lambda t: t[0])]
        dup_list = [v for _, v in sorted(dup_list, key=lambda t: t[0])]
        dw_list = [v for _, v in sorted(dw_list, key=lambda t: t[0])]
        for r in range(4):
            y_list.append(dot(mixed_list[r], w2_full))
        dw_sum = scatter4(dw_list)
        y_sum = scatter4(y_list)
        act_out = (hidden_f + y_sum).astype(BF16)

        w_all = jnp.concatenate(w_rows, axis=0)
        dgate_all = jnp.concatenate(dgate_list, axis=0)
        dup_all = jnp.concatenate(dup_list, axis=0)
        mixed_all = jnp.concatenate(mixed_list, axis=0)
        dy_all = jnp.concatenate(dy_list, axis=0)

        def column_total(grad_all):
            far = dot_tn(w_all[:, half_d:], grad_all)
            near = dot_tn(w_all[:, :half_d], grad_all)
            return near + send_s(far)

        def column_grad(total):
            part = [total[r * d_shard:(r + 1) * d_shard] for r in range(4)]
            pieces = [part[0], send_x(part[1]), send_y(part[2]), send_d(part[3])]
            return pick_blocks(quarter_table, jnp.concatenate(pieces, axis=1), f_quarter)

        mixed_mine, mixed_far = pick_half(mixed_all)
        down_grad = dot_tn(mixed_mine, dy_all) + send_s(dot_tn(mixed_far, dy_all))
        gate_total = column_total(dgate_all)
        up_total = column_total(dup_all)
        gate_grad = column_grad(gate_total)
        up_grad = column_grad(up_total)
        dw_sum = after(dw_sum, gate_total, up_total)

        grad_normed_b = dw_sum.astype(BF16).astype(F32)
        gain2_part = jnp.sum(grad_normed_b * unit_b, axis=0, keepdims=True)
        grad_unit_b = grad_normed_b * gain2_rel
        rows_b = scale_b * (grad_unit_b - unit_b * jnp.mean(grad_unit_b * unit_b, axis=-1, keepdims=True))
        grad_hidden = (dy.astype(F32) + to_abs(rows_b)).astype(BF16)

        def row_grad(left, right):
            far = dot_tn(left[:, half_d:], right)
            near = dot_tn(left[:, :half_d], right)
            total = near + send_s(far)
            return scatter4([total[r * d_shard:(r + 1) * d_shard] for r in range(4)])

        wout_grad = row_grad(attn_rel, grad_hidden)
        dattn_rel = jnp.concatenate([dot_nt(grad_hidden, wo_mine), dot_nt(grad_hidden, wo_other)], axis=1).astype(BF16)
        dattn = to_abs(dattn_rel)
        d_keep, d_send = pick_half(dattn)
        dattn_heads = in_order(d_keep, send_s(d_send), 0).reshape(1, seq_len, n_q // 2, hd)
        dq_heads, dk_heads, dv_heads = attn_backward(q_heads, k_heads, v_heads, dattn_heads, log_norm, q_block)
        dqkv = jnp.concatenate([dq_heads.reshape(seq_len, hq), dk_heads.astype(BF16).reshape(seq_len, hk), dv_heads.astype(BF16).reshape(seq_len, hk)], axis=1)
        dqkv_own = jnp.where(first, dqkv[:n_tok], dqkv[n_tok:])
        dqkv_far = send_s(jnp.where(first, dqkv[n_tok:], dqkv[:n_tok]))
        dq_tok = in_order(dqkv_own[:, :hq], dqkv_far[:, :hq], 1)
        dk_tok = in_order(dqkv_own[:, hq:hq + hk], dqkv_far[:, hq:hq + hk], 1)
        dv_tok = in_order(dqkv_own[:, hq + hk:], dqkv_far[:, hq + hk:], 1)
        grad_q = rope_rotate(dq_tok.astype(F32), cos_t, sin_t, -1.0).astype(BF16)
        grad_k = rope_rotate(dk_tok.astype(F32), cos_t, sin_t, -1.0).astype(BF16)
        grad_qkv = jnp.concatenate([grad_q, grad_k, dv_tok], axis=1)
        qkv_grad = row_grad(normed_a, grad_qkv)
        query_grad = qkv_grad[:, :q_cols].reshape(w_query.shape)
        key_grad = qkv_grad[:, q_cols:q_cols + kv_cols].reshape(w_key.shape)
        value_grad = qkv_grad[:, q_cols + kv_cols:].reshape(w_value.shape)
        grad_normed_a = jnp.concatenate([dot_nt(grad_qkv, qkv_mine), dot_nt(grad_qkv, qkv_other)], axis=1).astype(BF16).astype(F32)
        gain1_part = jnp.sum(grad_normed_a * unit_a, axis=0, keepdims=True)
        grad_unit_a = grad_normed_a * gain1_rel
        rows_a = scale_a * (grad_unit_a - unit_a * jnp.mean(grad_unit_a * unit_a, axis=-1, keepdims=True))
        in_grad = (grad_hidden.astype(F32) + to_abs(rows_a)).astype(BF16)

        gain_part = jnp.concatenate([gain1_part, gain2_part], axis=0)
        gain_half = gain_part[:, :half_d] + send_s(gain_part[:, half_d:])
        gp = [gain_half[:, r * d_shard:(r + 1) * d_shard] for r in range(4)]
        gain_grad = gp[0] + send_x(gp[1]) + send_y(gp[2]) + send_d(gp[3])
        return (act_out[None], in_grad[None], gain_grad[0], gain_grad[1], query_grad, key_grad, value_grad, wout_grad, gate_grad, up_grad, down_grad)

    return jax.shard_map(local_step, mesh=mesh, in_specs=(row_spec, pos_spec, row_spec, vec_spec, vec_spec, cube_spec, cube_spec, cube_spec, mat_spec, mat_spec, mat_spec, mat_spec), out_specs=(row_spec, row_spec, vec_spec, vec_spec, cube_spec, cube_spec, cube_spec, mat_spec, mat_spec, mat_spec, mat_spec), check_vma=False)
```

```python
import jax
import jax.numpy as jnp
from jax import lax
from jax.experimental import pallas as pl
from jax.experimental.pallas import tpu as pltpu
from jax.sharding import PartitionSpec as P

INTERPRET = False

EPS = 1e-5
ROPE_BASE = 10000.0
NEG_BIG = -1e30
F32 = jnp.float32
BF16 = jnp.bfloat16
BLK = 256


def dot(a, b):
    return lax.dot_general(a, b, (((1,), (0,)), ((), ())), preferred_element_type=F32)


def dot_nt(a, b):
    return lax.dot_general(a, b, (((1,), (1,)), ((), ())), preferred_element_type=F32)


def dot_tn(a, b):
    return lax.dot_general(a, b, (((0,), (0,)), ((), ())), preferred_element_type=F32)


def after(value, *deps):
    return lax.optimization_barrier((value,) + deps)[0]


def sds(shape, dtype):
    return jax.ShapeDtypeStruct(shape, dtype)


def whole(shape):
    zeros = (0,) * len(shape)
    return pl.BlockSpec(shape, lambda j, t: zeros)


def call(body, name, ids, args, grid, in_specs, out_specs, out_shape, scratch=(), gflop=1.0, mbytes=1.0, aliases=None):
    return pl.pallas_call(
        body,
        out_shape=out_shape,
        grid_spec=pltpu.PrefetchScalarGridSpec(num_scalar_prefetch=1, grid=(grid,), in_specs=in_specs, out_specs=out_specs, scratch_shapes=list(scratch)),
        cost_estimate=pl.CostEstimate(flops=int(gflop * 1e9), bytes_accessed=int(mbytes * 1e6), transcendentals=0),
        compiler_params=pltpu.CompilerParams(dimension_semantics=("arbitrary",)),
        input_output_aliases=aliases or {},
        interpret=INTERPRET,
        name=name,
    )(ids, *args)


SP, DP = 16, 17


def lane_block(index, width=BLK):
    return pl.ds(pl.multiple_of(index * width, width), width)


def norm_kernel(ids, act, gain_rel):
    rows, cols = act.shape
    tile = 128

    def body(t, x_ref, g_ref, o_ref):
        x = x_ref[...].astype(F32)
        scale = lax.rsqrt(jnp.mean(x * x, axis=-1, keepdims=True) + EPS)
        for p in range(8):
            blk = x_ref[:, lane_block(t[p])].astype(F32)
            o_ref[:, p * BLK:(p + 1) * BLK] = (blk * scale * g_ref[:, p * BLK:(p + 1) * BLK]).astype(BF16)

    return call(body, "norm_in", ids, (act, gain_rel), rows // tile,
                [pl.BlockSpec((tile, cols), lambda j, t: (j, 0)), whole((1, cols))],
                pl.BlockSpec((tile, cols), lambda j, t: (j, 0)), sds((rows, cols), BF16), gflop=2.0, mbytes=4)


def rope_lanes(values, cos_t, sin_t, sign):
    width = values.shape[1]
    reps = width // 128
    if reps > 1:
        cos_t = jnp.concatenate([cos_t] * reps, axis=1)
        sin_t = jnp.concatenate([sin_t] * reps, axis=1)
    lane = lax.broadcasted_iota(jnp.int32, values.shape, 1)
    up_roll = pltpu.roll(values, width - 32, 1)
    down_roll = pltpu.roll(values, 32, 1)
    other = jnp.where((lane & 63) < 32, -up_roll, down_roll)
    return values * cos_t + (other * sin_t if sign > 0 else -(other * sin_t))


def qkv_kernel(ids, u_rel, w_mine, w_other, cos_t, sin_t):
    rows, d_model = u_rel.shape
    half_d = d_model // 2

    def column(j, t):
        far = (j < 6).astype(jnp.int32)
        half = t[SP] ^ far
        tile = j - 6 * (1 - far)
        return jnp.where(tile < 4, half * 4 + tile, 2 * tile + half)

    def body(t, u_ref, wm_ref, wo_ref, cos_ref, sin_ref, far_ref, keep_ref):
        j = pl.program_id(0)
        acc = dot(u_ref[:, :half_d], wm_ref[...]) + dot(u_ref[:, half_d:], wo_ref[...])
        roped = rope_lanes(acc, cos_ref[...], sin_ref[...], 1)
        is_value = (j == 5) | (j == 11)
        out = jnp.where(is_value, acc, roped).astype(BF16)

        @pl.when(j < 6)
        def _():
            for e in range(4):
                far_ref[e] = out[:, 64 * e:64 * e + 64]

        @pl.when(j >= 6)
        def _():
            for e in range(4):
                keep_ref[e] = out[:, 64 * e:64 * e + 64]

    w_spec = pl.BlockSpec((half_d, BLK), lambda j, t: (0, column(j, t)))
    return call(body, "qkv_proj", ids, (u_rel, w_mine, w_other, cos_t, sin_t), 12,
                [whole((rows, d_model)), w_spec, w_spec, whole((rows, 128)), whole((rows, 128))],
                [pl.BlockSpec((4, rows, 64), lambda j, t: (jnp.minimum(j, 5), 0, 0)), pl.BlockSpec((4, rows, 64), lambda j, t: (jnp.maximum(j - 6, 0), 0, 0))],
                [sds((24, rows, 64), BF16)] * 2, gflop=6.5, mbytes=20)


def ordered_rows(t, ref, own, other, rows):
    ref[pl.ds(pl.multiple_of(t[SP] * rows, rows), rows), :] = own
    ref[pl.ds(pl.multiple_of((1 - t[SP]) * rows, rows), rows), :] = other


def masked_scores(q_tile, keys, n_tile, tile):
    scores = dot_nt(q_tile, keys) * 0.125
    row = lax.broadcasted_iota(jnp.int32, (tile, tile), 0)
    col = lax.broadcasted_iota(jnp.int32, (tile, tile), 1)
    last = jnp.where(row >= col, scores[:, n_tile * tile:], NEG_BIG)
    return last if n_tile == 0 else jnp.concatenate([scores[:, :n_tile * tile], last], axis=1)


def attn_fwd_kernel(ids, keep, got):
    rows = keep.shape[1]
    seq = 2 * rows
    tile = 256

    def body(t, qk_ref, kk_ref, vk_ref, qg_ref, kg_ref, vg_ref, keep_ref, send_ref, ks, vs, qs, os):
        ordered_rows(t, ks, kk_ref[0], kg_ref[0], rows)
        ordered_rows(t, vs, vk_ref[0], vg_ref[0], rows)

        def head(h, carry):
            ordered_rows(t, qs, qk_ref[h], qg_ref[h], rows)
            for i in range(seq // tile):
                span = (i + 1) * tile
                scores = masked_scores(qs[i * tile:span, :], ks[:span, :], i, tile)
                top = jnp.max(scores, axis=-1, keepdims=True)
                expo = jnp.exp(scores - top)
                prob = (expo * (1.0 / jnp.sum(expo, axis=-1, keepdims=True))).astype(BF16)
                os[i * tile:span, :] = dot(prob, vs[:span, :]).astype(BF16)
            keep_ref[h] = os[pl.ds(pl.multiple_of(t[SP] * rows, rows), rows), :]
            send_ref[h] = os[pl.ds(pl.multiple_of((1 - t[SP]) * rows, rows), rows), :]
            return carry

        lax.fori_loop(0, 4, head, 0)

    q_spec = pl.BlockSpec((4, rows, 64), lambda j, t: (j, 0, 0))
    k_spec = pl.BlockSpec((1, rows, 64), lambda j, t: (16 + j, 0, 0))
    v_spec = pl.BlockSpec((1, rows, 64), lambda j, t: (20 + j, 0, 0))
    return call(body, "attn_fwd", ids, (keep, keep, keep, got, got, got), 4, [q_spec, k_spec, v_spec] * 2,
                [q_spec, q_spec], [sds((16, rows, 64), BF16)] * 2, [pltpu.VMEM((seq, 64), BF16)] * 4, gflop=20, mbytes=10)


def attn_bwd_kernel(ids, keep, got, do_keep, do_got):
    rows = keep.shape[1]
    seq = 2 * rows
    tile = 256

    def body(t, qk_ref, kk_ref, vk_ref, dk_ref, qg_ref, kg_ref, vg_ref, dg_ref, keep_ref, send_ref, ks, vs, qs, ds, dqs, dks, dvs):
        g = pl.program_id(0)
        ordered_rows(t, ks, kk_ref[0], kg_ref[0], rows)
        ordered_rows(t, vs, vk_ref[0], vg_ref[0], rows)
        dks[...] = jnp.zeros_like(dks)
        dvs[...] = jnp.zeros_like(dvs)
        own = pl.ds(pl.multiple_of(t[SP] * rows, rows), rows)
        far = pl.ds(pl.multiple_of((1 - t[SP]) * rows, rows), rows)

        def head(h, carry):
            ordered_rows(t, qs, qk_ref[h], qg_ref[h], rows)
            ordered_rows(t, ds, dk_ref[h], dg_ref[h], rows)
            for i in range(seq // tile):
                span = (i + 1) * tile
                q_tile = qs[i * tile:span, :]
                do_tile = ds[i * tile:span, :]
                scores = masked_scores(q_tile, ks[:span, :], i, tile)
                top = jnp.max(scores, axis=-1, keepdims=True)
                expo = jnp.exp(scores - top)
                prob = expo * (1.0 / jnp.sum(expo, axis=-1, keepdims=True))
                grad_prob = dot_nt(do_tile, vs[:span, :])
                inner = jnp.sum(prob * grad_prob, axis=-1, keepdims=True)
                grad_scores = (prob * (grad_prob - inner) * 0.125).astype(BF16)
                dqs[i * tile:span, :] = dot(grad_scores, ks[:span, :]).astype(BF16)
                dks[:span, :] += dot_tn(grad_scores, q_tile)
                dvs[:span, :] += dot_tn(prob.astype(BF16), do_tile)
            keep_ref[4 * g + h] = dqs[own, :]
            send_ref[4 * g + h] = dqs[far, :]
            return carry

        lax.fori_loop(0, 4, head, 0)
        keep_ref[16 + g] = dks[own, :].astype(BF16)
        send_ref[16 + g] = dks[far, :].astype(BF16)
        keep_ref[20 + g] = dvs[own, :].astype(BF16)
        send_ref[20 + g] = dvs[far, :].astype(BF16)

    q_spec = pl.BlockSpec((4, rows, 64), lambda j, t: (j, 0, 0))
    k_spec = pl.BlockSpec((1, rows, 64), lambda j, t: (16 + j, 0, 0))
    v_spec = pl.BlockSpec((1, rows, 64), lambda j, t: (20 + j, 0, 0))
    return call(body, "attn_bwd", ids, (keep, keep, keep, do_keep, got, got, got, do_got), 4, [q_spec, k_spec, v_spec, q_spec] * 2,
                [whole((24, rows, 64))] * 2, [sds((24, rows, 64), BF16)] * 2,
                [pltpu.VMEM((seq, 64), BF16)] * 5 + [pltpu.VMEM((seq, 64), F32)] * 2, gflop=50, mbytes=20)


def out_proj_kernel(ids, o_keep, o_got, w_mine, w_other, act, gain_rel):
    rows, d_model = act.shape
    half_d = d_model // 2
    tile = 512

    def body(t, ok_ref, og_ref, wm_ref, wo_ref, x_ref, g_ref, a_ref, h_ref, w_ref, a_abs):
        j = pl.program_id(0)

        @pl.when(j == 0)
        def _():
            for ref, half in ((ok_ref, t[SP]), (og_ref, 1 - t[SP])):
                for p in range(8):
                    a_abs[:, lane_block(half * 8 + p, 128)] = jnp.concatenate([ref[2 * p], ref[2 * p + 1]], axis=1)
            for p in range(8):
                a_ref[:, p * BLK:(p + 1) * BLK] = a_abs[:, lane_block(t[p])]

        acc = dot(a_ref[:, :half_d], wm_ref[...]) + dot(a_ref[:, half_d:], wo_ref[...])
        cols = lane_block(j, tile)
        h_ref[:, cols] = (x_ref[:, cols].astype(F32) + acc).astype(BF16)

        @pl.when(j == d_model // tile - 1)
        def _():
            for i in range(rows // 128):
                part = slice(i * 128, (i + 1) * 128)
                h = h_ref[part, :].astype(F32)
                scale = lax.rsqrt(jnp.mean(h * h, axis=-1, keepdims=True) + EPS)
                for p in range(8):
                    blk = h_ref[part, lane_block(t[p])].astype(F32)
                    w_ref[part, p * BLK:(p + 1) * BLK] = (blk * scale * g_ref[:, p * BLK:(p + 1) * BLK]).astype(BF16)

    w_spec = pl.BlockSpec((half_d, tile), lambda j, t: (0, j))
    return call(body, "out_proj", ids, (o_keep, o_got, w_mine, w_other, act, gain_rel), d_model // tile,
                [whole((16, rows, 64)), whole((16, rows, 64)), w_spec, w_spec, whole((rows, d_model)), whole((1, d_model))],
                [whole((rows, d_model))] * 3, [sds((rows, d_model), BF16)] * 3, [pltpu.VMEM((rows, d_model), BF16)], gflop=4.3, mbytes=20)


def swapped(place, k):
    return (place & 4) | ((place & 3) ^ k)


def ffn_in_kernel(ids, k, w_parts, dy_parts, w1, w3, w2, buffers):
    d_model, f_cols = w1.shape
    tile = 512
    rows = sum(p.shape[0] for p in w_parts)
    n_parts = len(w_parts)
    n_buf = 5 if buffers is not None else 0

    def body(t, *refs):
        w_refs, dy_refs = refs[:n_parts], refs[n_parts:2 * n_parts]
        w1_ref, w3_ref, w2_ref = refs[2 * n_parts:2 * n_parts + 3]
        wall_ref, dyall_ref, m_ref, dg_ref, du_ref = refs[2 * n_parts + 3 + n_buf:]
        j = pl.program_id(0)

        @pl.when(j == 0)
        def _():
            start = 0
            for wp, dp_ in zip(w_refs, dy_refs):
                n = wp.shape[0]
                for p in range(8):
                    src = swapped(p, k)
                    wall_ref[start:start + n, p * BLK:(p + 1) * BLK] = wp[:, src * BLK:(src + 1) * BLK]
                dyall_ref[start:start + n, :] = dp_[...]
                start += n

        gate = dot(wall_ref[...], w1_ref[...])
        up = dot(wall_ref[...], w3_ref[...])
        back = dot_nt(dyall_ref[...], w2_ref[...]).astype(BF16).astype(F32)
        sig = jax.nn.sigmoid(gate)
        act = gate * sig
        m_ref[...] = (act * up).astype(BF16)
        du_ref[...] = (back * act).astype(BF16)
        dg_ref[...] = (back * up * sig * (1.0 + gate * (1.0 - sig))).astype(BF16)

    in_specs = [whole(p.shape) for p in w_parts] + [whole(p.shape) for p in dy_parts]
    in_specs += [pl.BlockSpec((d_model, tile), lambda j, t: (0, j)), pl.BlockSpec((d_model, tile), lambda j, t: (0, j)), pl.BlockSpec((tile, d_model), lambda j, t: (j, 0))]
    in_specs += [pl.BlockSpec(memory_space=pl.ANY)] * n_buf
    args = tuple(w_parts) + tuple(dy_parts) + (w1, w3, w2) + (tuple(buffers) if n_buf else ())
    aliases = {1 + 2 * n_parts + 3 + i: i for i in range(n_buf)}
    row_spec = pl.BlockSpec((rows, d_model), lambda j, t: (k, 0))
    tile_spec = pl.BlockSpec((rows, tile), lambda j, t: (k, j))
    return call(body, "ffn_in_%d" % k, ids, args, f_cols // tile, in_specs, [row_spec, row_spec, tile_spec, tile_spec, tile_spec],
                [sds((4 * rows, d_model), BF16)] * 2 + [sds((4 * rows, f_cols), BF16)] * 3, gflop=13, mbytes=36, aliases=aliases)


def ffn_out_kernel(ids, k, mixed, dgate, dup, w1, w3, w2):
    d_model, f_cols = w1.shape
    rows = mixed.shape[0] // 4
    half = rows // 2

    def body(t, m_ref, dg_ref, du_ref, w1_ref, w3_ref, w2_ref, wa_ref, wb_ref, ya_ref, yb_ref):
        dw = dot_nt(dg_ref[...], w1_ref[...]) + dot_nt(du_ref[...], w3_ref[...])
        wa_ref[...] = dw[:half]
        wb_ref[...] = dw[half:]
        y = dot(m_ref[...], w2_ref[...])
        ya_ref[...] = y[:half]
        yb_ref[...] = y[half:]

    row_spec = pl.BlockSpec((rows, f_cols), lambda j, t: (k, 0))
    w_spec = pl.BlockSpec((BLK, f_cols), lambda j, t: (j, 0))
    dw_spec = pl.BlockSpec((half, BLK), lambda j, t: (0, (j & 4) | ((j & 3) ^ k)))
    y_spec = pl.BlockSpec((half, BLK), lambda j, t: (0, j))
    return call(body, "ffn_out_%d" % k, ids, (mixed, dgate, dup, w1, w3, w2), 8,
                [row_spec, row_spec, row_spec, w_spec, w_spec, pl.BlockSpec((f_cols, BLK), lambda j, t: (0, j))],
                [dw_spec, dw_spec, y_spec, y_spec], [sds((half, d_model), F32)] * 4, gflop=13, mbytes=40)


def norm_back(t, grad_ref, rows, src_ref, gain_ref, base_ref, out_ref, gain_out_ref):
    src = src_ref[rows, :].astype(F32)
    scale = lax.rsqrt(jnp.mean(src * src, axis=-1, keepdims=True) + EPS)
    inner = jnp.zeros_like(scale)
    for p in range(8):
        cols = slice(p * BLK, (p + 1) * BLK)
        unit = src_ref[rows, lane_block(t[p])].astype(F32) * scale
        grad = grad_ref[rows, cols].astype(F32)
        gain_out_ref[:, cols] += jnp.sum(grad * unit, axis=0, keepdims=True)
        inner += jnp.sum(grad * gain_ref[:, cols] * unit, axis=-1, keepdims=True)
    inner = inner * (1.0 / src.shape[1])
    for p in range(8):
        cols = slice(p * BLK, (p + 1) * BLK)
        place = lane_block(t[p])
        unit = src_ref[rows, place].astype(F32) * scale
        grad_rows = scale * (grad_ref[rows, cols].astype(F32) * gain_ref[:, cols] - unit * inner)
        out_ref[rows, place] = (base_ref[rows, place].astype(F32) + grad_rows).astype(BF16)


def hidden_grad_kernel(ids, parts_a, parts_b, hidden, gain_rel, dy):
    rows, d_model = hidden.shape
    half = rows // 2
    tile = 128
    n_half = half // tile

    def body(t, a0, a1, a2, b0, b1, b2, h_ref, g_ref, dy_ref, out_ref, gain_ref, grad):
        j = pl.program_id(0)

        @pl.when(j == 0)
        def _():
            gain_ref[...] = jnp.zeros_like(gain_ref)

        @pl.when(j < n_half)
        def _():
            grad[...] = (a0[...] + a1[...] + a2[...]).astype(BF16)

        @pl.when(j >= n_half)
        def _():
            grad[...] = (b0[...] + b1[...] + b2[...]).astype(BF16)

        norm_back(t, grad, slice(None), h_ref, g_ref, dy_ref, out_ref, gain_ref)

    a_spec = pl.BlockSpec((tile, d_model), lambda j, t: (jnp.minimum(j, n_half - 1), 0))
    b_spec = pl.BlockSpec((tile, d_model), lambda j, t: (jnp.maximum(j - n_half, 0), 0))
    row_spec = pl.BlockSpec((tile, d_model), lambda j, t: (j, 0))
    return call(body, "hidden_grad", ids, tuple(parts_a) + tuple(parts_b) + (hidden, gain_rel, dy), rows // tile,
                [a_spec] * 3 + [b_spec] * 3 + [row_spec, whole((1, d_model)), row_spec],
                [row_spec, whole((1, d_model))], [sds((rows, d_model), BF16), sds((1, d_model), F32)],
                [pltpu.VMEM((tile, d_model), BF16)], gflop=5, mbytes=20)


def attn_grad_kernel(ids, grad_hidden, w_mine, w_other):
    rows, d_model = grad_hidden.shape

    def block_row(j, t):
        half = t[SP] ^ (j < 2).astype(jnp.int32)
        return (half * 2 + (j & 1)) ^ t[DP]

    def body(t, g_ref, wm_ref, wo_ref, far_ref, keep_ref):
        j = pl.program_id(0)
        grads = [dot_nt(g_ref[...], ref[...]).astype(BF16) for ref in (wm_ref, wo_ref)]
        for cond, ref in ((j < 2, far_ref), (j >= 2, keep_ref)):
            @pl.when(cond)
            def _():
                for s in range(2):
                    for e in range(4):
                        ref[(t[SP] ^ s) * 4 + e] = grads[s][:, 64 * e:64 * e + 64]

    w_spec = pl.BlockSpec((BLK, d_model), lambda j, t: (block_row(j, t), 0))
    return call(body, "attn_grad", ids, (grad_hidden, w_mine, w_other), 4, [whole((rows, d_model)), w_spec, w_spec],
                [pl.BlockSpec((8, rows, 64), lambda j, t: (jnp.minimum(j, 1), 0, 0)), pl.BlockSpec((8, rows, 64), lambda j, t: (jnp.maximum(j - 2, 0), 0, 0))],
                [sds((16, rows, 64), BF16)] * 2, gflop=4.3, mbytes=14)


def unrope_kernel(ids, keep, got, cos_t, sin_t):
    rows = keep.shape[1]
    tile = 128

    def body(t, k_ref, g_ref, cos_ref, sin_ref, o_ref):
        for ref, half in ((k_ref, t[SP]), (g_ref, 1 - t[SP])):
            for p in range(12):
                pair = jnp.concatenate([ref[2 * p], ref[2 * p + 1]], axis=1)
                if p < 10:
                    pair = rope_lanes(pair.astype(F32), cos_ref[...], sin_ref[...], -1).astype(BF16)
                if p < 8:
                    place = half * 8 + p
                elif p < 10:
                    place = 16 + half * 2 + (p - 8)
                else:
                    place = 20 + half * 2 + (p - 10)
                o_ref[:, lane_block(place, 128)] = pair

    h_spec = pl.BlockSpec((24, tile, 64), lambda j, t: (0, j, 0))
    t_spec = pl.BlockSpec((tile, 128), lambda j, t: (j, 0))
    return call(body, "unrope", ids, (keep, got, cos_t, sin_t), rows // tile, [h_spec, h_spec, t_spec, t_spec],
                pl.BlockSpec((tile, 3072), lambda j, t: (j, 0)), sds((rows, 3072), BF16), gflop=3, mbytes=10)


def input_grad_kernel(ids, grad_qkv, w_mine, w_other, act, gain_rel, grad_hidden):
    rows, d_model = act.shape
    cols = grad_qkv.shape[1]

    def body(t, g_ref, wm_ref, wo_ref, x_ref, gain_ref, gh_ref, out_ref, gain_out_ref, grad):
        j = pl.program_id(0)

        @pl.when(j < 4)
        def _():
            grad[:, lane_block(j)] = dot_nt(g_ref[...], wm_ref[...]).astype(BF16)

        @pl.when(j >= 4)
        def _():
            grad[:, lane_block(j)] = dot_nt(g_ref[...], wo_ref[...]).astype(BF16)

        @pl.when(j == 7)
        def _():
            gain_out_ref[...] = jnp.zeros_like(gain_out_ref)

            def step(i, carry):
                norm_back(t, grad, pl.ds(pl.multiple_of(i * 128, 128), 128), x_ref, gain_ref, gh_ref, out_ref, gain_out_ref)
                return carry

            lax.fori_loop(0, rows // 128, step, 0)

    return call(body, "input_grad", ids, (grad_qkv, w_mine, w_other, act, gain_rel, grad_hidden), 8,
                [whole((rows, cols)), pl.BlockSpec((BLK, cols), lambda j, t: (jnp.minimum(j, 3), 0)), pl.BlockSpec((BLK, cols), lambda j, t: (jnp.maximum(j - 4, 0), 0)),
                 whole((rows, d_model)), whole((1, d_model)), whole((rows, d_model))],
                [whole((rows, d_model)), whole((1, d_model))], [sds((rows, d_model), BF16), sds((1, d_model), F32)],
                [pltpu.VMEM((rows, d_model), BF16)], gflop=10, mbytes=20)


def quarter_kernel(ids, w1, w3):
    rows, cols = w1.shape
    width = cols // 4

    def body(t, a_ref, b_ref, *outs):
        j = pl.program_id(0)
        for r in range(4):
            @pl.when(j == r)
            def _():
                outs[r][:rows, :] = a_ref[...]
                outs[r][rows:, :] = b_ref[...]

    spec = pl.BlockSpec((rows, width), lambda j, t: (0, t[DP] ^ j))
    return call(body, "quarters", ids, (w1, w3), 4, [spec, spec], [whole((2 * rows, width))] * 4, [sds((2 * rows, width), w1.dtype)] * 4, gflop=2, mbytes=17)


def place_kernel(ids, pieces):
    rows, width = pieces[0].shape

    def body(t, *refs):
        j = pl.program_id(0)
        for r in range(4):
            @pl.when(j == r)
            def _():
                refs[4][...] = refs[r][...]

    return call(body, "place", ids, pieces, 4, [whole((rows, width))] * 4, pl.BlockSpec((rows, width), lambda j, t: (0, t[DP] ^ j)),
                sds((rows, 4 * width), pieces[0].dtype), gflop=2, mbytes=17)


def solution(mesh):
    flat_axes = ("dp", "sp")
    row_spec = P("dp", "sp", None)
    pos_spec = P("dp", "sp")
    vec_spec = P(flat_axes)
    mat_spec = P(flat_axes, None)
    cube_spec = P(flat_axes, None, None)
    x_pairs = [(i, i ^ 1) for i in range(4)]
    y_pairs = [(i, i ^ 2) for i in range(4)]
    d_pairs = [(i, i ^ 3) for i in range(4)]
    s_pairs = [(0, 1), (1, 0)]

    def send_x(v):
        return lax.ppermute(v, "dp", x_pairs)

    def send_y(v):
        return lax.ppermute(v, "dp", y_pairs)

    def send_d(v):
        return lax.ppermute(v, "dp", d_pairs)

    def send_s(v):
        return lax.ppermute(v, "sp", s_pairs)

    def spread(own):
        return own, send_x(own), send_y(own)

    def relay(parts):
        own, from_x, from_y = parts
        half = own.shape[0] // 2
        return send_y(from_x[:half]), send_x(from_y[half:])

    def scatter4(halves, split=False):
        (a0, b0), (a1, b1), (a2, b2), (a3, b3) = halves
        u1 = send_x(a1)
        u2 = send_y(b2)
        t1 = send_x(a3)
        t2 = send_y(b3)
        v1 = send_x(b1 + t2)
        v2 = send_y(a2 + t1)
        if split:
            return (a0, u1, v2), (b0, v1, u2)
        return jnp.concatenate([a0 + u1 + v2, b0 + v1 + u2], axis=0)

    def local_step(act_in, positions, out_grad, norm1_gain, norm2_gain, w_query, w_key, w_value, w_out, w_gate, w_up, w_down):
        dp = lax.axis_index("dp")
        sp = lax.axis_index("sp")
        first = sp == 0
        n_q, n_kv, hd = w_query.shape[1], w_key.shape[1], w_query.shape[2]
        q_cols, kv_cols = n_q * hd, n_kv * hd
        half_d = act_in.shape[2] // 2
        place = jnp.arange(8, dtype=jnp.int32)
        rel_table = ((place & 3) ^ dp) * 2 + ((place >> 2) ^ sp)
        abs_table = ((place & 1) ^ sp) * 4 + ((place >> 1) ^ dp)
        ids = jnp.concatenate([rel_table, abs_table, jnp.stack([sp, dp])]).astype(jnp.int32)

        act = act_in[0]
        dy = out_grad[0]
        pos = positions[0]

        w_qkv = jnp.concatenate([w_query.reshape(BLK, q_cols), w_key.reshape(BLK, kv_cols), w_value.reshape(BLK, kv_cols)], axis=1)
        qkv_parts = spread(w_qkv)
        wo_parts = spread(w_out)
        gains = jnp.stack([norm1_gain, norm2_gain])
        gain_mine = jnp.concatenate([gains, send_x(gains), send_y(gains), send_d(gains)], axis=1)
        gain_rel = jnp.concatenate([gain_mine, send_s(gain_mine)], axis=1).astype(F32)
        gain1_rel, gain2_rel = gain_rel[0:1], gain_rel[1:2]
        w2_other = send_s(w_down)
        w2 = jnp.where(first, jnp.concatenate([w_down, w2_other], axis=0), jnp.concatenate([w2_other, w_down], axis=0))

        inv_freq = ROPE_BASE ** (-(jnp.arange(hd // 2, dtype=F32) * (2.0 / hd)))
        angles = pos.astype(F32)[:, None] * inv_freq
        cos_t = jnp.tile(jnp.cos(angles), (1, 4))
        sin_t = jnp.tile(jnp.sin(angles), (1, 4))
        u_rel = norm_kernel(ids, act, gain1_rel)
        quarters = quarter_kernel(ids, w_gate, w_up)

        qkv_mine = jnp.concatenate(qkv_parts + relay(qkv_parts), axis=0)
        qkv_other = send_s(qkv_mine)
        wo_mine = jnp.concatenate(wo_parts + relay(wo_parts), axis=0)
        wo_other = send_s(wo_mine)

        q1, q2, q3 = after(tuple(quarters[1:]), qkv_parts[1], qkv_parts[2])
        pairs = [quarters[0], send_x(q1), send_y(q2), send_d(q3)]
        w1_mine = jnp.concatenate([p[:BLK] for p in pairs], axis=0)
        w3_mine = jnp.concatenate([p[BLK:] for p in pairs], axis=0)
        w1 = jnp.concatenate([w1_mine, send_s(w1_mine)], axis=0)
        w3 = jnp.concatenate([w3_mine, send_s(w3_mine)], axis=0)

        qkv_far, qkv_keep = qkv_kernel(ids, u_rel, qkv_mine, qkv_other, cos_t, sin_t)
        qkv_got = send_s(qkv_far)
        o_keep, o_far = attn_fwd_kernel(ids, qkv_keep, qkv_got)
        o_got = send_s(o_far)
        attn_rel, hidden, normed = out_proj_kernel(ids, o_keep, o_got, wo_mine, wo_other, act, gain2_rel)

        w_parts = spread(normed)
        dy_parts = spread(after(dy, wo_parts[1], wo_parts[2]))
        w_diag = relay(w_parts)
        dy_diag = relay(dy_parts)
        bufs = ffn_in_kernel(ids, 0, [normed], [dy], w1, w3, w2, None)
        bufs = ffn_in_kernel(ids, 1, [w_parts[1]], [dy_parts[1]], w1, w3, w2, bufs)
        out1 = ffn_out_kernel(ids, 1, *bufs[2:], w1, w3, w2)
        bufs = ffn_in_kernel(ids, 2, [w_parts[2]], [dy_parts[2]], w1, w3, w2, after(tuple(bufs), *out1))
        out2 = ffn_out_kernel(ids, 2, *bufs[2:], w1, w3, w2)
        bufs = ffn_in_kernel(ids, 3, w_diag, dy_diag, w1, w3, w2, after(tuple(bufs), *out2))
        out3 = ffn_out_kernel(ids, 3, *bufs[2:], w1, w3, w2)
        bufs = after(tuple(bufs), *out3)
        out0 = ffn_out_kernel(ids, 0, *bufs[2:], w1, w3, w2)
        w_all, dy_all, mixed, dgate, dup = bufs
        parts_a, parts_b = scatter4([(o[0], o[1]) for o in (out0, out1, out2, out3)], split=True)
        y_sum = scatter4([(o[2], o[3]) for o in (out0, out1, out2, out3)])
        act_out = (hidden.astype(F32) + y_sum).astype(BF16)

        def column_total(grad_all):
            far = dot_tn(w_all[:, half_d:], grad_all)
            near = dot_tn(w_all[:, :half_d], grad_all)
            return near + send_s(far)

        def column_grad(total):
            part = [total[r * BLK:(r + 1) * BLK] for r in range(4)]
            return place_kernel(ids, [part[0], send_x(part[1]), send_y(part[2]), send_d(part[3])])

        gate_total = column_total(dgate)
        up_total = column_total(dup)
        gate_grad = column_grad(gate_total)
        up_grad = column_grad(up_total)
        half_f = mixed.shape[1] // 2
        mixed_mine = jnp.where(first, mixed[:, :half_f], mixed[:, half_f:])
        mixed_far = jnp.where(first, mixed[:, half_f:], mixed[:, :half_f])
        down_grad = dot_tn(mixed_mine, dy_all) + send_s(dot_tn(mixed_far, dy_all))

        hidden_after = after(hidden, gate_total, up_total)
        grad_hidden, gain2_part = hidden_grad_kernel(ids, parts_a, parts_b, hidden_after, gain2_rel, dy)

        def row_grad(left, right):
            far = dot_tn(left[:, half_d:], right)
            near = dot_tn(left[:, :half_d], right)
            total = near + send_s(far)
            half = BLK // 2
            return scatter4([(total[r * BLK:r * BLK + half], total[r * BLK + half:(r + 1) * BLK]) for r in range(4)])

        do_far, do_keep = attn_grad_kernel(ids, grad_hidden, wo_mine, wo_other)
        do_got = send_s(do_far)
        d_keep, d_far = attn_bwd_kernel(ids, qkv_keep, qkv_got, do_keep, do_got)
        d_got = send_s(d_far)
        wout_grad = row_grad(attn_rel, grad_hidden)
        grad_qkv = unrope_kernel(ids, d_keep, d_got, cos_t, sin_t)
        qkv_grad = row_grad(u_rel, grad_qkv)
        query_grad = qkv_grad[:, :q_cols].reshape(w_query.shape)
        key_grad = qkv_grad[:, q_cols:q_cols + kv_cols].reshape(w_key.shape)
        value_grad = qkv_grad[:, q_cols + kv_cols:].reshape(w_value.shape)
        in_grad, gain1_part = input_grad_kernel(ids, grad_qkv, qkv_mine, qkv_other, act, gain1_rel, grad_hidden)

        gain_part = jnp.concatenate([gain1_part, gain2_part], axis=0)
        gain_half = gain_part[:, :half_d] + send_s(gain_part[:, half_d:])
        gp = [gain_half[:, r * BLK:(r + 1) * BLK] for r in range(4)]
        gain_grad = gp[0] + send_x(gp[1]) + send_y(gp[2]) + send_d(gp[3])
        return (act_out[None], in_grad[None], gain_grad[0], gain_grad[1], query_grad, key_grad, value_grad, wout_grad, gate_grad, up_grad, down_grad)

    return jax.shard_map(local_step, mesh=mesh, in_specs=(row_spec, pos_spec, row_spec, vec_spec, vec_spec, cube_spec, cube_spec, cube_spec, mat_spec, mat_spec, mat_spec, mat_spec), out_specs=(row_spec, row_spec, vec_spec, vec_spec, cube_spec, cube_spec, cube_spec, mat_spec, mat_spec, mat_spec, mat_spec), check_vma=False)
```

```python
import jax
import jax.numpy as jnp
from jax import lax
from jax.experimental import pallas as pl
from jax.experimental.pallas import tpu as pltpu
from jax.sharding import PartitionSpec as P

INTERPRET = False

EPS = 1e-5
ROPE_BASE = 10000.0
NEG_BIG = -1e30
F32 = jnp.float32
BF16 = jnp.bfloat16
BLK = 256
TOKENS = 512


def dot(a, b):
    return lax.dot_general(a, b, (((1,), (0,)), ((), ())), preferred_element_type=F32)


def dot_nt(a, b):
    return lax.dot_general(a, b, (((1,), (1,)), ((), ())), preferred_element_type=F32)


def dot_tn(a, b):
    return lax.dot_general(a, b, (((0,), (0,)), ((), ())), preferred_element_type=F32)


def after(value, *deps):
    return lax.optimization_barrier((value,) + deps)[0]


def sds(shape, dtype):
    return jax.ShapeDtypeStruct(shape, dtype)


def whole(shape):
    zeros = (0,) * len(shape)
    return pl.BlockSpec(shape, lambda j, t: zeros)


def call(body, ids, args, grid, in_specs, out_specs, out_shape, scratch=(), gflop=1.0, mbytes=1.0, aliases=None):
    return pl.pallas_call(
        body,
        out_shape=out_shape,
        grid_spec=pltpu.PrefetchScalarGridSpec(num_scalar_prefetch=1, grid=(grid,), in_specs=in_specs, out_specs=out_specs, scratch_shapes=list(scratch)),
        cost_estimate=pl.CostEstimate(flops=int(gflop * 1e9), bytes_accessed=int(mbytes * 1e6), transcendentals=0),
        compiler_params=pltpu.CompilerParams(dimension_semantics=("arbitrary",)),
        input_output_aliases=aliases or {},
        interpret=INTERPRET,
    )(ids, *args)


SP, DP = 16, 17


def lane_block(index, width=BLK):
    return pl.ds(pl.multiple_of(index * width, width), width)


def norm_kernel(ids, act, gain_rel):
    rows, cols = act.shape
    tile = 128

    def body(t, x_ref, g_ref, o_ref):
        x = x_ref[...].astype(F32)
        scale = lax.rsqrt(jnp.mean(x * x, axis=-1, keepdims=True) + EPS)
        for p in range(8):
            blk = x_ref[:, lane_block(t[p])].astype(F32)
            o_ref[:, p * BLK:(p + 1) * BLK] = (blk * scale * g_ref[:, p * BLK:(p + 1) * BLK]).astype(BF16)

    return call(body, ids, (act, gain_rel), rows // tile,
                [pl.BlockSpec((tile, cols), lambda j, t: (j, 0)), whole((1, cols))],
                pl.BlockSpec((tile, cols), lambda j, t: (j, 0)), sds((rows, cols), BF16), gflop=2.0, mbytes=4)


def rope_lanes(values, cos_t, sin_t, sign):
    width = values.shape[1]
    reps = width // 128
    if reps > 1:
        cos_t = jnp.concatenate([cos_t] * reps, axis=1)
        sin_t = jnp.concatenate([sin_t] * reps, axis=1)
    lane = lax.broadcasted_iota(jnp.int32, values.shape, 1)
    up_roll = pltpu.roll(values, width - 32, 1)
    down_roll = pltpu.roll(values, 32, 1)
    other = jnp.where((lane & 63) < 32, -up_roll, down_roll)
    return values * cos_t + (other * sin_t if sign > 0 else -(other * sin_t))


def fill_tile(scratch, refs):
    start = 0
    for ref in refs:
        n = ref.shape[0]
        scratch[start:start + n, :] = ref[...]
        start += n


def qkv_kernel(ids, u_rel, pieces, cos_t, sin_t):
    rows, d_model = u_rel.shape
    cols = pieces[0].shape[1]
    n_pieces = len(pieces)

    def column(j, t):
        far = (j < 6).astype(jnp.int32)
        half = t[SP] ^ far
        tile = j - 6 * (1 - far)
        return jnp.where(tile < 4, half * 4 + tile, 2 * tile + half)

    def body(t, u_ref, cos_ref, sin_ref, *refs):
        far_ref, keep_ref, w_ref = refs[n_pieces:]
        j = pl.program_id(0)
        fill_tile(w_ref, refs[:n_pieces])
        acc = dot(u_ref[...], w_ref[...])
        roped = rope_lanes(acc, cos_ref[...], sin_ref[...], 1)
        is_value = (j == 5) | (j == 11)
        out = jnp.where(is_value, acc, roped).astype(BF16)

        @pl.when(j < 6)
        def _():
            far_ref[0] = out[:, :128]
            far_ref[1] = out[:, 128:]

        @pl.when(j >= 6)
        def _():
            keep_ref[0] = out[:, :128]
            keep_ref[1] = out[:, 128:]

    w_specs = [pl.BlockSpec((p.shape[0], BLK), lambda j, t: (0, column(j, t))) for p in pieces]
    return call(body, ids, (u_rel, cos_t, sin_t) + tuple(pieces), 12,
                [whole((rows, d_model)), whole((rows, 128)), whole((rows, 128))] + w_specs,
                [pl.BlockSpec((2, rows, 128), lambda j, t: (jnp.minimum(j, 5), 0, 0)), pl.BlockSpec((2, rows, 128), lambda j, t: (jnp.maximum(j - 6, 0), 0, 0)),
                 pl.BlockSpec((d_model, BLK), lambda j, t: (0, column(j, t)))],
                [sds((12, rows, 128), BF16)] * 2 + [sds((d_model, cols), BF16)], gflop=6.5, mbytes=30)


def ordered_rows(t, ref, own, other, rows):
    ref[pl.ds(pl.multiple_of(t[SP] * rows, rows), rows), :] = own
    ref[pl.ds(pl.multiple_of((1 - t[SP]) * rows, rows), rows), :] = other


def one_head(pair, odd):
    return jnp.where(odd == 1, pair[:, 64:], pair[:, :64])


def masked_scores(q_tile, keys, first_row, span):
    scores = dot_nt(q_tile, keys) * 0.125
    row = lax.broadcasted_iota(jnp.int32, (q_tile.shape[0], 256), 0) + first_row
    col = lax.broadcasted_iota(jnp.int32, (q_tile.shape[0], 256), 1)
    last = jnp.where(row >= col, scores[:, span - 256:], NEG_BIG)
    return last if span == 256 else jnp.concatenate([scores[:, :span - 256], last], axis=1)


def own_rows(t, rows):
    return pl.ds(pl.multiple_of(t[SP] * rows, rows), rows), pl.ds(pl.multiple_of((1 - t[SP]) * rows, rows), rows)


def attn_fwd_kernel(ids, keep, got):
    rows = keep.shape[1]
    seq = 2 * rows
    tile = 256

    def body(t, qk_ref, kk_ref, vk_ref, qg_ref, kg_ref, vg_ref, keep_ref, send_ref, ks, vs, qs, os):
        odd = pl.program_id(0) & 1
        ordered_rows(t, ks, one_head(kk_ref[0], odd), one_head(kg_ref[0], odd), rows)
        ordered_rows(t, vs, one_head(vk_ref[0], odd), one_head(vg_ref[0], odd), rows)

        def head(h, carry):
            ordered_rows(t, qs, one_head(qk_ref[h // 2], h & 1), one_head(qg_ref[h // 2], h & 1), rows)
            for i in range(seq // tile):
                span = (i + 1) * tile
                scores = masked_scores(qs[i * tile:span, :], ks[:span, :], 0, span)
                top = jnp.max(scores, axis=-1, keepdims=True)
                expo = jnp.exp(scores - top)
                prob = (expo * (1.0 / jnp.sum(expo, axis=-1, keepdims=True))).astype(BF16)
                os[h, i * tile:span, :] = dot(prob, vs[:span, :]).astype(BF16)
            return carry

        lax.fori_loop(0, 4, head, 0)
        for rows_here, ref in zip(own_rows(t, rows), (keep_ref, send_ref)):
            for p in range(2):
                ref[p] = jnp.concatenate([os[2 * p, rows_here, :], os[2 * p + 1, rows_here, :]], axis=1)

    q_spec = pl.BlockSpec((2, rows, 128), lambda j, t: (j, 0, 0))
    k_spec = pl.BlockSpec((1, rows, 128), lambda j, t: (8 + j // 2, 0, 0))
    v_spec = pl.BlockSpec((1, rows, 128), lambda j, t: (10 + j // 2, 0, 0))
    return call(body, ids, (keep, keep, keep, got, got, got), 4, [q_spec, k_spec, v_spec] * 2,
                [q_spec, q_spec], [sds((8, rows, 128), BF16)] * 2,
                [pltpu.VMEM((seq, 64), BF16)] * 3 + [pltpu.VMEM((4, seq, 64), BF16)], gflop=20, mbytes=10)


def attn_bwd_kernel(ids, keep, got, do_keep, do_got):
    rows = keep.shape[1]
    seq = 2 * rows
    tile = 256

    def body(t, qk_ref, kk_ref, vk_ref, dk_ref, qg_ref, kg_ref, vg_ref, dg_ref, keep_ref, send_ref, ks, vs, qs, ds, dqs, dks, dvs):
        g = pl.program_id(0)
        odd = g & 1
        ordered_rows(t, ks, one_head(kk_ref[0], odd), one_head(kg_ref[0], odd), rows)
        ordered_rows(t, vs, one_head(vk_ref[0], odd), one_head(vg_ref[0], odd), rows)
        dks[odd] = jnp.zeros_like(ks, F32)
        dvs[odd] = jnp.zeros_like(vs, F32)

        def head(h, carry):
            ordered_rows(t, qs, one_head(qk_ref[h // 2], h & 1), one_head(qg_ref[h // 2], h & 1), rows)
            ordered_rows(t, ds, one_head(dk_ref[h // 2], h & 1), one_head(dg_ref[h // 2], h & 1), rows)
            for i in range(seq // tile):
                span = (i + 1) * tile

                def strip(n, carry):
                    here = pl.ds(pl.multiple_of(i * tile + n * 128, 128), 128)
                    q_tile = qs[here, :]
                    do_tile = ds[here, :]
                    scores = masked_scores(q_tile, ks[:span, :], n * 128, span)
                    top = jnp.max(scores, axis=-1, keepdims=True)
                    expo = jnp.exp(scores - top)
                    prob = expo * (1.0 / jnp.sum(expo, axis=-1, keepdims=True))
                    grad_prob = dot_nt(do_tile, vs[:span, :])
                    inner = jnp.sum(prob * grad_prob, axis=-1, keepdims=True)
                    grad_scores = (prob * (grad_prob - inner) * 0.125).astype(BF16)
                    dqs[h, here, :] = dot(grad_scores, ks[:span, :]).astype(BF16)
                    dks[odd, :span, :] += dot_tn(grad_scores, q_tile)
                    dvs[odd, :span, :] += dot_tn(prob.astype(BF16), do_tile)
                    return carry

                lax.fori_loop(0, tile // 128, strip, 0)
            return carry

        lax.fori_loop(0, 4, head, 0)
        for rows_here, ref in zip(own_rows(t, rows), (keep_ref, send_ref)):
            for p in range(2):
                ref[2 * g + p] = jnp.concatenate([dqs[2 * p, rows_here, :], dqs[2 * p + 1, rows_here, :]], axis=1)

            @pl.when(odd == 1)
            def _():
                ref[8 + g // 2] = jnp.concatenate([dks[0, rows_here, :], dks[1, rows_here, :]], axis=1).astype(BF16)
                ref[10 + g // 2] = jnp.concatenate([dvs[0, rows_here, :], dvs[1, rows_here, :]], axis=1).astype(BF16)

    q_spec = pl.BlockSpec((2, rows, 128), lambda j, t: (j, 0, 0))
    k_spec = pl.BlockSpec((1, rows, 128), lambda j, t: (8 + j // 2, 0, 0))
    v_spec = pl.BlockSpec((1, rows, 128), lambda j, t: (10 + j // 2, 0, 0))
    return call(body, ids, (keep, keep, keep, do_keep, got, got, got, do_got), 4, [q_spec, k_spec, v_spec, q_spec] * 2,
                [whole((12, rows, 128))] * 2, [sds((12, rows, 128), BF16)] * 2,
                [pltpu.VMEM((seq, 64), BF16)] * 4 + [pltpu.VMEM((4, seq, 64), BF16)] + [pltpu.VMEM((2, seq, 64), F32)] * 2, gflop=50, mbytes=20)


def out_proj_kernel(ids, o_keep, o_got, pieces, act, gain_rel):
    rows, d_model = act.shape
    half = rows // 2
    tile = 256
    n_pieces = len(pieces)

    def body(t, ok_ref, og_ref, x_ref, g_ref, *refs):
        a_ref, h_ref, wa_ref, wb_ref, w_ref, a_abs = refs[n_pieces:]
        j = pl.program_id(0)

        @pl.when(j == 0)
        def _():
            for ref, side in ((ok_ref, t[SP]), (og_ref, 1 - t[SP])):
                for p in range(8):
                    a_abs[:, lane_block(side * 8 + p, 128)] = ref[p]
            for p in range(8):
                a_ref[:, p * BLK:(p + 1) * BLK] = a_abs[:, lane_block(t[p])]

        fill_tile(w_ref, refs[:n_pieces])
        acc = dot(a_ref[...], w_ref[...])
        cols = lane_block(j, tile)
        h_ref[:, cols] = (x_ref[:, cols].astype(F32) + acc).astype(BF16)

        @pl.when(j == d_model // tile - 1)
        def _():
            for out_ref, start in ((wa_ref, 0), (wb_ref, half)):
                def normed(i, carry):
                    part = pl.ds(pl.multiple_of(start + i * 64, 64), 64)
                    h = h_ref[part, :].astype(F32)
                    scale = lax.rsqrt(jnp.mean(h * h, axis=-1, keepdims=True) + EPS)
                    for p in range(8):
                        blk = h_ref[part, lane_block(t[p])].astype(F32)
                        out_ref[pl.ds(pl.multiple_of(i * 64, 64), 64), p * BLK:(p + 1) * BLK] = (blk * scale * g_ref[:, p * BLK:(p + 1) * BLK]).astype(BF16)
                    return carry

                lax.fori_loop(0, half // 64, normed, 0)

    w_specs = [pl.BlockSpec((p.shape[0], tile), lambda j, t: (0, j)) for p in pieces]
    return call(body, ids, (o_keep, o_got, act, gain_rel) + tuple(pieces), d_model // tile,
                [whole((8, rows, 128)), whole((8, rows, 128)), whole((rows, d_model)), whole((1, d_model))] + w_specs,
                [whole((rows, d_model))] * 2 + [whole((half, d_model))] * 2 + [pl.BlockSpec((d_model, tile), lambda j, t: (0, j))],
                [sds((rows, d_model), BF16)] * 2 + [sds((half, d_model), BF16)] * 2 + [sds((d_model, d_model), BF16)],
                [pltpu.VMEM((rows, d_model), BF16)], gflop=4.3, mbytes=26)


def swapped(place, k):
    return (place & 4) | ((place & 3) ^ k)


def ffn_fwd_kernel(ids, place, chunks, w1, w3, buffers):
    d_model, f_cols = w1.shape
    tile = 256
    owners = [k for k, parts in chunks for _ in parts]
    parts = [p for _, parts in chunks for p in parts]
    rows = sum(p.shape[0] for p in parts)
    n_parts = len(parts)
    n_buf = 4 if buffers is not None else 0

    def body(t, *refs):
        w1_ref, w3_ref = refs[n_parts:n_parts + 2]
        wall_ref, m_ref, gate_ref, up_ref = refs[n_parts + 2 + n_buf:]

        @pl.when(pl.program_id(0) == 0)
        def _():
            start = 0
            for k, ref in zip(owners, refs):
                n = ref.shape[0]
                for p in range(8):
                    src = swapped(p, k)
                    wall_ref[start:start + n, p * BLK:(p + 1) * BLK] = ref[:, src * BLK:(src + 1) * BLK]
                start += n

        def strip(n, carry):
            here = pl.ds(pl.multiple_of(n * TOKENS, TOKENS), TOKENS)
            gate = dot(wall_ref[here, :], w1_ref[...])
            up = dot(wall_ref[here, :], w3_ref[...])
            gate_ref[here, :] = gate
            up_ref[here, :] = up
            m_ref[here, :] = (gate * jax.nn.sigmoid(gate) * up).astype(BF16)
            return carry

        lax.fori_loop(0, rows // TOKENS, strip, 0)

    in_specs = [whole(p.shape) for p in parts] + [pl.BlockSpec((d_model, tile), lambda j, t: (0, j))] * 2 + [pl.BlockSpec(memory_space=pl.ANY)] * n_buf
    args = tuple(parts) + (w1, w3) + (tuple(buffers) if n_buf else ())
    tile_spec = pl.BlockSpec((rows, tile), lambda j, t: (place, j))
    total = 4 * TOKENS
    return call(body, ids, args, f_cols // tile, in_specs, [pl.BlockSpec((rows, d_model), lambda j, t: (place, 0))] + [tile_spec] * 3,
                [sds((total, d_model), BF16), sds((total, f_cols), BF16), sds((total, f_cols), F32), sds((total, f_cols), F32)],
                gflop=8.6, mbytes=30, aliases={1 + n_parts + 2 + i: i for i in range(n_buf)})


def ffn_bwd_kernel(ids, place, parts, gate_pre, up_pre, w2, buffers):
    f_cols, d_model = w2.shape
    tile = 256
    rows = sum(p.shape[0] for p in parts)
    n_parts = len(parts)
    n_buf = 3 if buffers is not None else 0

    def body(t, *refs):
        gate_ref, up_ref, w2_ref = refs[n_parts:n_parts + 3]
        dyall_ref, dg_ref, du_ref = refs[n_parts + 3 + n_buf:]

        @pl.when(pl.program_id(0) == 0)
        def _():
            fill_tile(dyall_ref, refs[:n_parts])

        def strip(n, carry):
            here = pl.ds(pl.multiple_of(n * TOKENS, TOKENS), TOKENS)
            back = dot_nt(dyall_ref[here, :], w2_ref[...]).astype(BF16).astype(F32)
            gate = gate_ref[here, :]
            sig = jax.nn.sigmoid(gate)
            du_ref[here, :] = (back * (gate * sig)).astype(BF16)
            dg_ref[here, :] = (back * up_ref[here, :] * sig * (1.0 + gate * (1.0 - sig))).astype(BF16)
            return carry

        lax.fori_loop(0, rows // TOKENS, strip, 0)

    tile_spec = pl.BlockSpec((rows, tile), lambda j, t: (place, j))
    in_specs = [whole(p.shape) for p in parts] + [tile_spec, tile_spec, pl.BlockSpec((tile, d_model), lambda j, t: (j, 0))] + [pl.BlockSpec(memory_space=pl.ANY)] * n_buf
    args = tuple(parts) + (gate_pre, up_pre, w2) + (tuple(buffers) if n_buf else ())
    total = 4 * TOKENS
    return call(body, ids, args, f_cols // tile, in_specs, [pl.BlockSpec((rows, d_model), lambda j, t: (place, 0))] + [tile_spec] * 2,
                [sds((total, d_model), BF16)] + [sds((total, f_cols), BF16)] * 2,
                gflop=8.6, mbytes=40, aliases={1 + n_parts + 3 + i: i for i in range(n_buf)})


def ffn_dw_kernel(ids, place, owners, dgate, dup, w1, w3):
    d_model, f_cols = w1.shape
    half = TOKENS // 2

    def body(t, dg_ref, du_ref, w1_ref, w3_ref, *outs):
        dw = dot_nt(dg_ref[...], w1_ref[...]) + dot_nt(du_ref[...], w3_ref[...])
        for i, out in enumerate(outs):
            out[...] = dw[i * half:(i + 1) * half]

    row_spec = pl.BlockSpec((2 * TOKENS, f_cols), lambda j, t: (place, 0))
    w_spec = pl.BlockSpec((BLK, f_cols), lambda j, t: (j, 0))

    def out_spec(k):
        return pl.BlockSpec((half, BLK), lambda j, t: (0, (j & 4) | ((j & 3) ^ k)))

    return call(body, ids, (dgate, dup, w1, w3), 8, [row_spec, row_spec, w_spec, w_spec],
                [out_spec(k) for k in owners for _ in range(2)], [sds((half, d_model), F32)] * 4, gflop=17, mbytes=35)


def ffn_y_kernel(ids, place, mixed, w2):
    f_cols, d_model = w2.shape
    half = TOKENS // 2
    tile = 256

    def body(t, m_ref, w2_ref, *outs):
        y = dot(m_ref[...], w2_ref[...])
        for i, out in enumerate(outs):
            out[...] = y[i * half:(i + 1) * half]

    out_spec = pl.BlockSpec((half, tile), lambda j, t: (0, j))
    return call(body, ids, (mixed, w2), d_model // tile, [pl.BlockSpec((2 * TOKENS, f_cols), lambda j, t: (place, 0)), pl.BlockSpec((f_cols, tile), lambda j, t: (0, j))],
                [out_spec] * 4, [sds((half, d_model), F32)] * 4, gflop=8.6, mbytes=20)


def weight_grad_kernel(ids, left, right, first_block, received, parts):
    rows, cols = right.shape
    n_out = 4 * max(parts, 1)
    sub = BLK // max(parts, 1)
    tile = 512

    def body(t, l_ref, r_ref, *refs):
        j = pl.program_id(0)
        total, sem = refs[-2:]
        outs = refs[-2 - (n_out if parts else 1):-2]
        slot = j & 1

        def copies(r, slot):
            if not parts:
                return [pltpu.make_async_copy(total.at[slot], outs[0].at[pl.ds(pl.multiple_of(r * BLK, BLK), BLK), :], sem.at[slot, 0])]
            return [pltpu.make_async_copy(total.at[slot, pl.ds(i * sub, sub), :], outs[r * parts + i], sem.at[slot, i]) for i in range(parts)]

        @pl.when(j >= 2)
        def _():
            for copy in copies(0, slot):
                copy.wait()

        def tile_step(n, carry):
            here = lane_block(n, tile)
            part = dot_tn(l_ref[...], r_ref[:, here])
            if received is not None:
                part = part + refs[0][:, here]
            total[slot, :, here] = part
            return carry

        lax.fori_loop(0, cols // tile, tile_step, 0)
        if parts:
            for r in range(4):
                @pl.when(j == r)
                def _():
                    for copy in copies(r, slot):
                        copy.start()
        else:
            for copy in copies(j, slot):
                copy.start()

        @pl.when(j == 3)
        def _():
            for last in (1 - slot, slot):
                for copy in copies(0, last):
                    copy.wait()

    in_specs = [pl.BlockSpec((rows, BLK), lambda j, t: (0, first_block(t) + j)), whole((rows, cols))]
    args = (left, right)
    if received is not None:
        in_specs.append(pl.BlockSpec((BLK, cols), lambda j, t: (j, 0)))
        args += (received,)
    out_shape = [sds((sub, cols), F32)] * n_out if parts else [sds((4 * BLK, cols), F32)]
    return call(body, ids, args, 4, in_specs, [pl.BlockSpec(memory_space=pl.ANY)] * len(out_shape), out_shape,
                [pltpu.VMEM((2, BLK, cols), F32), pltpu.SemaphoreType.DMA((2, max(parts, 1)))], gflop=2e-9 * rows * cols * 4 * BLK, mbytes=25)


def add_kernel(ids, a, b):
    rows, cols = a.shape

    def body(t, a_ref, b_ref, o_ref):
        o_ref[...] = a_ref[...] + b_ref[...]

    spec = pl.BlockSpec((rows // 4, cols), lambda j, t: (j, 0))
    return call(body, ids, (a, b), 4, [spec, spec], spec, sds((rows, cols), a.dtype), gflop=1, mbytes=6)


def sum_kernel(ids, top, bottom, widths, base=None):
    rows, cols = top[0].shape
    tile = rows // 2
    n_in = 6 if base is None else 7
    dtype = F32 if base is None else base.dtype

    def body(t, *refs):
        j = pl.program_id(0)
        for side in range(2):
            @pl.when(j // 2 == side)
            def _():
                a, b, c = refs[3 * side:3 * side + 3]
                start = 0
                for width, out in zip(widths, refs[n_in:]):
                    cut = slice(start, start + width)
                    total = a[:, cut] + b[:, cut] + c[:, cut]
                    if base is not None:
                        total = refs[6][...].astype(F32) + total
                    out[...] = total.astype(dtype)
                    start += width

    top_spec = pl.BlockSpec((tile, cols), lambda j, t: (jnp.minimum(j, 1), 0))
    bottom_spec = pl.BlockSpec((tile, cols), lambda j, t: (jnp.maximum(j - 2, 0), 0))
    args = tuple(top) + tuple(bottom) + ((base,) if base is not None else ())
    base_specs = [pl.BlockSpec((tile, cols), lambda j, t: (j, 0))] * (n_in - 6)
    return call(body, ids, args, 4, [top_spec] * 3 + [bottom_spec] * 3 + base_specs,
                [pl.BlockSpec((tile, w), lambda j, t: (j, 0)) for w in widths], [sds((2 * rows, w), dtype) for w in widths], gflop=2, mbytes=20)


def move_kernel(ids, moves, sources, out_shapes):
    n_src, n_out, n = len(sources), len(out_shapes), len(moves)

    def body(t, *refs):
        srcs, outs = refs[:n_src], refs[n_src:n_src + n_out]
        bufs = refs[n_src + n_out:n_src + n_out + n]
        in_sem, out_sem = refs[n_src + n_out + n:]
        loads, stores = [], []
        for i, (src, src_at, out, out_at, _) in enumerate(moves):
            loads.append(pltpu.make_async_copy(srcs[src].at[src_at(t)], bufs[i], in_sem.at[i]))
            stores.append(pltpu.make_async_copy(bufs[i], outs[out].at[out_at(t)], out_sem.at[i]))
        for load in loads:
            load.start()
        for load, store in zip(loads, stores):
            load.wait()
            store.start()
        for store in stores:
            store.wait()

    shapes = [pltpu.VMEM(shape, sources[src].dtype) for src, _, _, _, shape in moves]
    any_spec = pl.BlockSpec(memory_space=pl.ANY)
    return call(body, ids, tuple(sources), 1, [any_spec] * n_src, [any_spec] * n_out, list(out_shapes),
                shapes + [pltpu.SemaphoreType.DMA((n,))] * 2, gflop=2, mbytes=17)


def everything(t):
    return slice(None), slice(None)


def row_at(start, size):
    return lambda t: (slice(start, start + size), slice(None))


def norm_back(t, grad_ref, rows, src_ref, gain_ref, base_ref, out_ref, gain_out_ref):
    src = src_ref[rows, :].astype(F32)
    scale = lax.rsqrt(jnp.mean(src * src, axis=-1, keepdims=True) + EPS)
    inner = jnp.zeros_like(scale)
    for p in range(8):
        cols = slice(p * BLK, (p + 1) * BLK)
        unit = src_ref[rows, lane_block(t[p])].astype(F32) * scale
        grad = grad_ref[rows, cols].astype(F32)
        gain_out_ref[:, cols] += jnp.sum(grad * unit, axis=0, keepdims=True)
        inner += jnp.sum(grad * gain_ref[:, cols] * unit, axis=-1, keepdims=True)
    inner = inner * (1.0 / src.shape[1])
    for p in range(8):
        cols = slice(p * BLK, (p + 1) * BLK)
        place = lane_block(t[p])
        unit = src_ref[rows, place].astype(F32) * scale
        grad_rows = scale * (grad_ref[rows, cols].astype(F32) * gain_ref[:, cols] - unit * inner)
        out_ref[rows, place] = (base_ref[rows, place].astype(F32) + grad_rows).astype(BF16)


def hidden_grad_kernel(ids, parts_a, parts_b, hidden, gain_rel, dy):
    rows, d_model = hidden.shape
    half = rows // 2
    tile = 64
    n_half = half // tile

    def body(t, a0, a1, a2, b0, b1, b2, h_ref, g_ref, dy_ref, out_ref, gain_ref, grad):
        j = pl.program_id(0)

        @pl.when(j == 0)
        def _():
            gain_ref[...] = jnp.zeros_like(gain_ref)

        @pl.when(j < n_half)
        def _():
            grad[...] = (a0[...] + a1[...] + a2[...]).astype(BF16)

        @pl.when(j >= n_half)
        def _():
            grad[...] = (b0[...] + b1[...] + b2[...]).astype(BF16)

        norm_back(t, grad, slice(None), h_ref, g_ref, dy_ref, out_ref, gain_ref)

    a_spec = pl.BlockSpec((tile, d_model), lambda j, t: (jnp.minimum(j, n_half - 1), 0))
    b_spec = pl.BlockSpec((tile, d_model), lambda j, t: (jnp.maximum(j - n_half, 0), 0))
    row_spec = pl.BlockSpec((tile, d_model), lambda j, t: (j, 0))
    return call(body, ids, tuple(parts_a) + tuple(parts_b) + (hidden, gain_rel, dy), rows // tile,
                [a_spec] * 3 + [b_spec] * 3 + [row_spec, whole((1, d_model)), row_spec],
                [row_spec, whole((1, d_model))], [sds((rows, d_model), BF16), sds((1, d_model), F32)],
                [pltpu.VMEM((tile, d_model), BF16)], gflop=5, mbytes=20)


def attn_grad_kernel(ids, grad_hidden, w_full):
    rows, d_model = grad_hidden.shape

    def block_row(j, t):
        half = t[SP] ^ (j < 2).astype(jnp.int32)
        return (half * 2 + (j & 1)) ^ t[DP]

    def body(t, g_ref, wm_ref, wo_ref, far_ref, keep_ref):
        j = pl.program_id(0)
        grads = [dot_nt(g_ref[...], ref[...]).astype(BF16) for ref in (wm_ref, wo_ref)]
        for cond, ref in ((j < 2, far_ref), (j >= 2, keep_ref)):
            @pl.when(cond)
            def _():
                for s in range(2):
                    for e in range(2):
                        ref[(t[SP] ^ s) * 2 + e] = grads[s][:, 128 * e:128 * e + 128]

    return call(body, ids, (grad_hidden, w_full, w_full), 4,
                [whole((rows, d_model)), pl.BlockSpec((BLK, d_model), lambda j, t: (block_row(j, t), 0)), pl.BlockSpec((BLK, d_model), lambda j, t: (4 + block_row(j, t), 0))],
                [pl.BlockSpec((4, rows, 128), lambda j, t: (jnp.minimum(j, 1), 0, 0)), pl.BlockSpec((4, rows, 128), lambda j, t: (jnp.maximum(j - 2, 0), 0, 0))],
                [sds((8, rows, 128), BF16)] * 2, gflop=4.3, mbytes=14)


def unrope_kernel(ids, keep, got, cos_t, sin_t):
    rows = keep.shape[1]
    tile = 128

    def body(t, k_ref, g_ref, cos_ref, sin_ref, o_ref):
        for ref, half in ((k_ref, t[SP]), (g_ref, 1 - t[SP])):
            for p in range(12):
                pair = ref[p]
                if p < 10:
                    pair = rope_lanes(pair.astype(F32), cos_ref[...], sin_ref[...], -1).astype(BF16)
                if p < 8:
                    place = half * 8 + p
                elif p < 10:
                    place = 16 + half * 2 + (p - 8)
                else:
                    place = 20 + half * 2 + (p - 10)
                o_ref[:, lane_block(place, 128)] = pair

    h_spec = pl.BlockSpec((12, tile, 128), lambda j, t: (0, j, 0))
    t_spec = pl.BlockSpec((tile, 128), lambda j, t: (j, 0))
    return call(body, ids, (keep, got, cos_t, sin_t), rows // tile, [h_spec, h_spec, t_spec, t_spec],
                pl.BlockSpec((tile, 3072), lambda j, t: (j, 0)), sds((rows, 3072), BF16), gflop=3, mbytes=10)


def input_grad_kernel(ids, grad_qkv, w_full, act, gain_rel, grad_hidden):
    rows, d_model = act.shape
    cols = grad_qkv.shape[1]

    def body(t, g_ref, w_ref, x_ref, gain_ref, gh_ref, out_ref, gain_out_ref, grad):
        j = pl.program_id(0)
        grad[:, lane_block(j)] = dot_nt(g_ref[...], w_ref[...]).astype(BF16)

        @pl.when(j == 7)
        def _():
            gain_out_ref[...] = jnp.zeros_like(gain_out_ref)

            def step(i, carry):
                norm_back(t, grad, pl.ds(pl.multiple_of(i * 64, 64), 64), x_ref, gain_ref, gh_ref, out_ref, gain_out_ref)
                return carry

            lax.fori_loop(0, rows // 64, step, 0)

    return call(body, ids, (grad_qkv, w_full, act, gain_rel, grad_hidden), 8,
                [whole((rows, cols)), pl.BlockSpec((BLK, cols), lambda j, t: (j, 0)), whole((rows, d_model)), whole((1, d_model)), whole((rows, d_model))],
                [whole((rows, d_model)), whole((1, d_model))], [sds((rows, d_model), BF16), sds((1, d_model), F32)],
                [pltpu.VMEM((rows, d_model), BF16)], gflop=10, mbytes=20)


def solution(mesh):
    flat_axes = ("dp", "sp")
    row_spec = P("dp", "sp", None)
    pos_spec = P("dp", "sp")
    vec_spec = P(flat_axes)
    mat_spec = P(flat_axes, None)
    cube_spec = P(flat_axes, None, None)
    pair_lists = {"x": ("dp", [(i, i ^ 1) for i in range(4)]), "y": ("dp", [(i, i ^ 2) for i in range(4)]), "d": ("dp", [(i, i ^ 3) for i in range(4)]), "s": ("sp", [(0, 1), (1, 0)])}

    def send(way, v):
        axis, pairs = pair_lists[way]
        return lax.ppermute(v, axis, pairs)

    def gather_pieces(own, *deps):
        half = own.shape[0] // 2
        from_x = send("x", own)
        from_y = send("y", own)
        if deps:
            from_x, from_y = after((from_x, from_y), *deps)
        return [own, from_x, from_y, send("y", from_x[:half]), send("x", from_y[half:])]

    def both_cores(pieces):
        return pieces + [send("s", p) for p in pieces]

    def gather_rows(top, bottom):
        xa = send("x", top)
        yb = send("y", bottom)
        xb = send("x", bottom)
        ya = send("y", top)
        return [top, bottom], [xa, xb], [ya, yb], [send("y", xa), send("x", yb)]

    def scatter4(ids, halves):
        (a0, b0), (a1, b1), (a2, b2), (a3, b3) = halves
        u1 = send("x", a1)
        u2 = send("y", b2)
        t1 = send("x", a3)
        t2 = send("y", b3)
        v1 = send("x", add_kernel(ids, b1, t2))
        v2 = send("y", add_kernel(ids, a2, t1))
        return (a0, u1, v2), (b0, v1, u2)

    def layer(act_in, positions, out_grad, norm1_gain, norm2_gain, w_query, w_key, w_value, w_out, w_gate, w_up, w_down):
        dp = lax.axis_index("dp")
        sp = lax.axis_index("sp")
        n_q, n_kv, hd = w_query.shape[1], w_key.shape[1], w_query.shape[2]
        q_cols, kv_cols = n_q * hd, n_kv * hd
        n_tok, d_model = act_in.shape[1:]
        half_d = d_model // 2
        half_t = n_tok // 2
        f_cols = w_gate.shape[1]
        quarter = f_cols // 4
        place = jnp.arange(8, dtype=jnp.int32)
        rel_table = ((place & 3) ^ dp) * 2 + ((place >> 2) ^ sp)
        abs_table = ((place & 1) ^ sp) * 4 + ((place >> 1) ^ dp)
        ids = jnp.concatenate([rel_table, abs_table, jnp.stack([sp, dp])]).astype(jnp.int32)

        act = act_in[0]
        dy = out_grad[0]
        pos = positions[0]

        wo_pieces = both_cores(gather_pieces(w_out))
        w_qkv = jnp.concatenate([w_query.reshape(BLK, q_cols), w_key.reshape(BLK, kv_cols), w_value.reshape(BLK, kv_cols)], axis=1)
        gains = jnp.stack([norm1_gain, norm2_gain])
        gain_mine = jnp.concatenate([gains, send("x", gains), send("y", gains), send("d", gains)], axis=1)
        gain_rel = jnp.concatenate([gain_mine, send("s", gain_mine)], axis=1).astype(F32)
        gain1_rel, gain2_rel = gain_rel[0:1], gain_rel[1:2]

        w2_rows = w_down.shape[0]

        def w2_at(side):
            return lambda t: (pl.ds(pl.multiple_of((t[SP] ^ side) * w2_rows, w2_rows), w2_rows), slice(None))

        w2_pair = [w_down, send("s", w_down)]
        (w2,) = move_kernel(ids, [(i, everything, 0, w2_at(i), w_down.shape) for i in range(2)], w2_pair, [sds((2 * w2_rows, d_model), BF16)])

        inv_freq = ROPE_BASE ** (-(jnp.arange(hd // 2, dtype=F32) * (2.0 / hd)))
        angles = pos.astype(F32)[:, None] * inv_freq
        cos_t = jnp.tile(jnp.cos(angles), (1, 4))
        sin_t = jnp.tile(jnp.sin(angles), (1, 4))
        u_rel = norm_kernel(ids, after(act, cos_t, sin_t), gain1_rel)
        qkv_pieces = both_cores(gather_pieces(w_qkv, u_rel, w2))

        def quarter_at(r):
            return lambda t: (slice(None), pl.ds(pl.multiple_of((t[DP] ^ r) * quarter, quarter), quarter))

        moves = [(i, quarter_at(r), r, row_at(i * BLK, BLK), (BLK, quarter)) for r in (1, 2, 3, 0) for i in range(2)]
        q0, q1, q2, q3 = move_kernel(ids, moves, [w_gate, w_up], [sds((2 * BLK, quarter), BF16)] * 4)
        f_pieces = both_cores([q0, send("x", q1), send("y", q2), send("d", q3)])
        moves = [(i, row_at(o * BLK, BLK), o, row_at(i * BLK, BLK), (BLK, quarter)) for i in range(8) for o in range(2)]
        w1, w3 = move_kernel(ids, moves, f_pieces, [sds((d_model, quarter), BF16)] * 2)

        qkv_far, qkv_keep, wqkv_full = qkv_kernel(ids, u_rel, qkv_pieces, cos_t, sin_t)
        qkv_got = send("s", qkv_far)
        o_keep, o_far = attn_fwd_kernel(ids, qkv_keep, qkv_got)
        o_got = send("s", o_far)
        attn_rel, hidden, normed_a, normed_b, wo_full = out_proj_kernel(ids, o_keep, o_got, wo_pieces, act, gain2_rel)

        w_rows = gather_rows(normed_a, normed_b)
        dy_rows = gather_rows(dy[:half_t], dy[half_t:])
        fwd = ffn_fwd_kernel(ids, 0, [(0, w_rows[0])], w1, w3, None)
        fwd = ffn_fwd_kernel(ids, 1, [(1, w_rows[1]), (2, w_rows[2])], w1, w3, fwd)
        y1 = ffn_y_kernel(ids, 1, fwd[1], w2)
        bwd = ffn_bwd_kernel(ids, 1, dy_rows[1] + dy_rows[2], fwd[2], fwd[3], w2, None)
        dw1 = ffn_dw_kernel(ids, 1, (1, 2), bwd[1], bwd[2], w1, w3)
        w_all, mixed, gate_pre, up_pre = ffn_fwd_kernel(ids, 1, [(3, w_rows[3])], w1, w3, fwd)
        dy_all, dgate, dup = ffn_bwd_kernel(ids, 0, [dy] + dy_rows[3], gate_pre, up_pre, w2, bwd)
        dw0 = ffn_dw_kernel(ids, 0, (0, 3), dgate, dup, w1, w3)
        y0 = ffn_y_kernel(ids, 0, mixed, w2)
        parts_a, parts_b = scatter4(ids, [dw0[:2], dw1[:2], dw1[2:], dw0[2:]])
        y_a, y_b = scatter4(ids, [y0[:2], y1[:2], y1[2:], y0[2:]])
        (act_out,) = sum_kernel(ids, y_a, y_b, (d_model,), hidden)

        def column_grad(grad_all):
            (far,) = weight_grad_kernel(ids, w_all, grad_all, lambda t: 4, None, 0)
            parts = weight_grad_kernel(ids, w_all, grad_all, lambda t: 0, send("s", far), 1)
            return [parts[0], send("x", parts[1]), send("y", parts[2]), send("d", parts[3])]

        def placed(pieces):
            return move_kernel(ids, [(r, everything, 0, quarter_at(r), (BLK, quarter)) for r in range(4)], pieces, [sds((BLK, f_cols), F32)])[0]

        gate_pieces = column_grad(dgate)
        up_pieces = column_grad(dup)
        (down_far,) = weight_grad_kernel(ids, mixed, dy_all, lambda t: (1 - t[SP]) * 4, None, 0)
        (down_grad,) = weight_grad_kernel(ids, mixed, dy_all, lambda t: t[SP] * 4, send("s", down_far), 0)
        gate_grad = placed(gate_pieces)
        up_grad = placed(up_pieces)

        grad_hidden, gain2_part = hidden_grad_kernel(ids, parts_a, parts_b, hidden, gain2_rel, dy)

        def row_grad(left, right):
            (far,) = weight_grad_kernel(ids, left, right, lambda t: 4, None, 0)
            parts = weight_grad_kernel(ids, left, right, lambda t: 0, send("s", far), 2)
            return scatter4(ids, [(parts[2 * r], parts[2 * r + 1]) for r in range(4)])

        do_far, do_keep = attn_grad_kernel(ids, grad_hidden, wo_full)
        do_got = send("s", do_far)
        d_keep, d_far = attn_bwd_kernel(ids, qkv_keep, qkv_got, do_keep, do_got)
        d_got = send("s", d_far)
        wo_a, wo_b = row_grad(attn_rel, grad_hidden)
        grad_qkv = unrope_kernel(ids, d_keep, d_got, cos_t, sin_t)
        qkv_a, qkv_b = row_grad(u_rel, grad_qkv)
        q_grad, k_grad, v_grad = sum_kernel(ids, qkv_a, qkv_b, (q_cols, kv_cols, kv_cols))
        query_grad = q_grad.reshape(w_query.shape)
        key_grad = k_grad.reshape(w_key.shape)
        value_grad = v_grad.reshape(w_value.shape)
        wo_a = (after(wo_a[0], query_grad, key_grad, value_grad),) + wo_a[1:]
        (wout_grad,) = sum_kernel(ids, wo_a, wo_b, (d_model,))
        in_grad, gain1_part = input_grad_kernel(ids, grad_qkv, wqkv_full, act, gain1_rel, grad_hidden)

        gain_part = jnp.concatenate([gain1_part, gain2_part], axis=0)
        gain_half = gain_part[:, :half_d] + send("s", gain_part[:, half_d:])
        gp = [gain_half[:, r * BLK:(r + 1) * BLK] for r in range(4)]
        gain_grad = gp[0] + send("x", gp[1]) + send("y", gp[2]) + send("d", gp[3])
        return (act_out[None], in_grad[None], gain_grad[0], gain_grad[1], query_grad, key_grad, value_grad, wout_grad, gate_grad, up_grad, down_grad)

    return jax.shard_map(layer, mesh=mesh, in_specs=(row_spec, pos_spec, row_spec, vec_spec, vec_spec, cube_spec, cube_spec, cube_spec, mat_spec, mat_spec, mat_spec, mat_spec), out_specs=(row_spec, row_spec, vec_spec, vec_spec, cube_spec, cube_spec, cube_spec, mat_spec, mat_spec, mat_spec, mat_spec), check_vma=False)
```

```python
import jax
import jax.numpy as jnp
from jax import lax
from jax.experimental import pallas as pl
from jax.experimental.pallas import tpu as pltpu
from jax.sharding import PartitionSpec as P

INTERPRET = False

EPS = 1e-5
ROPE_BASE = 10000.0
NEG_BIG = -1e30
F32 = jnp.float32
BF16 = jnp.bfloat16
CHIPS = 4
PLACES = 8
BLK = 256
HALF_BLK = BLK // 2
TOKENS = 512
HALF_TOKENS = TOKENS // 2
HEAD = 64
HALF_HEAD = HEAD // 2
PAIR = 2 * HEAD
ATTN_SCALE = HEAD ** -0.5
GROUPS = 4
GROUP_HEADS = 4
Q_PAIRS = 8
KV_PAIRS = 2
K_SLAB = Q_PAIRS
V_SLAB = K_SLAB + KV_PAIRS
SLABS = V_SLAB + KV_PAIRS
ALL = slice(None)
MANY = pltpu.SemaphoreType.DMA


def dot(a, b):
    return lax.dot_general(a, b, (((1,), (0,)), ((), ())), preferred_element_type=F32)


def dot_nt(a, b):
    return lax.dot_general(a, b, (((1,), (1,)), ((), ())), preferred_element_type=F32)


def dot_tn(a, b):
    return lax.dot_general(a, b, (((0,), (0,)), ((), ())), preferred_element_type=F32)


def after(value, *deps):
    first, *_ = lax.optimization_barrier((value,) + deps)
    return first


def sds(shape, dtype):
    return jax.ShapeDtypeStruct(shape, dtype)


def like(v):
    return sds(v.shape, v.dtype)


def fixed(j, t):
    return 0


def moving(j, t):
    return j


def until(n):
    return lambda j, t: jnp.minimum(j, n - 1)


def since(n):
    return lambda j, t: jnp.maximum(j - n, 0)


def always(n):
    return lambda j, t: n


def spec(shape, *index):
    return pl.BlockSpec(shape, lambda j, t: tuple(f(j, t) for f in index))


def whole(v):
    return spec(v.shape, *[fixed] * len(v.shape))


def anywhere(n):
    return [pl.BlockSpec(memory_space=pl.ANY)] * n


def call(body, ids, args, grid, in_specs, out_specs, out_shape, scratch=(), gflop=1.0, aliases=None):
    return pl.pallas_call(
        body,
        out_shape=out_shape,
        grid_spec=pltpu.PrefetchScalarGridSpec(num_scalar_prefetch=1, grid=(grid,), in_specs=in_specs, out_specs=out_specs, scratch_shapes=list(scratch)),
        cost_estimate=pl.CostEstimate(flops=int(gflop * 1e9), bytes_accessed=int(1e7), transcendentals=0),
        compiler_params=pltpu.CompilerParams(dimension_semantics=("arbitrary",)),
        input_output_aliases=aliases or {},
        interpret=INTERPRET,
    )(ids, *args)


def step_id():
    return pl.program_id(0)


def loop(count, body):
    def one(i, carry):
        body(i)
        return carry

    lax.fori_loop(0, count, one, 0)


SP = 2 * PLACES
DP = SP + 1


def part(index, size):
    return pl.ds(pl.multiple_of(index * size, size), size)


def cols_of(p):
    return slice(p * BLK, (p + 1) * BLK)


def row_sum(v):
    return jnp.sum(v, axis=-1, keepdims=True)


def row_scale(x):
    return lax.rsqrt(row_sum(x * x) * (1.0 / x.shape[-1]) + EPS)


def write_normed(t, src, rows, gain, out, out_rows):
    scale = row_scale(src[rows, :].astype(F32))
    for p in range(PLACES):
        blk = src[rows, part(t[p], BLK)].astype(F32)
        out[out_rows, cols_of(p)] = (blk * scale * gain[:, cols_of(p)]).astype(BF16)


def norm_kernel(ids, act, gain_rel):
    rows, cols = act.shape
    tile = HALF_BLK

    def body(t, x_ref, g_ref, o_ref):
        write_normed(t, x_ref, ALL, g_ref, o_ref, ALL)

    io = spec((tile, cols), moving, fixed)
    return call(body, ids, (act, gain_rel), rows // tile, [io, whole(gain_rel)], io, like(act))


def rope_lanes(values, cos_t, sin_t, sign):
    width = values.shape[-1]
    reps = width // PAIR
    if reps > 1:
        cos_t = jnp.concatenate([cos_t] * reps, axis=1)
        sin_t = jnp.concatenate([sin_t] * reps, axis=1)
    lane = lax.broadcasted_iota(jnp.int32, values.shape, 1)
    up_roll = pltpu.roll(values, width - HALF_HEAD, 1)
    down_roll = pltpu.roll(values, HALF_HEAD, 1)
    other = jnp.where((lane & (HEAD - 1)) < HALF_HEAD, -up_roll, down_roll)
    return values * cos_t + (other * sin_t if sign > 0 else -(other * sin_t))


def fill(scratch, refs):
    start = 0
    for ref in refs:
        n, _ = ref.shape
        scratch[start:start + n, :] = ref[:]
        start += n


def qkv_kernel(ids, u_rel, pieces, cos_t, sin_t):
    rows, d_model = u_rel.shape
    cols = pieces[0].shape[1]
    n_pieces = len(pieces)
    tiles = SLABS // 2
    q_tiles = Q_PAIRS // 2

    def column(j, t):
        far = (j < tiles).astype(jnp.int32)
        half = t[SP] ^ far
        tile = j - tiles * (1 - far)
        return jnp.where(tile < q_tiles, half * q_tiles + tile, 2 * tile + half)

    def body(t, u_ref, cos_ref, sin_ref, *refs):
        far_ref, keep_ref, w_ref = refs[n_pieces:]
        j = step_id()
        fill(w_ref, refs[:n_pieces])
        acc = dot(u_ref[:], w_ref[:])
        roped = rope_lanes(acc, cos_ref[:], sin_ref[:], 1)
        is_value = (j == tiles - 1) | (j == 2 * tiles - 1)
        out = jnp.where(is_value, acc, roped).astype(BF16)
        for cond, ref in ((j < tiles, far_ref), (j >= tiles, keep_ref)):
            @pl.when(cond)
            def _():
                for e in range(2):
                    ref[e] = out[:, e * PAIR:(e + 1) * PAIR]

    w_specs = [spec((p.shape[0], BLK), fixed, column) for p in pieces]
    slab = (2, rows, PAIR)
    return call(body, ids, (u_rel, cos_t, sin_t) + tuple(pieces), 2 * tiles,
                [whole(u_rel), whole(cos_t), whole(sin_t)] + w_specs,
                [spec(slab, until(tiles), fixed, fixed), spec(slab, since(tiles), fixed, fixed), spec((d_model, BLK), fixed, column)],
                [sds((SLABS, rows, PAIR), BF16)] * 2 + [sds((d_model, cols), BF16)], gflop=6.5)


def core_rows(t, rows):
    return part(t[SP], rows), part(1 - t[SP], rows)


def in_order(t, ref, own, other):
    for here, v in zip(core_rows(t, own.shape[0]), (own, other)):
        ref[here, :] = v


def one_head(pair, odd):
    return jnp.where(odd == 1, pair[:, HEAD:], pair[:, :HEAD])


def softmax_rows(q_tile, keys, first_row, span):
    scores = dot_nt(q_tile, keys) * ATTN_SCALE
    edge = span - BLK
    shape = (q_tile.shape[0], BLK)
    row = lax.broadcasted_iota(jnp.int32, shape, 0) + first_row
    col = lax.broadcasted_iota(jnp.int32, shape, 1)
    last = jnp.where(row >= col, scores[:, edge:], NEG_BIG)
    scores = jnp.concatenate([scores[:, :edge], last], axis=1) if edge else last
    expo = jnp.exp(scores - jnp.max(scores, axis=-1, keepdims=True))
    return expo * (1.0 / row_sum(expo))


def head_specs(rows):
    slabs = (2, rows, PAIR)
    one = (1, rows, PAIR)
    q_spec = spec(slabs, moving, fixed, fixed)
    return q_spec, [q_spec] + [spec(one, lambda j, t, base=base: base + j // 2, fixed, fixed) for base in (K_SLAB, V_SLAB)]


def attn_fwd_kernel(ids, keep, got):
    _, rows, _ = keep.shape
    seq = 2 * rows

    def body(t, qk_ref, kk_ref, vk_ref, qg_ref, kg_ref, vg_ref, keep_ref, send_ref, ks, vs, qs, os):
        odd = step_id() & 1
        in_order(t, ks, one_head(kk_ref[0], odd), one_head(kg_ref[0], odd))
        in_order(t, vs, one_head(vk_ref[0], odd), one_head(vg_ref[0], odd))

        def head(h):
            in_order(t, qs, one_head(qk_ref[h // 2], h & 1), one_head(qg_ref[h // 2], h & 1))
            for span in range(BLK, seq + BLK, BLK):
                prob = softmax_rows(qs[span - BLK:span, :], ks[:span, :], 0, span).astype(BF16)
                os[h, span - BLK:span, :] = dot(prob, vs[:span, :]).astype(BF16)

        loop(GROUP_HEADS, head)
        for here, ref in zip(core_rows(t, rows), (keep_ref, send_ref)):
            for p in range(2):
                ref[p] = jnp.concatenate([os[2 * p, here, :], os[2 * p + 1, here, :]], axis=1)

    q_spec, specs = head_specs(rows)
    return call(body, ids, (keep,) * 3 + (got,) * 3, GROUPS, specs * 2,
                [q_spec] * 2, [sds((Q_PAIRS, rows, PAIR), BF16)] * 2,
                [pltpu.VMEM((seq, HEAD), BF16)] * 3 + [pltpu.VMEM((GROUP_HEADS, seq, HEAD), BF16)], gflop=20)


def attn_bwd_kernel(ids, keep, got, do_keep, do_got):
    _, rows, _ = keep.shape
    seq = 2 * rows
    strip_rows = HALF_BLK

    def body(t, qk_ref, kk_ref, vk_ref, dk_ref, qg_ref, kg_ref, vg_ref, dg_ref, keep_ref, send_ref, ks, vs, qs, ds, dqs, dks, dvs):
        g = step_id()
        odd = g & 1
        in_order(t, ks, one_head(kk_ref[0], odd), one_head(kg_ref[0], odd))
        in_order(t, vs, one_head(vk_ref[0], odd), one_head(vg_ref[0], odd))
        dks[odd] = jnp.zeros_like(ks, F32)
        dvs[odd] = jnp.zeros_like(vs, F32)

        def head(h):
            in_order(t, qs, one_head(qk_ref[h // 2], h & 1), one_head(qg_ref[h // 2], h & 1))
            in_order(t, ds, one_head(dk_ref[h // 2], h & 1), one_head(dg_ref[h // 2], h & 1))
            for span in range(BLK, seq + BLK, BLK):
                def strip(n):
                    here = part((span - BLK) // strip_rows + n, strip_rows)
                    q_tile = qs[here, :]
                    do_tile = ds[here, :]
                    prob = softmax_rows(q_tile, ks[:span, :], n * strip_rows, span)
                    grad_prob = dot_nt(do_tile, vs[:span, :])
                    inner = row_sum(prob * grad_prob)
                    grad_scores = (prob * (grad_prob - inner) * ATTN_SCALE).astype(BF16)
                    dqs[h, here, :] = dot(grad_scores, ks[:span, :]).astype(BF16)
                    dks[odd, :span, :] += dot_tn(grad_scores, q_tile)
                    dvs[odd, :span, :] += dot_tn(prob.astype(BF16), do_tile)

                loop(BLK // strip_rows, strip)

        loop(GROUP_HEADS, head)
        for here, ref in zip(core_rows(t, rows), (keep_ref, send_ref)):
            for p in range(2):
                ref[2 * g + p] = jnp.concatenate([dqs[2 * p, here, :], dqs[2 * p + 1, here, :]], axis=1)

            @pl.when(odd == 1)
            def _():
                for base, acc in ((K_SLAB, dks), (V_SLAB, dvs)):
                    ref[base + g // 2] = jnp.concatenate([acc[0, here, :], acc[1, here, :]], axis=1).astype(BF16)

    q_spec, specs = head_specs(rows)
    return call(body, ids, (keep,) * 3 + (do_keep,) + (got,) * 3 + (do_got,), GROUPS, (specs + [q_spec]) * 2,
                [whole(keep)] * 2, [like(keep)] * 2,
                [pltpu.VMEM((seq, HEAD), BF16)] * 4 + [pltpu.VMEM((GROUP_HEADS, seq, HEAD), BF16)] + [pltpu.VMEM((2, seq, HEAD), F32)] * 2, gflop=50)


def out_proj_kernel(ids, o_keep, o_got, pieces, act, gain_rel):
    rows, d_model = act.shape
    tile = BLK
    strip_rows = HEAD
    n_pieces = len(pieces)

    def body(t, ok_ref, og_ref, x_ref, g_ref, *refs):
        a_ref, h_ref, wa_ref, wb_ref, w_ref, a_abs = refs[n_pieces:]
        j = step_id()

        @pl.when(j == 0)
        def _():
            for ref, side in ((ok_ref, t[SP]), (og_ref, 1 - t[SP])):
                for p in range(Q_PAIRS):
                    a_abs[:, part(side * Q_PAIRS + p, PAIR)] = ref[p]
            for p in range(PLACES):
                a_ref[:, cols_of(p)] = a_abs[:, part(t[p], BLK)]

        fill(w_ref, refs[:n_pieces])
        acc = dot(a_ref[:], w_ref[:])
        cols = part(j, tile)
        h_ref[:, cols] = (x_ref[:, cols].astype(F32) + acc).astype(BF16)

        @pl.when(j == d_model // tile - 1)
        def _():
            strips = HALF_TOKENS // strip_rows
            for side, out_ref in enumerate((wa_ref, wb_ref)):
                loop(strips, lambda i: write_normed(t, h_ref, part(side * strips + i, strip_rows), g_ref, out_ref, part(i, strip_rows)))

    w_specs = [spec((p.shape[0], tile), fixed, moving) for p in pieces]
    half = sds((HALF_TOKENS, d_model), BF16)
    return call(body, ids, (o_keep, o_got, act, gain_rel) + tuple(pieces), d_model // tile,
                [whole(o_keep), whole(o_got), whole(act), whole(gain_rel)] + w_specs,
                [whole(act)] * 2 + [whole(half)] * 2 + [spec((d_model, tile), fixed, moving)],
                [like(act)] * 2 + [half] * 2 + [sds((d_model, d_model), BF16)], [pltpu.VMEM((rows, d_model), BF16)], gflop=4.3)


def swapped(place, k):
    return place ^ k


def ffn_fwd_kernel(ids, place, chunks, w1, w3, buffers):
    d_model, f_cols = w1.shape
    tile = BLK
    owners = [k for k, parts in chunks for _ in parts]
    parts = [p for _, parts in chunks for p in parts]
    rows = sum(p.shape[0] for p in parts)
    n_parts = len(parts)
    n_buf = len(buffers)

    def body(t, *refs):
        w1_ref, w3_ref = refs[n_parts:n_parts + 2]
        wall_ref, m_ref, gate_ref, up_ref = refs[n_parts + 2 + n_buf:]

        @pl.when(step_id() == 0)
        def _():
            start = 0
            for k, ref in zip(owners, refs):
                n, _ = ref.shape
                for p in range(PLACES):
                    wall_ref[start:start + n, cols_of(p)] = ref[:, cols_of(swapped(p, k))]
                start += n

        gate = dot(wall_ref[:], w1_ref[:])
        up = dot(wall_ref[:], w3_ref[:])
        gate_ref[:] = gate
        up_ref[:] = up
        m_ref[:] = (gate * jax.nn.sigmoid(gate) * up).astype(BF16)

    w_spec = spec((d_model, tile), fixed, moving)
    tile_spec = spec((rows, tile), always(place), moving)
    total = CHIPS * TOKENS
    return call(body, ids, tuple(parts) + (w1, w3) + tuple(buffers), f_cols // tile, [whole(p) for p in parts] + [w_spec] * 2 + anywhere(n_buf),
                [spec((rows, d_model), always(place), fixed)] + [tile_spec] * 3,
                [sds((total, d_model), BF16), sds((total, f_cols), BF16)] + [sds((total, f_cols), F32)] * 2,
                gflop=8.6, aliases={n_parts + 3 + i: i for i in range(n_buf)})


def ffn_bwd_kernel(ids, place, parts, gate_pre, up_pre, w2, buffers):
    f_cols, d_model = w2.shape
    tile = BLK
    rows = sum(p.shape[0] for p in parts)
    n_parts = len(parts)
    n_buf = len(buffers)

    def body(t, *refs):
        gate_ref, up_ref, w2_ref = refs[n_parts:n_parts + 3]
        dyall_ref, dg_ref, du_ref = refs[n_parts + 3 + n_buf:]

        @pl.when(step_id() == 0)
        def _():
            fill(dyall_ref, refs[:n_parts])

        def strip(n):
            here = part(n, TOKENS)
            back = dot_nt(dyall_ref[here, :], w2_ref[:]).astype(BF16).astype(F32)
            gate = gate_ref[here, :]
            sig = jax.nn.sigmoid(gate)
            du_ref[here, :] = (back * (gate * sig)).astype(BF16)
            dg_ref[here, :] = (back * up_ref[here, :] * sig * (1.0 + gate * (1.0 - sig))).astype(BF16)

        loop(rows // TOKENS, strip)

    tile_spec = spec((rows, tile), always(place), moving)
    total = CHIPS * TOKENS
    return call(body, ids, tuple(parts) + (gate_pre, up_pre, w2) + tuple(buffers), f_cols // tile,
                [whole(p) for p in parts] + [tile_spec] * 2 + [spec((tile, d_model), moving, fixed)] + anywhere(n_buf),
                [spec((rows, d_model), always(place), fixed)] + [tile_spec] * 2,
                [sds((total, d_model), BF16)] + [sds((total, f_cols), BF16)] * 2,
                gflop=8.6, aliases={n_parts + 4 + i: i for i in range(n_buf)})


def write_halves(outs, value):
    for i, out in enumerate(outs):
        out[:] = value[i * HALF_TOKENS:(i + 1) * HALF_TOKENS]


def ffn_dw_kernel(ids, place, owners, dgate, dup, w1, w3):
    d_model, f_cols = w1.shape

    def body(t, dg_ref, du_ref, w1_ref, w3_ref, *outs):
        write_halves(outs, dot_nt(dg_ref[:], w1_ref[:]) + dot_nt(du_ref[:], w3_ref[:]))

    row_spec = spec((2 * TOKENS, f_cols), always(place), fixed)
    w_spec = spec((BLK, f_cols), moving, fixed)
    out_specs = [spec((HALF_TOKENS, BLK), fixed, lambda j, t, k=k: j ^ k) for k in owners for _ in range(2)]
    return call(body, ids, (dgate, dup, w1, w3), d_model // BLK, [row_spec, row_spec, w_spec, w_spec],
                out_specs, [sds((HALF_TOKENS, d_model), F32)] * len(out_specs), gflop=17)


def ffn_y_kernel(ids, place, mixed, w2):
    f_cols, d_model = w2.shape

    def body(t, m_ref, w2_ref, *outs):
        write_halves(outs, dot(m_ref[:], w2_ref[:]))

    return call(body, ids, (mixed, w2), d_model // BLK, [spec((2 * TOKENS, f_cols), always(place), fixed), spec((f_cols, BLK), fixed, moving)],
                [spec((HALF_TOKENS, BLK), fixed, moving)] * 4, [sds((HALF_TOKENS, d_model), F32)] * 4, gflop=8.6)


def weight_grad_kernel(ids, left, right, first_block, received, parts):
    rows, cols = right.shape
    per = max(parts, 1)
    sub = BLK // per
    tile = TOKENS
    out_shape = [sds((sub, cols), F32)] * (CHIPS * parts) if parts else [sds((CHIPS * BLK, cols), F32)]
    n_out = len(out_shape)

    def body(t, l_ref, r_ref, *refs):
        j = step_id()
        *ins, total, sem = refs
        outs = ins[len(ins) - n_out:]
        slot = j & 1

        def copies(r, slot):
            if not parts:
                return [pltpu.make_async_copy(total.at[slot], outs[0].at[part(r, BLK), :], sem.at[slot, 0])]
            return [pltpu.make_async_copy(total.at[slot, pl.ds(i * sub, sub), :], outs[r * parts + i], sem.at[slot, i]) for i in range(parts)]

        def drain(slot):
            for copy in copies(0, slot):
                copy.wait()

        @pl.when(j >= 2)
        def _():
            drain(slot)

        def tile_step(n):
            here = part(n, tile)
            piece = dot_tn(l_ref[:], r_ref[:, here])
            if received is not None:
                piece = piece + ins[0][:, here]
            total[slot, :, here] = piece

        loop(cols // tile, tile_step)
        if parts:
            for r in range(CHIPS):
                @pl.when(j == r)
                def _():
                    for copy in copies(r, slot):
                        copy.start()
        else:
            for copy in copies(j, slot):
                copy.start()

        @pl.when(j == CHIPS - 1)
        def _():
            drain(1 - slot)
            drain(slot)

    in_specs = [spec((rows, BLK), fixed, lambda j, t: first_block(t) + j), whole(right)]
    args = (left, right)
    if received is not None:
        in_specs.append(spec((BLK, cols), moving, fixed))
        args += (received,)
    return call(body, ids, args, CHIPS, in_specs, anywhere(n_out), out_shape, [pltpu.VMEM((2, BLK, cols), F32), MANY((2, per))], gflop=8.6)


def add_kernel(ids, a, b):
    rows, cols = a.shape

    def body(t, a_ref, b_ref, o_ref):
        o_ref[:] = a_ref[:] + b_ref[:]

    io = spec((rows // CHIPS, cols), moving, fixed)
    return call(body, ids, (a, b), CHIPS, [io] * 2, io, like(a))


def sum_kernel(ids, top, bottom, widths, base=None):
    n = len(top)
    rows, cols = top[0].shape
    tile = rows // 2
    bases = () if base is None else (base,)
    dtype = F32 if base is None else base.dtype
    n_in = 2 * n + len(bases)

    def body(t, *refs):
        j = step_id()
        for side in range(2):
            @pl.when(j // 2 == side)
            def _():
                start = 0
                for width, out in zip(widths, refs[n_in:]):
                    cut = slice(start, start + width)
                    terms = [ref[:, cut] for ref in refs[n * side:n * (side + 1)]]
                    total = sum(terms[1:], terms[0])
                    for ref in refs[2 * n:n_in]:
                        total = ref[:].astype(F32) + total
                    out[:] = total.astype(dtype)
                    start += width

    top_spec = spec((tile, cols), until(2), fixed)
    bottom_spec = spec((tile, cols), since(2), fixed)
    return call(body, ids, tuple(top) + tuple(bottom) + bases, 4, [top_spec] * n + [bottom_spec] * n + [spec((tile, cols), moving, fixed) for _ in bases],
                [spec((tile, w), moving, fixed) for w in widths], [sds((2 * rows, w), dtype) for w in widths])


def move_kernel(ids, moves, sources, out_shapes):
    n_src, n_out, n = len(sources), len(out_shapes), len(moves)

    def body(t, *refs):
        srcs, outs = refs[:n_src], refs[n_src:n_src + n_out]
        *bufs, in_sem, out_sem = refs[n_src + n_out:]
        loads, stores = [], []
        for i, (src, src_at, out, out_at, _) in enumerate(moves):
            loads.append(pltpu.make_async_copy(srcs[src].at[src_at(t)], bufs[i], in_sem.at[i]))
            stores.append(pltpu.make_async_copy(bufs[i], outs[out].at[out_at(t)], out_sem.at[i]))
        for load in loads:
            load.start()
        for load, store in zip(loads, stores):
            load.wait()
            store.start()
        for store in stores:
            store.wait()

    shapes = [pltpu.VMEM(shape, sources[src].dtype) for src, _, _, _, shape in moves]
    return call(body, ids, tuple(sources), 1, anywhere(n_src), anywhere(n_out), list(out_shapes), shapes + [MANY((n,))] * 2)


def everything(t):
    return ALL, ALL


def row_at(index, size):
    return lambda t: (slice(index * size, (index + 1) * size), ALL)


def norm_back(t, grad_ref, rows, src_ref, gain_ref, base_ref, out_ref, gain_out_ref):
    src = src_ref[rows, :].astype(F32)
    scale = row_scale(src)
    inner = jnp.zeros_like(scale)
    for p in range(PLACES):
        cols = cols_of(p)
        unit = src_ref[rows, part(t[p], BLK)].astype(F32) * scale
        grad = grad_ref[rows, cols].astype(F32)
        gain_out_ref[:, cols] += jnp.sum(grad * unit, axis=0, keepdims=True)
        inner += row_sum(grad * gain_ref[:, cols] * unit)
    inner = inner * (1.0 / src.shape[-1])
    for p in range(PLACES):
        cols = cols_of(p)
        place = part(t[p], BLK)
        unit = src_ref[rows, place].astype(F32) * scale
        grad_rows = scale * (grad_ref[rows, cols].astype(F32) * gain_ref[:, cols] - unit * inner)
        out_ref[rows, place] = (base_ref[rows, place].astype(F32) + grad_rows).astype(BF16)


def hidden_grad_kernel(ids, top, bottom, hidden, gain_rel, dy):
    rows, d_model = hidden.shape
    tile = HEAD
    n_half = HALF_TOKENS // tile
    n = len(top)

    def body(t, *refs):
        h_ref, g_ref, dy_ref, out_ref, gain_ref, grad = refs[2 * n:]
        j = step_id()

        @pl.when(j == 0)
        def _():
            gain_ref[:] = jnp.zeros_like(gain_ref)

        for cond, terms in ((j < n_half, refs[:n]), (j >= n_half, refs[n:2 * n])):
            @pl.when(cond)
            def _():
                a, b, c = terms
                grad[:] = (a[:] + b[:] + c[:]).astype(BF16)

        norm_back(t, grad, ALL, h_ref, g_ref, dy_ref, out_ref, gain_ref)

    shape = (tile, d_model)
    row_spec = spec(shape, moving, fixed)
    return call(body, ids, tuple(top) + tuple(bottom) + (hidden, gain_rel, dy), rows // tile,
                [spec(shape, until(n_half), fixed)] * n + [spec(shape, since(n_half), fixed)] * n + [row_spec, whole(gain_rel), row_spec],
                [row_spec, whole(gain_rel)], [like(hidden), like(gain_rel)], [pltpu.VMEM(shape, BF16)], gflop=5)


def attn_grad_kernel(ids, grad_hidden, w_full):
    rows, d_model = grad_hidden.shape
    half = CHIPS // 2

    def block_row(j, t):
        side = t[SP] ^ (j < half).astype(jnp.int32)
        return (side * half + (j & 1)) ^ t[DP]

    def body(t, g_ref, w_ref, far_ref, keep_ref):
        j = step_id()

        def one_core(s):
            grad = dot_nt(g_ref[:], w_ref[s]).astype(BF16)
            for cond, ref in ((j < half, far_ref), (j >= half, keep_ref)):
                @pl.when(cond)
                def _():
                    for e in range(2):
                        ref[(t[SP] ^ s) * 2 + e] = grad[:, e * PAIR:(e + 1) * PAIR]

        loop(2, one_core)

    slabs = (CHIPS, rows, PAIR)
    return call(body, ids, (grad_hidden, w_full.reshape(2, CHIPS * BLK, d_model)), CHIPS,
                [whole(grad_hidden), spec((2, BLK, d_model), fixed, block_row, fixed)],
                [spec(slabs, until(half), fixed, fixed), spec(slabs, since(half), fixed, fixed)],
                [sds((Q_PAIRS, rows, PAIR), BF16)] * 2, gflop=4.3)


def unrope_kernel(ids, keep, got, cos_t, sin_t):
    _, rows, _ = keep.shape
    tile = HALF_BLK
    cols = 2 * SLABS * PAIR

    def body(t, k_ref, g_ref, cos_ref, sin_ref, o_ref):
        for ref, side in ((k_ref, t[SP]), (g_ref, 1 - t[SP])):
            for first, count, roped in ((0, Q_PAIRS, True), (K_SLAB, KV_PAIRS, True), (V_SLAB, KV_PAIRS, False)):
                def move(p):
                    pair = ref[first + p]
                    if roped:
                        pair = rope_lanes(pair.astype(F32), cos_ref[:], sin_ref[:], -1).astype(BF16)
                    o_ref[:, part(2 * first + side * count + p, PAIR)] = pair

                loop(count, move)

    h_spec = spec((SLABS, tile, PAIR), fixed, moving, fixed)
    t_spec = spec((tile, PAIR), moving, fixed)
    return call(body, ids, (keep, got, cos_t, sin_t), rows // tile, [h_spec, h_spec, t_spec, t_spec],
                spec((tile, cols), moving, fixed), sds((rows, cols), BF16))


def input_grad_kernel(ids, grad_qkv, w_full, act, gain_rel, grad_hidden):
    rows, d_model = act.shape
    _, cols = grad_qkv.shape
    strip_rows = HEAD

    def body(t, g_ref, w_ref, x_ref, gain_ref, gh_ref, out_ref, gain_out_ref, grad):
        j = step_id()
        grad[:, part(j, BLK)] = dot_nt(g_ref[:], w_ref[:]).astype(BF16)

        @pl.when(j == PLACES - 1)
        def _():
            gain_out_ref[:] = jnp.zeros_like(gain_out_ref)
            loop(rows // strip_rows, lambda i: norm_back(t, grad, part(i, strip_rows), x_ref, gain_ref, gh_ref, out_ref, gain_out_ref))

    return call(body, ids, (grad_qkv, w_full, act, gain_rel, grad_hidden), PLACES,
                [whole(grad_qkv), spec((BLK, cols), moving, fixed), whole(act), whole(gain_rel), whole(grad_hidden)],
                [whole(act), whole(gain_rel)], [like(act), like(gain_rel)], [pltpu.VMEM((rows, d_model), BF16)], gflop=10)


def solution(mesh):
    flat_axes = ("dp", "sp")
    row_spec = P("dp", "sp", None)
    pos_spec = P("dp", "sp")
    vec_spec = P(flat_axes)
    mat_spec = P(flat_axes, None)
    cube_spec = P(flat_axes, None, None)
    hops = {"x": 1, "y": 2, "d": 3}

    def send(way, v):
        if way == "s":
            return lax.ppermute(v, "sp", [(0, 1), (1, 0)])
        return lax.ppermute(v, "dp", [(i, i ^ hops[way]) for i in range(CHIPS)])

    def gather_pieces(own, *deps):
        from_x = send("x", own)
        from_y = send("y", own)
        if deps:
            from_x, from_y = after((from_x, from_y), *deps)
        return [own, from_x, from_y, send("y", from_x[:HALF_BLK]), send("x", from_y[HALF_BLK:])]

    def both_cores(pieces):
        return pieces + [send("s", p) for p in pieces]

    def gather_rows(top, bottom):
        xa = send("x", top)
        yb = send("y", bottom)
        xb = send("x", bottom)
        ya = send("y", top)
        return [top, bottom], [xa, xb], [ya, yb], [send("y", xa), send("x", yb)]

    def scatter4(ids, halves):
        (a0, b0), (a1, b1), (a2, b2), (a3, b3) = halves
        u1 = send("x", a1)
        u2 = send("y", b2)
        t1 = send("x", a3)
        t2 = send("y", b3)
        v1 = send("x", add_kernel(ids, b1, t2))
        v2 = send("y", add_kernel(ids, a2, t1))
        return (a0, u1, v2), (b0, u2, v1)

    def layer(act_in, positions, out_grad, norm1_gain, norm2_gain, w_query, w_key, w_value, w_out, w_gate, w_up, w_down):
        dp = lax.axis_index("dp")
        sp = lax.axis_index("sp")
        _, n_q, hd = w_query.shape
        _, n_kv, _ = w_key.shape
        q_cols, kv_cols = n_q * hd, n_kv * hd
        (act,), (pos,), (dy,) = act_in, positions, out_grad
        _, d_model = act.shape
        half_d = d_model // 2
        _, f_cols = w_gate.shape
        quarter = f_cols // CHIPS
        place = jnp.arange(PLACES, dtype=jnp.int32)
        rel_table = ((place % CHIPS) ^ dp) * 2 + ((place // CHIPS) ^ sp)
        abs_table = ((place % 2) ^ sp) * CHIPS + ((place // 2) ^ dp)
        ids = jnp.concatenate([rel_table, abs_table, jnp.stack([sp, dp])]).astype(jnp.int32)

        wo_pieces = both_cores(gather_pieces(w_out))
        w_qkv = jnp.concatenate([w.reshape(BLK, -1) for w in (w_query, w_key, w_value)], axis=1)
        gains = jnp.stack([norm1_gain, norm2_gain])
        gain_mine = jnp.concatenate([gains, send("x", gains), send("y", gains), send("d", gains)], axis=1)
        gain_rel = jnp.concatenate([gain_mine, send("s", gain_mine)], axis=1).astype(F32)
        gain1_rel, gain2_rel = gain_rel[:1], gain_rel[1:]
        w2_rows, _ = w_down.shape

        def w2_at(side):
            return lambda t: (part(t[SP] ^ side, w2_rows), ALL)

        w2_pair = [w_down, send("s", w_down)]
        (w2,) = move_kernel(ids, [(i, everything, 0, w2_at(i), w_down.shape) for i in range(2)], w2_pair, [sds((2 * w2_rows, d_model), BF16)])

        inv_freq = ROPE_BASE ** (-(jnp.arange(HALF_HEAD, dtype=F32) * (1.0 / HALF_HEAD)))
        angles = pos.astype(F32)[:, None] * inv_freq
        cos_t = jnp.tile(jnp.cos(angles), (1, 4))
        sin_t = jnp.tile(jnp.sin(angles), (1, 4))
        u_rel = norm_kernel(ids, after(act, cos_t, sin_t), gain1_rel)
        qkv_pieces = both_cores(gather_pieces(w_qkv, u_rel, w2))

        def quarter_at(r):
            return lambda t: (ALL, part(t[DP] ^ r, quarter))

        tile_shape = (BLK, quarter)
        moves = [(i, quarter_at(r), r, row_at(i, BLK), tile_shape) for r in range(CHIPS) for i in range(2)]
        q0, q1, q2, q3 = move_kernel(ids, moves, [w_gate, w_up], [sds((2 * BLK, quarter), BF16)] * CHIPS)
        f_pieces = both_cores([q0, send("x", q1), send("y", q2), send("d", q3)])
        moves = [(i, row_at(o, BLK), o, row_at(i, BLK), tile_shape) for i in range(PLACES) for o in range(2)]
        w1, w3 = move_kernel(ids, moves, f_pieces, [sds((d_model, quarter), BF16)] * 2)

        qkv_far, qkv_keep, wqkv_full = qkv_kernel(ids, u_rel, qkv_pieces, cos_t, sin_t)
        qkv_got = send("s", qkv_far)
        o_keep, o_far = attn_fwd_kernel(ids, qkv_keep, qkv_got)
        o_got = send("s", o_far)
        attn_rel, hidden, normed_a, normed_b, wo_full = out_proj_kernel(ids, o_keep, o_got, wo_pieces, act, gain2_rel)

        w_rows = gather_rows(normed_a, normed_b)
        dy_rows = gather_rows(dy[:HALF_TOKENS], dy[HALF_TOKENS:])
        fwd = ffn_fwd_kernel(ids, 0, [(0, w_rows[0])], w1, w3, ())
        fwd = ffn_fwd_kernel(ids, 1, list(enumerate(w_rows))[1:3], w1, w3, fwd)
        y1 = ffn_y_kernel(ids, 1, fwd[1], w2)
        bwd = ffn_bwd_kernel(ids, 1, dy_rows[1] + dy_rows[2], fwd[2], fwd[3], w2, ())
        dw1 = ffn_dw_kernel(ids, 1, (1, 2), bwd[1], bwd[2], w1, w3)
        w_all, mixed, gate_pre, up_pre = ffn_fwd_kernel(ids, 1, [(3, w_rows[3])], w1, w3, fwd)
        dy_all, dgate, dup = ffn_bwd_kernel(ids, 0, [dy] + dy_rows[3], gate_pre, up_pre, w2, bwd)
        dw0 = ffn_dw_kernel(ids, 0, (0, 3), dgate, dup, w1, w3)
        y0 = ffn_y_kernel(ids, 0, mixed, w2)

        def by_chip(pair0, pair1):
            return [pair0[:2], pair1[:2], pair1[2:], pair0[2:]]

        dw_top, dw_bottom = scatter4(ids, by_chip(dw0, dw1))
        y_top, y_bottom = scatter4(ids, by_chip(y0, y1))
        (act_out,) = sum_kernel(ids, y_top, y_bottom, (d_model,), hidden)

        def column_grad(grad_all):
            (far,) = weight_grad_kernel(ids, w_all, grad_all, lambda t: CHIPS, None, 0)
            own, *rest = weight_grad_kernel(ids, w_all, grad_all, lambda t: 0, send("s", far), 1)
            return [own] + [send(way, v) for way, v in zip("xyd", rest)]

        def placed(pieces):
            return move_kernel(ids, [(r, everything, 0, quarter_at(r), tile_shape) for r in range(CHIPS)], pieces, [sds((BLK, f_cols), F32)])

        gate_pieces = column_grad(dgate)
        up_pieces = column_grad(dup)
        (down_far,) = weight_grad_kernel(ids, mixed, dy_all, lambda t: (1 - t[SP]) * CHIPS, None, 0)
        (down_grad,) = weight_grad_kernel(ids, mixed, dy_all, lambda t: t[SP] * CHIPS, send("s", down_far), 0)
        (gate_grad,) = placed(gate_pieces)
        (up_grad,) = placed(up_pieces)

        grad_hidden, gain2_part = hidden_grad_kernel(ids, dw_top, dw_bottom, hidden, gain2_rel, dy)

        def row_grad(left, right):
            (far,) = weight_grad_kernel(ids, left, right, lambda t: CHIPS, None, 0)
            parts = weight_grad_kernel(ids, left, right, lambda t: 0, send("s", far), 2)
            return scatter4(ids, list(zip(parts[::2], parts[1::2])))

        do_far, do_keep = attn_grad_kernel(ids, grad_hidden, wo_full)
        do_got = send("s", do_far)
        d_keep, d_far = attn_bwd_kernel(ids, qkv_keep, qkv_got, do_keep, do_got)
        d_got = send("s", d_far)
        wo_top, wo_bottom = row_grad(attn_rel, grad_hidden)
        grad_qkv = unrope_kernel(ids, d_keep, d_got, cos_t, sin_t)
        qkv_top, qkv_bottom = row_grad(u_rel, grad_qkv)
        q_grad, k_grad, v_grad = sum_kernel(ids, qkv_top, qkv_bottom, (q_cols, kv_cols, kv_cols))
        query_grad = q_grad.reshape(w_query.shape)
        key_grad = k_grad.reshape(w_key.shape)
        value_grad = v_grad.reshape(w_value.shape)
        top = add_kernel(ids, *wo_top[:2])
        bottom = add_kernel(ids, *wo_bottom[:2])
        top, bottom = after((top, bottom), query_grad, key_grad, value_grad)
        (wout_grad,) = sum_kernel(ids, (top, wo_top[2]), (bottom, wo_bottom[2]), (d_model,))
        in_grad, gain1_part = input_grad_kernel(ids, grad_qkv, wqkv_full, act, gain1_rel, grad_hidden)

        gain_part = jnp.concatenate([gain1_part, gain2_part], axis=0)
        gain_half = gain_part[:, :half_d] + send("s", gain_part[:, half_d:])
        own, to_x, to_y, to_d = [gain_half[:, cols_of(r)] for r in range(CHIPS)]
        gain1_grad, gain2_grad = own + send("x", to_x) + send("y", to_y) + send("d", to_d)
        return (act_out[None], in_grad[None], gain1_grad, gain2_grad, query_grad, key_grad, value_grad, wout_grad, gate_grad, up_grad, down_grad)

    return jax.shard_map(layer, mesh=mesh, in_specs=(row_spec, pos_spec, row_spec, vec_spec, vec_spec, cube_spec, cube_spec, cube_spec, mat_spec, mat_spec, mat_spec, mat_spec), out_specs=(row_spec, row_spec, vec_spec, vec_spec, cube_spec, cube_spec, cube_spec, mat_spec, mat_spec, mat_spec, mat_spec), check_vma=False)
```

```python
import jax
import jax.numpy as jnp
from jax import lax
from jax.experimental import pallas as pl
from jax.experimental.pallas import tpu as pltpu
from jax.sharding import PartitionSpec as P

INTERPRET = False

EPS = 1e-5
ROPE_BASE = 10000.0
NEG_BIG = -1e30
F32 = jnp.float32
BF16 = jnp.bfloat16
CHIPS = 4
PLACES = 8
BLK = 256
HALF_BLK = BLK // 2
TOKENS = 512
HALF_TOKENS = TOKENS // 2
HEAD = 64
HALF_HEAD = HEAD // 2
PAIR = 2 * HEAD
ATTN_SCALE = HEAD ** -0.5
GROUPS = 4
GROUP_HEADS = 4
Q_PAIRS = 8
KV_PAIRS = 2
K_SLAB = Q_PAIRS
V_SLAB = K_SLAB + KV_PAIRS
SLABS = V_SLAB + KV_PAIRS
ALL = slice(None)
MANY = pltpu.SemaphoreType.DMA


def dot(a, b):
    return lax.dot_general(a, b, (((1,), (0,)), ((), ())), preferred_element_type=F32)


def dot_nt(a, b):
    return lax.dot_general(a, b, (((1,), (1,)), ((), ())), preferred_element_type=F32)


def dot_tn(a, b):
    return lax.dot_general(a, b, (((0,), (0,)), ((), ())), preferred_element_type=F32)


def after(value, *deps):
    first, *_ = lax.optimization_barrier((value,) + deps)
    return first


def sds(shape, dtype):
    return jax.ShapeDtypeStruct(shape, dtype)


def like(v):
    return sds(v.shape, v.dtype)


def fixed(j, t):
    return 0


def moving(j, t):
    return j


def until(n):
    return lambda j, t: jnp.minimum(j, n - 1)


def since(n):
    return lambda j, t: jnp.maximum(j - n, 0)


def always(n):
    return lambda j, t: n


def spec(shape, *index):
    return pl.BlockSpec(shape, lambda j, t: tuple(f(j, t) for f in index))


def whole(v):
    return spec(v.shape, *[fixed] * len(v.shape))


def anywhere(n):
    return [pl.BlockSpec(memory_space=pl.ANY)] * n


def call(body, ids, args, grid, in_specs, out_specs, out_shape, scratch=(), gflop=1.0, aliases=None):
    return pl.pallas_call(
        body,
        out_shape=out_shape,
        grid_spec=pltpu.PrefetchScalarGridSpec(num_scalar_prefetch=1, grid=(grid,), in_specs=in_specs, out_specs=out_specs, scratch_shapes=list(scratch)),
        cost_estimate=pl.CostEstimate(flops=int(gflop * 1e9), bytes_accessed=int(1e7), transcendentals=0),
        compiler_params=pltpu.CompilerParams(dimension_semantics=("arbitrary",)),
        input_output_aliases=aliases or {},
        interpret=INTERPRET,
    )(ids, *args)


def step_id():
    return pl.program_id(0)


def loop(count, body):
    def one(i, carry):
        body(i)
        return carry

    lax.fori_loop(0, count, one, 0)


SP = 2 * PLACES
DP = SP + 1


def part(index, size):
    return pl.ds(pl.multiple_of(index * size, size), size)


def cols_of(p):
    return slice(p * BLK, (p + 1) * BLK)


def row_sum(v):
    return jnp.sum(v, axis=-1, keepdims=True)


def row_scale(x):
    return lax.rsqrt(row_sum(x * x) * (1.0 / x.shape[-1]) + EPS)


def write_normed(t, src, rows, gain, out, out_rows):
    scale = row_scale(src[rows, :].astype(F32))
    for p in range(PLACES):
        blk = src[rows, part(t[p], BLK)].astype(F32)
        out[out_rows, cols_of(p)] = (blk * scale * gain[:, cols_of(p)]).astype(BF16)


def to_neighbour(k):
    return [p for p in range(PLACES) if p & k]


def here_blocks(k):
    return [p for p in range(PLACES) if not p & k]


def copy_blocks(dst, src, places):
    for i, p in enumerate(places):
        dst[:, cols_of(i)] = src[:, cols_of(p)]


def norm_kernel(ids, act, gain_rel):
    rows, cols = act.shape
    tile = HALF_BLK

    def body(t, x_ref, g_ref, o_ref, send_ref):
        write_normed(t, x_ref, ALL, g_ref, o_ref, ALL)
        copy_blocks(send_ref, o_ref, to_neighbour(1))

    io = spec((tile, cols), moving, fixed)
    return call(body, ids, (act, gain_rel), rows // tile, [io, whole(gain_rel)],
                [io, spec((tile, cols // 2), moving, fixed)], [like(act), sds((rows, cols // 2), BF16)])


def rope_lanes(values, cos_t, sin_t, sign):
    width = values.shape[-1]
    reps = width // PAIR
    if reps > 1:
        cos_t = jnp.concatenate([cos_t] * reps, axis=1)
        sin_t = jnp.concatenate([sin_t] * reps, axis=1)
    lane = lax.broadcasted_iota(jnp.int32, values.shape, 1)
    up_roll = pltpu.roll(values, width - HALF_HEAD, 1)
    down_roll = pltpu.roll(values, HALF_HEAD, 1)
    other = jnp.where((lane & (HEAD - 1)) < HALF_HEAD, -up_roll, down_roll)
    return values * cos_t + (other * sin_t if sign > 0 else -(other * sin_t))


def fill(scratch, refs):
    start = 0
    for ref in refs:
        n, _ = ref.shape
        scratch[start:start + n, :] = ref[:]
        start += n


def qkv_kernel(ids, u_rel, pieces, cos_t, sin_t):
    rows, d_model = u_rel.shape
    cols = pieces[0].shape[1]
    n_pieces = len(pieces)
    tiles = SLABS // 2
    q_tiles = Q_PAIRS // 2

    def column(j, t):
        far = (j < tiles).astype(jnp.int32)
        half = t[SP] ^ far
        tile = j - tiles * (1 - far)
        return jnp.where(tile < q_tiles, half * q_tiles + tile, 2 * tile + half)

    def body(t, u_ref, cos_ref, sin_ref, *refs):
        far_ref, keep_ref, w_ref = refs[n_pieces:]
        j = step_id()
        fill(w_ref, refs[:n_pieces])
        acc = dot(u_ref[:], w_ref[:])
        roped = rope_lanes(acc, cos_ref[:], sin_ref[:], 1)
        is_value = (j == tiles - 1) | (j == 2 * tiles - 1)
        out = jnp.where(is_value, acc, roped).astype(BF16)
        for cond, ref in ((j < tiles, far_ref), (j >= tiles, keep_ref)):
            @pl.when(cond)
            def _():
                for e in range(2):
                    ref[e] = out[:, e * PAIR:(e + 1) * PAIR]

    w_specs = [spec((p.shape[0], BLK), fixed, column) for p in pieces]
    slab = (2, rows, PAIR)
    return call(body, ids, (u_rel, cos_t, sin_t) + tuple(pieces), 2 * tiles,
                [whole(u_rel), whole(cos_t), whole(sin_t)] + w_specs,
                [spec(slab, until(tiles), fixed, fixed), spec(slab, since(tiles), fixed, fixed), spec((d_model, BLK), fixed, column)],
                [sds((SLABS, rows, PAIR), BF16)] * 2 + [sds((d_model, cols), BF16)], gflop=6.5)


def core_rows(t, rows):
    return part(t[SP], rows), part(1 - t[SP], rows)


def in_order(t, ref, own, other):
    for here, v in zip(core_rows(t, own.shape[0]), (own, other)):
        ref[here, :] = v


def one_head(pair, odd):
    return jnp.where(odd == 1, pair[:, HEAD:], pair[:, :HEAD])


def softmax_rows(q_tile, keys, first_row, span):
    scores = dot_nt(q_tile, keys) * ATTN_SCALE
    edge = span - BLK
    shape = (q_tile.shape[0], BLK)
    row = lax.broadcasted_iota(jnp.int32, shape, 0) + first_row
    col = lax.broadcasted_iota(jnp.int32, shape, 1)
    last = jnp.where(row >= col, scores[:, edge:], NEG_BIG)
    scores = jnp.concatenate([scores[:, :edge], last], axis=1) if edge else last
    expo = jnp.exp(scores - jnp.max(scores, axis=-1, keepdims=True))
    return expo * (1.0 / row_sum(expo))


def head_specs(rows):
    slabs = (2, rows, PAIR)
    one = (1, rows, PAIR)
    q_spec = spec(slabs, moving, fixed, fixed)
    return q_spec, [q_spec] + [spec(one, lambda j, t, base=base: base + j // 2, fixed, fixed) for base in (K_SLAB, V_SLAB)]


def attn_fwd_kernel(ids, keep, got):
    _, rows, _ = keep.shape
    seq = 2 * rows

    def body(t, qk_ref, kk_ref, vk_ref, qg_ref, kg_ref, vg_ref, keep_ref, send_ref, ks, vs, qs, os):
        odd = step_id() & 1
        in_order(t, ks, one_head(kk_ref[0], odd), one_head(kg_ref[0], odd))
        in_order(t, vs, one_head(vk_ref[0], odd), one_head(vg_ref[0], odd))

        def head(h):
            in_order(t, qs, one_head(qk_ref[h // 2], h & 1), one_head(qg_ref[h // 2], h & 1))
            for span in range(BLK, seq + BLK, BLK):
                prob = softmax_rows(qs[span - BLK:span, :], ks[:span, :], 0, span).astype(BF16)
                os[h, span - BLK:span, :] = dot(prob, vs[:span, :]).astype(BF16)

        loop(GROUP_HEADS, head)
        for here, ref in zip(core_rows(t, rows), (keep_ref, send_ref)):
            for p in range(2):
                ref[p] = jnp.concatenate([os[2 * p, here, :], os[2 * p + 1, here, :]], axis=1)

    q_spec, specs = head_specs(rows)
    return call(body, ids, (keep,) * 3 + (got,) * 3, GROUPS, specs * 2,
                [q_spec] * 2, [sds((Q_PAIRS, rows, PAIR), BF16)] * 2,
                [pltpu.VMEM((seq, HEAD), BF16)] * 3 + [pltpu.VMEM((GROUP_HEADS, seq, HEAD), BF16)], gflop=20)


def attn_bwd_kernel(ids, keep, got, do_keep, do_got):
    _, rows, _ = keep.shape
    seq = 2 * rows
    strip_rows = BLK

    def body(t, qk_ref, kk_ref, vk_ref, dk_ref, qg_ref, kg_ref, vg_ref, dg_ref, keep_ref, send_ref, ks, vs, qs, ds, dqs, dks, dvs):
        g = step_id()
        odd = g & 1
        in_order(t, ks, one_head(kk_ref[0], odd), one_head(kg_ref[0], odd))
        in_order(t, vs, one_head(vk_ref[0], odd), one_head(vg_ref[0], odd))
        dks[odd] = jnp.zeros_like(ks, F32)
        dvs[odd] = jnp.zeros_like(vs, F32)

        def head(h):
            in_order(t, qs, one_head(qk_ref[h // 2], h & 1), one_head(qg_ref[h // 2], h & 1))
            in_order(t, ds, one_head(dk_ref[h // 2], h & 1), one_head(dg_ref[h // 2], h & 1))
            for span in range(BLK, seq + BLK, BLK):
                def strip(n):
                    here = part((span - BLK) // strip_rows + n, strip_rows)
                    q_tile = qs[here, :]
                    do_tile = ds[here, :]
                    prob = softmax_rows(q_tile, ks[:span, :], n * strip_rows, span)
                    grad_prob = dot_nt(do_tile, vs[:span, :])
                    inner = row_sum(prob * grad_prob)
                    grad_scores = (prob * (grad_prob - inner) * ATTN_SCALE).astype(BF16)
                    dqs[h, here, :] = dot(grad_scores, ks[:span, :]).astype(BF16)
                    dks[odd, :span, :] += dot_tn(grad_scores, q_tile)
                    dvs[odd, :span, :] += dot_tn(prob.astype(BF16), do_tile)

                loop(BLK // strip_rows, strip)

        loop(GROUP_HEADS, head)
        for here, ref in zip(core_rows(t, rows), (keep_ref, send_ref)):
            for p in range(2):
                ref[2 * g + p] = jnp.concatenate([dqs[2 * p, here, :], dqs[2 * p + 1, here, :]], axis=1)

            @pl.when(odd == 1)
            def _():
                for base, acc in ((K_SLAB, dks), (V_SLAB, dvs)):
                    ref[base + g // 2] = jnp.concatenate([acc[0, here, :], acc[1, here, :]], axis=1).astype(BF16)

    q_spec, specs = head_specs(rows)
    return call(body, ids, (keep,) * 3 + (do_keep,) + (got,) * 3 + (do_got,), GROUPS, (specs + [q_spec]) * 2,
                [whole(keep)] * 2, [like(keep)] * 2,
                [pltpu.VMEM((seq, HEAD), BF16)] * 4 + [pltpu.VMEM((GROUP_HEADS, seq, HEAD), BF16)] + [pltpu.VMEM((2, seq, HEAD), F32)] * 2, gflop=50)


def out_proj_kernel(ids, o_keep, o_got, pieces, act, gain_rel):
    rows, d_model = act.shape
    tile = BLK
    strip_rows = HALF_HEAD
    n_pieces = len(pieces)

    def body(t, ok_ref, og_ref, x_ref, g_ref, *refs):
        a_ref, h_ref, wa_ref, wb_ref, w_ref, send_ref, a_abs = refs[n_pieces:]
        j = step_id()

        @pl.when(j == 0)
        def _():
            for ref, side in ((ok_ref, t[SP]), (og_ref, 1 - t[SP])):
                for p in range(Q_PAIRS):
                    a_abs[:, part(side * Q_PAIRS + p, PAIR)] = ref[p]
            for p in range(PLACES):
                a_ref[:, cols_of(p)] = a_abs[:, part(t[p], BLK)]
            copy_blocks(send_ref, a_ref, to_neighbour(2))

        fill(w_ref, refs[:n_pieces])
        acc = dot(a_ref[:], w_ref[:])
        cols = part(j, tile)
        h_ref[:, cols] = (x_ref[:, cols].astype(F32) + acc).astype(BF16)

        @pl.when(j == d_model // tile - 1)
        def _():
            strips = HALF_TOKENS // strip_rows
            for side, out_ref in enumerate((wa_ref, wb_ref)):
                loop(strips, lambda i: write_normed(t, h_ref, part(side * strips + i, strip_rows), g_ref, out_ref, part(i, strip_rows)))

    w_specs = [spec((p.shape[0], tile), fixed, moving) for p in pieces]
    half = sds((HALF_TOKENS, d_model), BF16)
    send = sds((rows, d_model // 2), BF16)
    return call(body, ids, (o_keep, o_got, act, gain_rel) + tuple(pieces), d_model // tile,
                [whole(o_keep), whole(o_got), whole(act), whole(gain_rel)] + w_specs,
                [whole(act)] * 2 + [whole(half)] * 2 + [spec((d_model, tile), fixed, moving), whole(send)],
                [like(act)] * 2 + [half] * 2 + [sds((d_model, d_model), BF16), send], [pltpu.VMEM((rows, d_model), BF16)], gflop=4.3)


def swapped(place, k):
    return place ^ k


def ffn_fwd_kernel(ids, place, chunks, w1, w3, buffers, strips=1):
    d_model, f_cols = w1.shape
    tile = BLK
    owners = [k for k, parts in chunks for _ in parts]
    parts = [p for _, parts in chunks for p in parts]
    rows = sum(p.shape[0] for p in parts)
    n_parts = len(parts)
    n_buf = len(buffers)

    def body(t, *refs):
        w1_ref, w3_ref = refs[n_parts:n_parts + 2]
        wall_ref, m_ref, gate_ref, up_ref = refs[n_parts + 2 + n_buf:]

        @pl.when(step_id() == 0)
        def _():
            start = 0
            for k, ref in zip(owners, refs):
                n, _ = ref.shape
                for p in range(PLACES):
                    wall_ref[start:start + n, cols_of(p)] = ref[:, cols_of(swapped(p, k))]
                start += n

        def strip(n):
            here = part(n, rows // strips)
            gate = dot(wall_ref[here, :], w1_ref[:])
            up = dot(wall_ref[here, :], w3_ref[:])
            gate_ref[here, :] = gate
            up_ref[here, :] = up
            m_ref[here, :] = (gate * jax.nn.sigmoid(gate) * up).astype(BF16)

        loop(strips, strip)

    w_spec = spec((d_model, tile), fixed, moving)
    tile_spec = spec((rows, tile), always(place), moving)
    total = CHIPS * TOKENS
    return call(body, ids, tuple(parts) + (w1, w3) + tuple(buffers), f_cols // tile, [whole(p) for p in parts] + [w_spec] * 2 + anywhere(n_buf),
                [spec((rows, d_model), always(place), fixed)] + [tile_spec] * 3,
                [sds((total, d_model), BF16), sds((total, f_cols), BF16)] + [sds((total, f_cols), F32)] * 2,
                gflop=8.6, aliases={n_parts + 3 + i: i for i in range(n_buf)})


def ffn_bwd_kernel(ids, place, parts, gate_pre, up_pre, w2, buffers):
    f_cols, d_model = w2.shape
    tile = BLK
    rows = sum(p.shape[0] for p in parts)
    n_parts = len(parts)
    n_buf = len(buffers)

    def body(t, *refs):
        gate_ref, up_ref, w2_ref = refs[n_parts:n_parts + 3]
        dyall_ref, dg_ref, du_ref = refs[n_parts + 3 + n_buf:]

        @pl.when(step_id() == 0)
        def _():
            fill(dyall_ref, refs[:n_parts])

        def strip(n):
            here = part(n, TOKENS)
            back = dot_nt(dyall_ref[here, :], w2_ref[:]).astype(BF16).astype(F32)
            gate = gate_ref[here, :]
            sig = jax.nn.sigmoid(gate)
            du_ref[here, :] = (back * (gate * sig)).astype(BF16)
            dg_ref[here, :] = (back * up_ref[here, :] * sig * (1.0 + gate * (1.0 - sig))).astype(BF16)

        loop(rows // TOKENS, strip)

    tile_spec = spec((rows, tile), always(place), moving)
    total = CHIPS * TOKENS
    return call(body, ids, tuple(parts) + (gate_pre, up_pre, w2) + tuple(buffers), f_cols // tile,
                [whole(p) for p in parts] + [tile_spec] * 2 + [spec((tile, d_model), moving, fixed)] + anywhere(n_buf),
                [spec((rows, d_model), always(place), fixed)] + [tile_spec] * 2,
                [sds((total, d_model), BF16)] + [sds((total, f_cols), BF16)] * 2,
                gflop=8.6, aliases={n_parts + 4 + i: i for i in range(n_buf)})


def write_halves(outs, value):
    for i, out in enumerate(outs):
        out[:] = value[i * HALF_TOKENS:(i + 1) * HALF_TOKENS]


def ffn_dw_kernel(ids, place, owners, dgate, dup, w1, w3):
    d_model, f_cols = w1.shape

    def body(t, dg_ref, du_ref, w1_ref, w3_ref, *outs):
        write_halves(outs, dot_nt(dg_ref[:], w1_ref[:]) + dot_nt(du_ref[:], w3_ref[:]))

    row_spec = spec((2 * TOKENS, f_cols), always(place), fixed)
    w_spec = spec((BLK, f_cols), moving, fixed)
    out_specs = [spec((HALF_TOKENS, BLK), fixed, lambda j, t, k=k: j ^ k) for k in owners for _ in range(2)]
    return call(body, ids, (dgate, dup, w1, w3), d_model // BLK, [row_spec, row_spec, w_spec, w_spec],
                out_specs, [sds((HALF_TOKENS, d_model), F32)] * len(out_specs), gflop=17)


def ffn_y_kernel(ids, place, mixed, w2):
    f_cols, d_model = w2.shape

    def body(t, m_ref, w2_ref, *outs):
        write_halves(outs, dot(m_ref[:], w2_ref[:]))

    return call(body, ids, (mixed, w2), d_model // BLK, [spec((2 * TOKENS, f_cols), always(place), fixed), spec((f_cols, BLK), fixed, moving)],
                [spec((HALF_TOKENS, BLK), fixed, moving)] * 4, [sds((HALF_TOKENS, d_model), F32)] * 4, gflop=8.6)


def weight_grad_kernel(ids, pairs, n_blocks, received, parts):
    _, cols = pairs[0][-1].shape
    per = max(parts, 1)
    sub = BLK // per
    tile = TOKENS
    out_shape = [sds((sub, cols), F32)] * (n_blocks * parts) if parts else [sds((n_blocks * BLK, cols), F32)]
    n_out = len(out_shape)
    n_ops = 2 * len(pairs)

    def body(t, *refs):
        j = step_id()
        *ins, total, sem = refs
        outs = ins[len(ins) - n_out:]
        slot = j & 1

        def copies(r, slot):
            if not parts:
                return [pltpu.make_async_copy(total.at[slot], outs[0].at[part(r, BLK), :], sem.at[slot, 0])]
            return [pltpu.make_async_copy(total.at[slot, pl.ds(i * sub, sub), :], outs[r * parts + i], sem.at[slot, i]) for i in range(parts)]

        def drain(slot):
            for copy in copies(0, slot):
                copy.wait()

        @pl.when(j >= 2)
        def _():
            drain(slot)

        def tile_step(n):
            here = part(n, tile)
            terms = [dot_tn(l[:], r[:, here]) for l, r in zip(ins[:n_ops:2], ins[1:n_ops:2])]
            if received is not None:
                terms.append(ins[n_ops][:, here])
            total[slot, :, here] = sum(terms[1:], terms[0])

        loop(cols // tile, tile_step)
        if parts:
            for r in range(n_blocks):
                @pl.when(j == r)
                def _():
                    for copy in copies(r, slot):
                        copy.start()
        else:
            for copy in copies(j, slot):
                copy.start()

        @pl.when(j == n_blocks - 1)
        def _():
            drain(1 - slot)
            drain(slot)

    in_specs, args = [], ()
    for left, block, right in pairs:
        in_specs += [spec((left.shape[0], BLK), fixed, block), whole(right)]
        args += (left, right)
    if received is not None:
        in_specs.append(spec((BLK, cols), moving, fixed))
        args += (received,)
    return call(body, ids, args, n_blocks, in_specs, anywhere(n_out), out_shape, [pltpu.VMEM((2, BLK, cols), F32), MANY((2, per))], gflop=8.6)


def later(first, stride=1):
    return lambda j, t: first + stride * j


def add_kernel(ids, a, b):
    rows, cols = a.shape

    def body(t, a_ref, b_ref, o_ref):
        o_ref[:] = a_ref[:] + b_ref[:]

    io = spec((rows // CHIPS, cols), moving, fixed)
    return call(body, ids, (a, b), CHIPS, [io] * 2, io, like(a))


def sum_kernel(ids, top, bottom, widths, base=None, dtype=F32):
    n = len(top)
    rows, cols = top[0].shape
    tile = rows // 2
    bases = () if base is None else (base,)
    n_in = 2 * n + len(bases)

    def body(t, *refs):
        j = step_id()
        for side in range(2):
            @pl.when(j // 2 == side)
            def _():
                start = 0
                for width, out in zip(widths, refs[n_in:]):
                    cut = slice(start, start + width)
                    terms = [ref[:, cut] for ref in refs[n * side:n * (side + 1)]]
                    total = sum(terms[1:], terms[0])
                    for ref in refs[2 * n:n_in]:
                        total = ref[:].astype(F32) + total
                    out[:] = total.astype(dtype)
                    start += width

    top_spec = spec((tile, cols), until(2), fixed)
    bottom_spec = spec((tile, cols), since(2), fixed)
    return call(body, ids, tuple(top) + tuple(bottom) + bases, 4, [top_spec] * n + [bottom_spec] * n + [spec((tile, cols), moving, fixed) for _ in bases],
                [spec((tile, w), moving, fixed) for w in widths], [sds((2 * rows, w), dtype) for w in widths])


def move_kernel(ids, moves, sources, out_shapes):
    n_src, n_out, n = len(sources), len(out_shapes), len(moves)

    def body(t, *refs):
        srcs, outs = refs[:n_src], refs[n_src:n_src + n_out]
        *bufs, in_sem, out_sem = refs[n_src + n_out:]
        loads, stores = [], []
        for i, (src, src_at, out, out_at, _) in enumerate(moves):
            loads.append(pltpu.make_async_copy(srcs[src].at[src_at(t)], bufs[i], in_sem.at[i]))
            stores.append(pltpu.make_async_copy(bufs[i], outs[out].at[out_at(t)], out_sem.at[i]))
        for load in loads:
            load.start()
        for load, store in zip(loads, stores):
            load.wait()
            store.start()
        for store in stores:
            store.wait()

    shapes = [pltpu.VMEM(shape, sources[src].dtype) for src, _, _, _, shape in moves]
    return call(body, ids, tuple(sources), 1, anywhere(n_src), anywhere(n_out), list(out_shapes), shapes + [MANY((n,))] * 2)


def everything(t):
    return ALL, ALL


def row_at(index, size):
    return lambda t: (slice(index * size, (index + 1) * size), ALL)


def norm_back(t, grad_ref, rows, src_ref, gain_ref, base_ref, out_ref, gain_out_ref):
    src = src_ref[rows, :].astype(F32)
    scale = row_scale(src)
    inner = jnp.zeros_like(scale)
    for p in range(PLACES):
        cols = cols_of(p)
        unit = src_ref[rows, part(t[p], BLK)].astype(F32) * scale
        grad = grad_ref[rows, cols].astype(F32)
        gain_out_ref[:, cols] += jnp.sum(grad * unit, axis=0, keepdims=True)
        inner += row_sum(grad * gain_ref[:, cols] * unit)
    inner = inner * (1.0 / src.shape[-1])
    for p in range(PLACES):
        cols = cols_of(p)
        place = part(t[p], BLK)
        unit = src_ref[rows, place].astype(F32) * scale
        grad_rows = scale * (grad_ref[rows, cols].astype(F32) * gain_ref[:, cols] - unit * inner)
        out_ref[rows, place] = (base_ref[rows, place].astype(F32) + grad_rows).astype(BF16)


def hidden_grad_kernel(ids, top, bottom, hidden, gain_rel, dy):
    rows, d_model = hidden.shape
    tile = HEAD
    n_half = HALF_TOKENS // tile
    n = len(top)

    def body(t, *refs):
        h_ref, g_ref, dy_ref, out_ref, gain_ref, grad = refs[2 * n:]
        j = step_id()

        @pl.when(j == 0)
        def _():
            gain_ref[:] = jnp.zeros_like(gain_ref)

        for cond, terms in ((j < n_half, refs[:n]), (j >= n_half, refs[n:2 * n])):
            @pl.when(cond)
            def _():
                a, b, c = terms
                grad[:] = (a[:] + b[:] + c[:]).astype(BF16)

        norm_back(t, grad, ALL, h_ref, g_ref, dy_ref, out_ref, gain_ref)

    shape = (tile, d_model)
    row_spec = spec(shape, moving, fixed)
    return call(body, ids, tuple(top) + tuple(bottom) + (hidden, gain_rel, dy), rows // tile,
                [spec(shape, until(n_half), fixed)] * n + [spec(shape, since(n_half), fixed)] * n + [row_spec, whole(gain_rel), row_spec],
                [row_spec, whole(gain_rel)], [like(hidden), like(gain_rel)], [pltpu.VMEM(shape, BF16)], gflop=5)


def attn_grad_kernel(ids, grad_hidden, w_full):
    rows, d_model = grad_hidden.shape
    half = CHIPS // 2

    def block_row(j, t):
        side = t[SP] ^ (j < half).astype(jnp.int32)
        return (side * half + (j & 1)) ^ t[DP]

    def body(t, g_ref, w_ref, far_ref, keep_ref):
        j = step_id()

        def one_core(s):
            grad = dot_nt(g_ref[:], w_ref[s]).astype(BF16)
            for cond, ref in ((j < half, far_ref), (j >= half, keep_ref)):
                @pl.when(cond)
                def _():
                    for e in range(2):
                        ref[(t[SP] ^ s) * 2 + e] = grad[:, e * PAIR:(e + 1) * PAIR]

        loop(2, one_core)

    slabs = (CHIPS, rows, PAIR)
    return call(body, ids, (grad_hidden, w_full.reshape(2, CHIPS * BLK, d_model)), CHIPS,
                [whole(grad_hidden), spec((2, BLK, d_model), fixed, block_row, fixed)],
                [spec(slabs, until(half), fixed, fixed), spec(slabs, since(half), fixed, fixed)],
                [sds((Q_PAIRS, rows, PAIR), BF16)] * 2, gflop=4.3)


def unrope_kernel(ids, keep, got, cos_t, sin_t):
    _, rows, _ = keep.shape
    tile = HALF_BLK
    cols = 2 * SLABS * PAIR

    def body(t, k_ref, g_ref, cos_ref, sin_ref, o_ref):
        for ref, side in ((k_ref, t[SP]), (g_ref, 1 - t[SP])):
            for first, count, roped in ((0, Q_PAIRS, True), (K_SLAB, KV_PAIRS, True), (V_SLAB, KV_PAIRS, False)):
                def move(p):
                    pair = ref[first + p]
                    if roped:
                        pair = rope_lanes(pair.astype(F32), cos_ref[:], sin_ref[:], -1).astype(BF16)
                    o_ref[:, part(2 * first + side * count + p, PAIR)] = pair

                loop(count, move)

    h_spec = spec((SLABS, tile, PAIR), fixed, moving, fixed)
    t_spec = spec((tile, PAIR), moving, fixed)
    return call(body, ids, (keep, got, cos_t, sin_t), rows // tile, [h_spec, h_spec, t_spec, t_spec],
                spec((tile, cols), moving, fixed), sds((rows, cols), BF16))


def input_grad_kernel(ids, grad_qkv, w_full, act, gain_rel, grad_hidden):
    rows, d_model = act.shape
    _, cols = grad_qkv.shape
    strip_rows = HALF_HEAD

    def body(t, g_ref, w_ref, x_ref, gain_ref, gh_ref, out_ref, gain_out_ref, grad):
        j = step_id()
        grad[:, part(j, BLK)] = dot_nt(g_ref[:], w_ref[:]).astype(BF16)

        @pl.when(j == PLACES - 1)
        def _():
            gain_out_ref[:] = jnp.zeros_like(gain_out_ref)
            loop(rows // strip_rows, lambda i: norm_back(t, grad, part(i, strip_rows), x_ref, gain_ref, gh_ref, out_ref, gain_out_ref))

    return call(body, ids, (grad_qkv, w_full, act, gain_rel, grad_hidden), PLACES,
                [whole(grad_qkv), spec((BLK, cols), moving, fixed), whole(act), whole(gain_rel), whole(grad_hidden)],
                [whole(act), whole(gain_rel)], [like(act), like(gain_rel)], [pltpu.VMEM((rows, d_model), BF16)], gflop=10)


def solution(mesh):
    flat_axes = ("dp", "sp")
    row_spec = P("dp", "sp", None)
    pos_spec = P("dp", "sp")
    vec_spec = P(flat_axes)
    mat_spec = P(flat_axes, None)
    cube_spec = P(flat_axes, None, None)
    hops = {"x": 1, "y": 2, "d": 3}

    def send(way, v):
        if way == "s":
            return lax.ppermute(v, "sp", [(0, 1), (1, 0)])
        return lax.ppermute(v, "dp", [(i, i ^ hops[way]) for i in range(CHIPS)])

    def gather_pieces(own, *deps):
        from_x = send("x", own)
        from_y = send("y", own)
        if deps:
            from_x, from_y = after((from_x, from_y), *deps)
        return [own, from_x, from_y, send("y", from_x[:HALF_BLK]), send("x", from_y[HALF_BLK:])]

    def both_cores(pieces):
        return pieces + [send("s", p) for p in pieces]

    def gather_rows(top, bottom):
        xa = send("x", top)
        yb = send("y", bottom)
        xb = send("x", bottom)
        ya = send("y", top)
        return [top, bottom], [xa, xb], [ya, yb], [send("y", xa), send("x", yb)]

    def scatter4(ids, halves):
        (a0, b0), (a1, b1), (a2, b2), (a3, b3) = halves
        u1 = send("x", a1)
        u2 = send("y", b2)
        t1 = send("x", a3)
        t2 = send("y", b3)
        v1 = send("x", add_kernel(ids, b1, t2))
        v2 = send("y", add_kernel(ids, a2, t1))
        return (a0, u1, v2), (b0, u2, v1)

    def layer(act_in, positions, out_grad, norm1_gain, norm2_gain, w_query, w_key, w_value, w_out, w_gate, w_up, w_down):
        dp = lax.axis_index("dp")
        sp = lax.axis_index("sp")
        _, n_q, hd = w_query.shape
        _, n_kv, _ = w_key.shape
        q_cols, kv_cols = n_q * hd, n_kv * hd
        (act,), (pos,), (dy,) = act_in, positions, out_grad
        _, d_model = act.shape
        half_d = d_model // 2
        _, f_cols = w_gate.shape
        quarter = f_cols // CHIPS
        place = jnp.arange(PLACES, dtype=jnp.int32)
        rel_table = ((place % CHIPS) ^ dp) * 2 + ((place // CHIPS) ^ sp)
        abs_table = ((place % 2) ^ sp) * CHIPS + ((place // 2) ^ dp)
        ids = jnp.concatenate([rel_table, abs_table, jnp.stack([sp, dp])]).astype(jnp.int32)

        wo_pieces = both_cores(gather_pieces(w_out))
        w_qkv = jnp.concatenate([w.reshape(BLK, -1) for w in (w_query, w_key, w_value)], axis=1)
        gains = jnp.stack([norm1_gain, norm2_gain])
        gain_mine = jnp.concatenate([gains, send("x", gains), send("y", gains), send("d", gains)], axis=1)
        gain_rel = jnp.concatenate([gain_mine, send("s", gain_mine)], axis=1).astype(F32)
        gain1_rel, gain2_rel = gain_rel[:1], gain_rel[1:]
        w2_rows, _ = w_down.shape

        def w2_at(side):
            return lambda t: (part(t[SP] ^ side, w2_rows), ALL)

        w2_pair = [w_down, send("s", w_down)]
        (w2,) = move_kernel(ids, [(i, everything, 0, w2_at(i), w_down.shape) for i in range(2)], w2_pair, [sds((2 * w2_rows, d_model), BF16)])

        inv_freq = ROPE_BASE ** (-(jnp.arange(HALF_HEAD, dtype=F32) * (1.0 / HALF_HEAD)))
        angles = pos.astype(F32)[:, None] * inv_freq
        cos_t = jnp.tile(jnp.cos(angles), (1, 4))
        sin_t = jnp.tile(jnp.sin(angles), (1, 4))
        u_rel, u_far = norm_kernel(ids, after(act, cos_t, sin_t), gain1_rel)
        u_near = send("x", u_far)
        qkv_pieces = both_cores(gather_pieces(w_qkv, u_rel, w2))

        def quarter_at(r):
            return lambda t: (ALL, part(t[DP] ^ r, quarter))

        tile_shape = (BLK, quarter)
        moves = [(i, quarter_at(r), r, row_at(i, BLK), tile_shape) for r in range(CHIPS) for i in range(2)]
        q0, q1, q2, q3 = move_kernel(ids, moves, [w_gate, w_up], [sds((2 * BLK, quarter), BF16)] * CHIPS)
        f_pieces = both_cores([q0, send("x", q1), send("y", q2), send("d", q3)])
        moves = [(i, row_at(o, BLK), o, row_at(i, BLK), tile_shape) for i in range(PLACES) for o in range(2)]
        w1, w3 = move_kernel(ids, moves, f_pieces, [sds((d_model, quarter), BF16)] * 2)

        qkv_far, qkv_keep, wqkv_full = qkv_kernel(ids, u_rel, qkv_pieces, cos_t, sin_t)
        qkv_got = send("s", qkv_far)
        o_keep, o_far = attn_fwd_kernel(ids, qkv_keep, qkv_got)
        o_got = send("s", o_far)
        attn_rel, hidden, normed_a, normed_b, wo_full, attn_far = out_proj_kernel(ids, o_keep, o_got, wo_pieces, act, gain2_rel)

        attn_near = send("y", attn_far)

        w_rows = gather_rows(normed_a, normed_b)
        dy_rows = gather_rows(dy[:HALF_TOKENS], dy[HALF_TOKENS:])
        fwd = ffn_fwd_kernel(ids, 0, [(0, w_rows[0])], w1, w3, (), 2)
        fwd = ffn_fwd_kernel(ids, 1, list(enumerate(w_rows))[1:3], w1, w3, fwd)
        y1 = ffn_y_kernel(ids, 1, fwd[1], w2)
        bwd = ffn_bwd_kernel(ids, 1, dy_rows[1] + dy_rows[2], fwd[2], fwd[3], w2, ())
        dw1 = ffn_dw_kernel(ids, 1, (1, 2), bwd[1], bwd[2], w1, w3)
        w_all, mixed, gate_pre, up_pre = ffn_fwd_kernel(ids, 1, [(3, w_rows[3])], w1, w3, fwd)
        dy_all, dgate, dup = ffn_bwd_kernel(ids, 0, [dy] + dy_rows[3], gate_pre, up_pre, w2, bwd)
        dw0 = ffn_dw_kernel(ids, 0, (0, 3), dgate, dup, w1, w3)
        y0 = ffn_y_kernel(ids, 0, mixed, w2)

        def by_chip(pair0, pair1):
            return [pair0[:2], pair1[:2], pair1[2:], pair0[2:]]

        dw_top, dw_bottom = scatter4(ids, by_chip(dw0, dw1))
        y_top, y_bottom = scatter4(ids, by_chip(y0, y1))
        (y_base,) = sum_kernel(ids, y_top[:2], y_bottom[:2], (d_model,), hidden)

        def both_grads(near, far, n_blocks, parts):
            (sent,) = weight_grad_kernel(ids, far, n_blocks, None, 0)
            return weight_grad_kernel(ids, near, n_blocks, send("s", sent), parts)

        def column_grad(grad_all):
            own, *rest = both_grads([(w_all, later(0), grad_all)], [(w_all, later(CHIPS), grad_all)], CHIPS, 1)
            return [own] + [send(way, v) for way, v in zip("xyd", rest)]

        def placed(pieces):
            return move_kernel(ids, [(r, everything, 0, quarter_at(r), tile_shape) for r in range(CHIPS)], pieces, [sds((BLK, f_cols), F32)])

        gate_pieces = column_grad(dgate)
        up_pieces = column_grad(dup)
        (down_grad,) = both_grads([(mixed, lambda j, t: t[SP] * CHIPS + j, dy_all)], [(mixed, lambda j, t: (1 - t[SP]) * CHIPS + j, dy_all)], CHIPS, 0)
        (gate_grad,) = placed(gate_pieces)
        (up_grad,) = placed(up_pieces)

        grad_hidden, gain2_part = hidden_grad_kernel(ids, dw_top, dw_bottom, hidden, gain2_rel, dy)

        def row_grad(k, way, left, left_near, right, right_near):
            blocks = here_blocks(k)
            first, second, *_ = blocks
            stride = second - first
            half = len(blocks) // 2
            near = [(left, later(0, stride), right), (left_near, later(0), right_near)]
            far = [(left, later(CHIPS, stride), right), (left_near, later(half), right_near)]
            own_top, own_bottom, top, bottom = both_grads(near, far, half, 2)
            return (own_top, send(way, top)), (own_bottom, send(way, bottom))

        do_far, do_keep = attn_grad_kernel(ids, grad_hidden, wo_full)
        do_got = send("s", do_far)
        d_keep, d_far = attn_bwd_kernel(ids, qkv_keep, qkv_got, do_keep, do_got)
        d_got = send("s", d_far)
        hidden_near = send("y", grad_hidden)
        wo_top, wo_bottom = row_grad(2, "x", attn_rel, attn_near, grad_hidden, hidden_near)
        (wout_grad,) = sum_kernel(ids, wo_top, wo_bottom, (d_model,))
        grad_qkv = unrope_kernel(ids, d_keep, d_got, cos_t, sin_t)
        qkv_near = send("x", grad_qkv)
        qkv_top, qkv_bottom = row_grad(1, "y", u_rel, u_near, grad_qkv, qkv_near)
        q_grad, k_grad, v_grad = sum_kernel(ids, qkv_top, qkv_bottom, (q_cols, kv_cols, kv_cols))
        query_grad = q_grad.reshape(w_query.shape)
        key_grad = k_grad.reshape(w_key.shape)
        value_grad = v_grad.reshape(w_value.shape)
        y_base = after(y_base, query_grad, key_grad, value_grad, wout_grad)
        (act_out,) = sum_kernel(ids, y_top[2:], y_bottom[2:], (d_model,), y_base, BF16)
        in_grad, gain1_part = input_grad_kernel(ids, grad_qkv, wqkv_full, act, gain1_rel, grad_hidden)

        gain_part = jnp.concatenate([gain1_part, gain2_part], axis=0)
        gain_half = gain_part[:, :half_d] + send("s", gain_part[:, half_d:])
        own, to_x, to_y, to_d = [gain_half[:, cols_of(r)] for r in range(CHIPS)]
        gain1_grad, gain2_grad = own + send("x", to_x) + send("y", to_y) + send("d", to_d)
        return (act_out[None], in_grad[None], gain1_grad, gain2_grad, query_grad, key_grad, value_grad, wout_grad, gate_grad, up_grad, down_grad)

    return jax.shard_map(layer, mesh=mesh, in_specs=(row_spec, pos_spec, row_spec, vec_spec, vec_spec, cube_spec, cube_spec, cube_spec, mat_spec, mat_spec, mat_spec, mat_spec), out_specs=(row_spec, row_spec, vec_spec, vec_spec, cube_spec, cube_spec, cube_spec, mat_spec, mat_spec, mat_spec, mat_spec), check_vma=False)
```

```python
import jax
import jax.numpy as jnp
from jax import lax
from jax.experimental import pallas as pl
from jax.experimental.pallas import tpu as pltpu
from jax.sharding import PartitionSpec as P

INTERPRET = False

EPS = 1e-5
ROPE_BASE = 10000.0
NEG_BIG = -1e30
F32 = jnp.float32
BF16 = jnp.bfloat16
CHIPS = 4
PLACES = 8
BLK = 256
HALF_BLK = BLK // 2
TOKENS = 512
HALF_TOKENS = TOKENS // 2
HEAD = 64
HALF_HEAD = HEAD // 2
PAIR = 2 * HEAD
ATTN_SCALE = HEAD ** -0.5
GROUPS = 4
GROUP_HEADS = 4
Q_PAIRS = 8
KV_PAIRS = 2
K_SLAB = Q_PAIRS
V_SLAB = K_SLAB + KV_PAIRS
SLABS = V_SLAB + KV_PAIRS
ALL = slice(None)
MANY = pltpu.SemaphoreType.DMA


def dot(a, b):
    return lax.dot_general(a, b, (((1,), (0,)), ((), ())), preferred_element_type=F32)


def dot_nt(a, b):
    return lax.dot_general(a, b, (((1,), (1,)), ((), ())), preferred_element_type=F32)


def dot_tn(a, b):
    return lax.dot_general(a, b, (((0,), (0,)), ((), ())), preferred_element_type=F32)


def after(value, *deps):
    first, *_ = lax.optimization_barrier((value,) + deps)
    return first


def sds(shape, dtype):
    return jax.ShapeDtypeStruct(shape, dtype)


def like(v):
    return sds(v.shape, v.dtype)


def fixed(j, t):
    return 0


def moving(j, t):
    return j


def until(n):
    return lambda j, t: jnp.minimum(j, n - 1)


def since(n):
    return lambda j, t: jnp.maximum(j - n, 0)


def always(n):
    return lambda j, t: n


def spec(shape, *index):
    return pl.BlockSpec(shape, lambda j, t: tuple(f(j, t) for f in index))


def whole(v):
    return spec(v.shape, *[fixed] * len(v.shape))


def anywhere(n):
    return [pl.BlockSpec(memory_space=pl.ANY)] * n


def call(body, ids, args, grid, in_specs, out_specs, out_shape, scratch=(), gflop=1.0, aliases=None):
    return pl.pallas_call(
        body,
        out_shape=out_shape,
        grid_spec=pltpu.PrefetchScalarGridSpec(num_scalar_prefetch=1, grid=(grid,), in_specs=in_specs, out_specs=out_specs, scratch_shapes=list(scratch)),
        cost_estimate=pl.CostEstimate(flops=int(gflop * 1e9), bytes_accessed=int(1e7), transcendentals=0),
        compiler_params=pltpu.CompilerParams(dimension_semantics=("arbitrary",)),
        input_output_aliases=aliases or {},
        interpret=INTERPRET,
    )(ids, *args)


def step_id():
    return pl.program_id(0)


def loop(count, body):
    def one(i, carry):
        body(i)
        return carry

    lax.fori_loop(0, count, one, 0)


SP = 2 * PLACES
DP = SP + 1


def part(index, size):
    return pl.ds(pl.multiple_of(index * size, size), size)


def cols_of(p):
    return slice(p * BLK, (p + 1) * BLK)


def row_sum(v):
    return jnp.sum(v, axis=-1, keepdims=True)


def row_scale(x):
    return lax.rsqrt(row_sum(x * x) * (1.0 / x.shape[-1]) + EPS)


def write_normed(t, src, rows, gain, out, out_rows):
    scale = row_scale(src[rows, :].astype(F32))
    for p in range(PLACES):
        blk = src[rows, part(t[p], BLK)].astype(F32)
        out[out_rows, cols_of(p)] = (blk * scale * gain[:, cols_of(p)]).astype(BF16)


def to_neighbour(k):
    return [p for p in range(PLACES) if p & k]


def here_blocks(k):
    return [p for p in range(PLACES) if not p & k]


def copy_blocks(dst, src, places):
    for i, p in enumerate(places):
        dst[:, cols_of(i)] = src[:, cols_of(p)]


def norm_kernel(ids, act, gain_rel):
    rows, cols = act.shape
    tile = HALF_BLK

    def body(t, x_ref, g_ref, o_ref, send_ref):
        write_normed(t, x_ref, ALL, g_ref, o_ref, ALL)
        copy_blocks(send_ref, o_ref, to_neighbour(1))

    io = spec((tile, cols), moving, fixed)
    return call(body, ids, (act, gain_rel), rows // tile, [io, whole(gain_rel)],
                [io, spec((tile, cols // 2), moving, fixed)], [like(act), sds((rows, cols // 2), BF16)])


def rope_lanes(values, cos_t, sin_t, sign):
    width = values.shape[-1]
    reps = width // PAIR
    if reps > 1:
        cos_t = jnp.concatenate([cos_t] * reps, axis=1)
        sin_t = jnp.concatenate([sin_t] * reps, axis=1)
    lane = lax.broadcasted_iota(jnp.int32, values.shape, 1)
    up_roll = pltpu.roll(values, width - HALF_HEAD, 1)
    down_roll = pltpu.roll(values, HALF_HEAD, 1)
    other = jnp.where((lane & (HEAD - 1)) < HALF_HEAD, -up_roll, down_roll)
    return values * cos_t + (other * sin_t if sign > 0 else -(other * sin_t))


def fill(scratch, refs):
    start = 0
    for ref in refs:
        n, _ = ref.shape
        scratch[start:start + n, :] = ref[:]
        start += n


def qkv_kernel(ids, u_rel, pieces, cos_t, sin_t):
    rows, d_model = u_rel.shape
    cols = pieces[0].shape[1]
    n_pieces = len(pieces)
    tiles = SLABS // 2
    q_tiles = Q_PAIRS // 2

    def column(j, t):
        far = (j < tiles).astype(jnp.int32)
        half = t[SP] ^ far
        tile = j - tiles * (1 - far)
        return jnp.where(tile < q_tiles, half * q_tiles + tile, 2 * tile + half)

    def body(t, u_ref, cos_ref, sin_ref, *refs):
        far_ref, keep_ref, w_ref = refs[n_pieces:]
        j = step_id()
        fill(w_ref, refs[:n_pieces])
        acc = dot(u_ref[:], w_ref[:])
        roped = rope_lanes(acc, cos_ref[:], sin_ref[:], 1)
        is_value = (j == tiles - 1) | (j == 2 * tiles - 1)
        out = jnp.where(is_value, acc, roped).astype(BF16)
        for cond, ref in ((j < tiles, far_ref), (j >= tiles, keep_ref)):
            @pl.when(cond)
            def _():
                for e in range(2):
                    ref[e] = out[:, e * PAIR:(e + 1) * PAIR]

    w_specs = [spec((p.shape[0], BLK), fixed, column) for p in pieces]
    slab = (2, rows, PAIR)
    return call(body, ids, (u_rel, cos_t, sin_t) + tuple(pieces), 2 * tiles,
                [whole(u_rel), whole(cos_t), whole(sin_t)] + w_specs,
                [spec(slab, until(tiles), fixed, fixed), spec(slab, since(tiles), fixed, fixed), spec((d_model, BLK), fixed, column)],
                [sds((SLABS, rows, PAIR), BF16)] * 2 + [sds((d_model, cols), BF16)], gflop=6.5)


def core_rows(t, rows):
    return part(t[SP], rows), part(1 - t[SP], rows)


def in_order(t, ref, own, other):
    for here, v in zip(core_rows(t, own.shape[0]), (own, other)):
        ref[here, :] = v


def one_head(pair, odd):
    return jnp.where(odd == 1, pair[:, HEAD:], pair[:, :HEAD])


def softmax_rows(q_tile, keys, first_row, span):
    scores = dot_nt(q_tile, keys) * ATTN_SCALE
    edge = span - BLK
    shape = (q_tile.shape[0], BLK)
    row = lax.broadcasted_iota(jnp.int32, shape, 0) + first_row
    col = lax.broadcasted_iota(jnp.int32, shape, 1)
    last = jnp.where(row >= col, scores[:, edge:], NEG_BIG)
    scores = jnp.concatenate([scores[:, :edge], last], axis=1) if edge else last
    expo = jnp.exp(scores - jnp.max(scores, axis=-1, keepdims=True))
    return expo * (1.0 / row_sum(expo))


def head_specs(rows):
    slabs = (2, rows, PAIR)
    one = (1, rows, PAIR)
    q_spec = spec(slabs, moving, fixed, fixed)
    return q_spec, [q_spec] + [spec(one, lambda j, t, base=base: base + j // 2, fixed, fixed) for base in (K_SLAB, V_SLAB)]


def attn_fwd_kernel(ids, keep, got):
    _, rows, _ = keep.shape
    seq = 2 * rows

    def body(t, qk_ref, kk_ref, vk_ref, qg_ref, kg_ref, vg_ref, keep_ref, send_ref, ks, vs, qs, os):
        odd = step_id() & 1
        in_order(t, ks, one_head(kk_ref[0], odd), one_head(kg_ref[0], odd))
        in_order(t, vs, one_head(vk_ref[0], odd), one_head(vg_ref[0], odd))

        def head(h):
            in_order(t, qs, one_head(qk_ref[h // 2], h & 1), one_head(qg_ref[h // 2], h & 1))
            for span in range(BLK, seq + BLK, BLK):
                prob = softmax_rows(qs[span - BLK:span, :], ks[:span, :], 0, span).astype(BF16)
                os[h, span - BLK:span, :] = dot(prob, vs[:span, :]).astype(BF16)

        loop(GROUP_HEADS, head)
        for here, ref in zip(core_rows(t, rows), (keep_ref, send_ref)):
            for p in range(2):
                ref[p] = jnp.concatenate([os[2 * p, here, :], os[2 * p + 1, here, :]], axis=1)

    q_spec, specs = head_specs(rows)
    return call(body, ids, (keep,) * 3 + (got,) * 3, GROUPS, specs * 2,
                [q_spec] * 2, [sds((Q_PAIRS, rows, PAIR), BF16)] * 2,
                [pltpu.VMEM((seq, HEAD), BF16)] * 3 + [pltpu.VMEM((GROUP_HEADS, seq, HEAD), BF16)], gflop=20)


def attn_bwd_kernel(ids, keep, got, do_keep, do_got):
    _, rows, _ = keep.shape
    seq = 2 * rows
    strip_rows = BLK

    def body(t, qk_ref, kk_ref, vk_ref, dk_ref, qg_ref, kg_ref, vg_ref, dg_ref, keep_ref, send_ref, ks, vs, qs, ds, dqs, dks, dvs):
        g = step_id()
        odd = g & 1
        in_order(t, ks, one_head(kk_ref[0], odd), one_head(kg_ref[0], odd))
        in_order(t, vs, one_head(vk_ref[0], odd), one_head(vg_ref[0], odd))
        dks[odd] = jnp.zeros_like(ks, F32)
        dvs[odd] = jnp.zeros_like(vs, F32)

        def head(h):
            in_order(t, qs, one_head(qk_ref[h // 2], h & 1), one_head(qg_ref[h // 2], h & 1))
            in_order(t, ds, one_head(dk_ref[h // 2], h & 1), one_head(dg_ref[h // 2], h & 1))
            for span in range(BLK, seq + BLK, BLK):
                def strip(n):
                    here = part((span - BLK) // strip_rows + n, strip_rows)
                    q_tile = qs[here, :]
                    do_tile = ds[here, :]
                    prob = softmax_rows(q_tile, ks[:span, :], n * strip_rows, span)
                    grad_prob = dot_nt(do_tile, vs[:span, :])
                    inner = row_sum(prob * grad_prob)
                    grad_scores = (prob * (grad_prob - inner) * ATTN_SCALE).astype(BF16)
                    dqs[h, here, :] = dot(grad_scores, ks[:span, :]).astype(BF16)
                    dks[odd, :span, :] += dot_tn(grad_scores, q_tile)
                    dvs[odd, :span, :] += dot_tn(prob.astype(BF16), do_tile)

                loop(BLK // strip_rows, strip)

        loop(GROUP_HEADS, head)
        for here, ref in zip(core_rows(t, rows), (keep_ref, send_ref)):
            for p in range(2):
                ref[2 * g + p] = jnp.concatenate([dqs[2 * p, here, :], dqs[2 * p + 1, here, :]], axis=1)

            @pl.when(odd == 1)
            def _():
                for base, acc in ((K_SLAB, dks), (V_SLAB, dvs)):
                    ref[base + g // 2] = jnp.concatenate([acc[0, here, :], acc[1, here, :]], axis=1).astype(BF16)

    q_spec, specs = head_specs(rows)
    return call(body, ids, (keep,) * 3 + (do_keep,) + (got,) * 3 + (do_got,), GROUPS, (specs + [q_spec]) * 2,
                [whole(keep)] * 2, [like(keep)] * 2,
                [pltpu.VMEM((seq, HEAD), BF16)] * 4 + [pltpu.VMEM((GROUP_HEADS, seq, HEAD), BF16)] + [pltpu.VMEM((2, seq, HEAD), F32)] * 2, gflop=50)


def out_proj_kernel(ids, o_keep, o_got, pieces, act, gain_rel):
    rows, d_model = act.shape
    tile = BLK
    strip_rows = HALF_HEAD
    n_pieces = len(pieces)

    def body(t, ok_ref, og_ref, x_ref, g_ref, *refs):
        a_ref, h_ref, normed_ref, w_ref, send_ref, a_abs = refs[n_pieces:]
        j = step_id()

        @pl.when(j == 0)
        def _():
            for ref, side in ((ok_ref, t[SP]), (og_ref, 1 - t[SP])):
                for p in range(Q_PAIRS):
                    a_abs[:, part(side * Q_PAIRS + p, PAIR)] = ref[p]
            for p in range(PLACES):
                a_ref[:, cols_of(p)] = a_abs[:, part(t[p], BLK)]
            copy_blocks(send_ref, a_ref, to_neighbour(2))

        fill(w_ref, refs[:n_pieces])
        acc = dot(a_ref[:], w_ref[:])
        cols = part(j, tile)
        h_ref[:, cols] = (x_ref[:, cols].astype(F32) + acc).astype(BF16)

        @pl.when(j == d_model // tile - 1)
        def _():
            def normed(i):
                here = part(i, strip_rows)
                write_normed(t, h_ref, here, g_ref, normed_ref, here)

            loop(rows // strip_rows, normed)

    w_specs = [spec((p.shape[0], tile), fixed, moving) for p in pieces]
    send = sds((rows, d_model // 2), BF16)
    return call(body, ids, (o_keep, o_got, act, gain_rel) + tuple(pieces), d_model // tile,
                [whole(o_keep), whole(o_got), whole(act), whole(gain_rel)] + w_specs,
                [whole(act)] * 3 + [spec((d_model, tile), fixed, moving), whole(send)],
                [like(act)] * 3 + [sds((d_model, d_model), BF16), send], [pltpu.VMEM((rows, d_model), BF16)], gflop=4.3)


def swapped(place, k):
    return place ^ k


def pair_spec(cols):
    return spec((2 * TOKENS, cols), fixed, fixed)


def ffn_fwd_kernel(ids, place, parts, w1, w3, buffers, strip_rows):
    d_model, f_cols = w1.shape
    tile = BLK
    owners = [k for k, _ in parts] if parts else []
    arrays = [v for _, v in parts] if parts else list(buffers)
    rows = sum(v.shape[0] for v in arrays) if parts else 2 * TOKENS
    total = CHIPS * TOKENS if parts else rows
    aliased = list(buffers) if parts else []
    n_in = len(arrays)

    def body(t, *refs):
        w1_ref, w3_ref = refs[n_in:n_in + 2]
        *own, m_ref, act_ref, slope_ref = refs[n_in + 2 + len(aliased):]
        (wall_ref,) = own if parts else refs[:1]

        if parts:
            @pl.when(step_id() == 0)
            def _():
                start = 0
                for k, ref in zip(owners, refs):
                    n, _ = ref.shape
                    for p in range(PLACES):
                        wall_ref[start:start + n, cols_of(p)] = ref[:, cols_of(swapped(p, k))]
                    start += n

        def strip(n):
            here = part(n, strip_rows)
            gate = dot(wall_ref[here, :], w1_ref[:])
            up = dot(wall_ref[here, :], w3_ref[:])
            sig = jax.nn.sigmoid(gate)
            act = gate * sig
            act_ref[here, :] = act
            slope_ref[here, :] = up * sig * (1.0 + gate * (1.0 - sig))
            m_ref[here, :] = (act * up).astype(BF16)

        loop(rows // strip_rows, strip)

    w_spec = spec((d_model, tile), fixed, moving)
    tile_spec = spec((rows, tile), always(place), moving)
    out_specs = [tile_spec] * 3
    out_shape = [sds((total, f_cols), BF16)] + [sds((total, f_cols), F32)] * 2
    if parts:
        out_specs = [spec((rows, d_model), always(place), fixed)] + out_specs
        out_shape = [sds((total, d_model), BF16)] + out_shape
    in_specs = ([whole(v) for v in arrays] if parts else [pair_spec(d_model)]) + [w_spec] * 2 + anywhere(len(aliased))
    return call(body, ids, tuple(arrays) + (w1, w3) + tuple(aliased), f_cols // tile, in_specs, out_specs, out_shape,
                gflop=8.6, aliases={n_in + 3 + i: i for i in range(len(aliased))})


def ffn_bwd_kernel(ids, place, parts, act, slope, w2, buffers, strip_rows):
    f_cols, d_model = w2.shape
    tile = BLK
    arrays = list(parts) if parts else list(buffers)
    rows = sum(v.shape[0] for v in arrays) if parts else 2 * TOKENS
    total = CHIPS * TOKENS if parts else rows
    aliased = list(buffers) if parts else []
    n_in = len(arrays)

    def body(t, *refs):
        act_ref, slope_ref, w2_ref = refs[n_in:n_in + 3]
        *own, dg_ref, du_ref = refs[n_in + 3 + len(aliased):]
        (dyall_ref,) = own if parts else refs[:1]

        if parts:
            @pl.when(step_id() == 0)
            def _():
                fill(dyall_ref, refs[:n_in])

        def strip(n):
            here = part(n, strip_rows)
            back = dot_nt(dyall_ref[here, :], w2_ref[:]).astype(BF16).astype(F32)
            du_ref[here, :] = (back * act_ref[here, :]).astype(BF16)
            dg_ref[here, :] = (back * slope_ref[here, :]).astype(BF16)

        loop(rows // strip_rows, strip)

    tile_spec = spec((rows, tile), always(place), moving)
    out_specs = [tile_spec] * 2
    out_shape = [sds((total, f_cols), BF16)] * 2
    if parts:
        out_specs = [spec((rows, d_model), always(place), fixed)] + out_specs
        out_shape = [sds((total, d_model), BF16)] + out_shape
    in_specs = ([whole(v) for v in arrays] if parts else [pair_spec(d_model)]) + [tile_spec] * 2 + [spec((tile, d_model), moving, fixed)] + anywhere(len(aliased))
    return call(body, ids, tuple(arrays) + (act, slope, w2) + tuple(aliased), f_cols // tile, in_specs, out_specs, out_shape,
                gflop=8.6, aliases={n_in + 4 + i: i for i in range(len(aliased))})


def write_chips(outs, value, accs):
    for i, out in enumerate(outs):
        rows = value[i * TOKENS:(i + 1) * TOKENS]
        out[:] = rows + accs[i][:] if accs else rows


def ffn_dw_kernel(ids, dgate, dup, w1, w3, accs):
    d_model, f_cols = w1.shape

    def body(t, dg_ref, du_ref, w1_ref, w3_ref, *refs):
        write_chips(refs[len(accs):], dot_nt(dg_ref[:], w1_ref[:]) + dot_nt(du_ref[:], w3_ref[:]), refs[:len(accs)])

    w_spec = spec((BLK, f_cols), moving, fixed)
    out_specs = [spec((TOKENS, BLK), fixed, lambda j, t, k=k: j ^ k) for k in range(2)]
    return call(body, ids, (dgate, dup, w1, w3) + tuple(accs), d_model // BLK, [pair_spec(f_cols)] * 2 + [w_spec] * 2 + out_specs[:len(accs)],
                out_specs, [sds((TOKENS, d_model), F32)] * 2, gflop=17)


def ffn_y_kernel(ids, mixed, w2, accs):
    f_cols, d_model = w2.shape

    def body(t, m_ref, w2_ref, *refs):
        write_chips(refs[len(accs):], dot(m_ref[:], w2_ref[:]), refs[:len(accs)])

    out_specs = [spec((TOKENS, BLK), fixed, moving)] * 2
    return call(body, ids, (mixed, w2) + tuple(accs), d_model // BLK, [pair_spec(f_cols), spec((f_cols, BLK), fixed, moving)] + out_specs[:len(accs)],
                out_specs, [sds((TOKENS, d_model), F32)] * 2, gflop=8.6)


def weight_grad_kernel(ids, pairs, n_blocks, received, parts):
    rows, cols = pairs[0][-1].shape
    per = max(parts, 1)
    sub = BLK // per
    tile = TOKENS
    out_shape = [sds((sub, cols), F32)] * (n_blocks * parts) if parts else [sds((n_blocks * BLK, cols), F32)]
    n_out = len(out_shape)
    n_ops = 2 * len(pairs)

    def body(t, *refs):
        j = step_id()
        *ins, flipped, total, sem = refs
        outs = ins[len(ins) - n_out:]
        slot = j & 1
        for i in range(len(pairs)):
            flipped[i] = ins[2 * i][:].T

        def copies(r, slot):
            if not parts:
                return [pltpu.make_async_copy(total.at[slot], outs[0].at[part(r, BLK), :], sem.at[slot, 0])]
            return [pltpu.make_async_copy(total.at[slot, pl.ds(i * sub, sub), :], outs[r * parts + i], sem.at[slot, i]) for i in range(parts)]

        def drain(slot):
            for copy in copies(0, slot):
                copy.wait()

        @pl.when(j >= 2)
        def _():
            drain(slot)

        def tile_step(n):
            here = part(n, tile)
            terms = [dot(flipped[i], ins[2 * i + 1][:, here]) for i in range(len(pairs))]
            if received is not None:
                terms.append(ins[n_ops][:, here])
            total[slot, :, here] = sum(terms[1:], terms[0])

        loop(cols // tile, tile_step)
        if parts:
            for r in range(n_blocks):
                @pl.when(j == r)
                def _():
                    for copy in copies(r, slot):
                        copy.start()
        else:
            for copy in copies(j, slot):
                copy.start()

        @pl.when(j == n_blocks - 1)
        def _():
            drain(1 - slot)
            drain(slot)

    in_specs, args = [], ()
    for left, block, right in pairs:
        in_specs += [spec((left.shape[0], BLK), fixed, block), whole(right)]
        args += (left, right)
    if received is not None:
        in_specs.append(spec((BLK, cols), moving, fixed))
        args += (received,)
    return call(body, ids, args, n_blocks, in_specs, anywhere(n_out), out_shape,
                [pltpu.VMEM((len(pairs), BLK, rows), BF16), pltpu.VMEM((2, BLK, cols), F32), MANY((2, per))], gflop=8.6)


def later(first, stride=1):
    return lambda j, t: first + stride * j


def sum_kernel(ids, terms, widths, dtype=F32):
    n = len(terms)
    rows, cols = terms[0].shape
    tile = rows // CHIPS

    def body(t, *refs):
        start = 0
        for width, out in zip(widths, refs[n:]):
            cut = slice(start, start + width)
            first, *rest = [ref[:, cut].astype(F32) for ref in refs[:n]]
            out[:] = sum(rest, first).astype(dtype)
            start += width

    return call(body, ids, tuple(terms), CHIPS, [spec((tile, cols), moving, fixed)] * n,
                [spec((tile, w), moving, fixed) for w in widths], [sds((rows, w), dtype) for w in widths])


def move_kernel(ids, moves, sources, out_shapes):
    n_src, n_out, n = len(sources), len(out_shapes), len(moves)

    def body(t, *refs):
        srcs, outs = refs[:n_src], refs[n_src:n_src + n_out]
        *bufs, in_sem, out_sem = refs[n_src + n_out:]
        loads, stores = [], []
        for i, (src, src_at, out, out_at, _) in enumerate(moves):
            loads.append(pltpu.make_async_copy(srcs[src].at[src_at(t)], bufs[i], in_sem.at[i]))
            stores.append(pltpu.make_async_copy(bufs[i], outs[out].at[out_at(t)], out_sem.at[i]))
        for load in loads:
            load.start()
        for load, store in zip(loads, stores):
            load.wait()
            store.start()
        for store in stores:
            store.wait()

    shapes = [pltpu.VMEM(shape, sources[src].dtype) for src, _, _, _, shape in moves]
    return call(body, ids, tuple(sources), 1, anywhere(n_src), anywhere(n_out), list(out_shapes), shapes + [MANY((n,))] * 2)


def everything(t):
    return ALL, ALL


def row_at(index, size):
    return lambda t: (slice(index * size, (index + 1) * size), ALL)


def norm_back(t, grad_ref, rows, src_ref, gain_ref, base_ref, out_ref, gain_out_ref):
    src = src_ref[rows, :].astype(F32)
    scale = row_scale(src)
    inner = jnp.zeros_like(scale)
    for p in range(PLACES):
        cols = cols_of(p)
        unit = src_ref[rows, part(t[p], BLK)].astype(F32) * scale
        grad = grad_ref[rows, cols].astype(F32)
        gain_out_ref[:, cols] += jnp.sum(grad * unit, axis=0, keepdims=True)
        inner += row_sum(grad * gain_ref[:, cols] * unit)
    inner = inner * (1.0 / src.shape[-1])
    for p in range(PLACES):
        cols = cols_of(p)
        place = part(t[p], BLK)
        unit = src_ref[rows, place].astype(F32) * scale
        grad_rows = scale * (grad_ref[rows, cols].astype(F32) * gain_ref[:, cols] - unit * inner)
        out_ref[rows, place] = (base_ref[rows, place].astype(F32) + grad_rows).astype(BF16)


def hidden_grad_kernel(ids, own, got, hidden, gain_rel, dy):
    rows, d_model = hidden.shape
    tile = HEAD

    def body(t, own_ref, got_ref, h_ref, g_ref, dy_ref, out_ref, gain_ref, grad):
        @pl.when(step_id() == 0)
        def _():
            gain_ref[:] = jnp.zeros_like(gain_ref)

        grad[:] = (own_ref[:] + got_ref[:]).astype(BF16)
        norm_back(t, grad, ALL, h_ref, g_ref, dy_ref, out_ref, gain_ref)

    shape = (tile, d_model)
    row_spec = spec(shape, moving, fixed)
    return call(body, ids, (own, got, hidden, gain_rel, dy), rows // tile, [row_spec] * 3 + [whole(gain_rel), row_spec],
                [row_spec, whole(gain_rel)], [like(hidden), like(gain_rel)], [pltpu.VMEM(shape, BF16)], gflop=5)


def attn_grad_kernel(ids, grad_hidden, w_full):
    rows, d_model = grad_hidden.shape
    half = CHIPS // 2

    def block_row(j, t):
        side = t[SP] ^ (j < half).astype(jnp.int32)
        return (side * half + (j & 1)) ^ t[DP]

    def body(t, g_ref, w_ref, far_ref, keep_ref):
        j = step_id()

        def one_core(s):
            grad = dot_nt(g_ref[:], w_ref[s]).astype(BF16)
            for cond, ref in ((j < half, far_ref), (j >= half, keep_ref)):
                @pl.when(cond)
                def _():
                    for e in range(2):
                        ref[(t[SP] ^ s) * 2 + e] = grad[:, e * PAIR:(e + 1) * PAIR]

        loop(2, one_core)

    slabs = (CHIPS, rows, PAIR)
    return call(body, ids, (grad_hidden, w_full.reshape(2, CHIPS * BLK, d_model)), CHIPS,
                [whole(grad_hidden), spec((2, BLK, d_model), fixed, block_row, fixed)],
                [spec(slabs, until(half), fixed, fixed), spec(slabs, since(half), fixed, fixed)],
                [sds((Q_PAIRS, rows, PAIR), BF16)] * 2, gflop=4.3)


def unrope_kernel(ids, keep, got, cos_t, sin_t):
    _, rows, _ = keep.shape
    tile = HALF_BLK
    cols = 2 * SLABS * PAIR

    def body(t, k_ref, g_ref, cos_ref, sin_ref, o_ref):
        for ref, side in ((k_ref, t[SP]), (g_ref, 1 - t[SP])):
            for first, count, roped in ((0, Q_PAIRS, True), (K_SLAB, KV_PAIRS, True), (V_SLAB, KV_PAIRS, False)):
                def move(p):
                    pair = ref[first + p]
                    if roped:
                        pair = rope_lanes(pair.astype(F32), cos_ref[:], sin_ref[:], -1).astype(BF16)
                    o_ref[:, part(2 * first + side * count + p, PAIR)] = pair

                loop(count, move)

    h_spec = spec((SLABS, tile, PAIR), fixed, moving, fixed)
    t_spec = spec((tile, PAIR), moving, fixed)
    return call(body, ids, (keep, got, cos_t, sin_t), rows // tile, [h_spec, h_spec, t_spec, t_spec],
                spec((tile, cols), moving, fixed), sds((rows, cols), BF16))


def input_grad_kernel(ids, grad_qkv, w_full, act, gain_rel, grad_hidden):
    rows, d_model = act.shape
    _, cols = grad_qkv.shape
    strip_rows = HALF_HEAD

    def body(t, g_ref, w_ref, x_ref, gain_ref, gh_ref, out_ref, gain_out_ref, grad):
        j = step_id()
        grad[:, part(j, BLK)] = dot_nt(g_ref[:], w_ref[:]).astype(BF16)

        @pl.when(j == PLACES - 1)
        def _():
            gain_out_ref[:] = jnp.zeros_like(gain_out_ref)
            loop(rows // strip_rows, lambda i: norm_back(t, grad, part(i, strip_rows), x_ref, gain_ref, gh_ref, out_ref, gain_out_ref))

    return call(body, ids, (grad_qkv, w_full, act, gain_rel, grad_hidden), PLACES,
                [whole(grad_qkv), spec((BLK, cols), moving, fixed), whole(act), whole(gain_rel), whole(grad_hidden)],
                [whole(act), whole(gain_rel)], [like(act), like(gain_rel)], [pltpu.VMEM((rows, d_model), BF16)], gflop=10)


def solution(mesh):
    flat_axes = ("dp", "sp")
    row_spec = P("dp", "sp", None)
    pos_spec = P("dp", "sp")
    vec_spec = P(flat_axes)
    mat_spec = P(flat_axes, None)
    cube_spec = P(flat_axes, None, None)
    hops = {"x": 1, "y": 2, "d": 3}

    def send(way, v):
        if way == "s":
            return lax.ppermute(v, "sp", [(0, 1), (1, 0)])
        return lax.ppermute(v, "dp", [(i, i ^ hops[way]) for i in range(CHIPS)])

    def gather_weight(own, *deps):
        from_x = send("x", own)
        from_y = send("y", own)
        return [own, from_x, from_y, send("x", after(from_y, *deps) if deps else from_y)]

    def both_cores(pieces):
        return pieces + [send("s", p) for p in pieces]

    def gather_rows(own):
        from_x = send("x", own)
        from_y = send("y", own)
        return [own, from_x, from_y, send("y", from_x)]

    def layer(act_in, positions, out_grad, norm1_gain, norm2_gain, w_query, w_key, w_value, w_out, w_gate, w_up, w_down):
        dp = lax.axis_index("dp")
        sp = lax.axis_index("sp")
        _, n_q, hd = w_query.shape
        _, n_kv, _ = w_key.shape
        q_cols, kv_cols = n_q * hd, n_kv * hd
        (act,), (pos,), (dy,) = act_in, positions, out_grad
        _, d_model = act.shape
        half_d = d_model // 2
        _, f_cols = w_gate.shape
        quarter = f_cols // CHIPS
        place = jnp.arange(PLACES, dtype=jnp.int32)
        rel_table = ((place % CHIPS) ^ dp) * 2 + ((place // CHIPS) ^ sp)
        abs_table = ((place % 2) ^ sp) * CHIPS + ((place // 2) ^ dp)
        ids = jnp.concatenate([rel_table, abs_table, jnp.stack([sp, dp])]).astype(jnp.int32)

        wo_pieces = both_cores(gather_weight(w_out, ids))
        w_qkv = jnp.concatenate([w.reshape(BLK, -1) for w in (w_query, w_key, w_value)], axis=1)
        gains = jnp.stack([norm1_gain, norm2_gain])
        gain_mine = jnp.concatenate([gains, send("x", gains), send("y", gains), send("d", gains)], axis=1)
        gain_rel = jnp.concatenate([gain_mine, send("s", gain_mine)], axis=1).astype(F32)
        gain1_rel, gain2_rel = gain_rel[:1], gain_rel[1:]
        w2_rows, _ = w_down.shape

        def ordered_w2(own, other):
            moves, sources = [], []
            for side, pieces in enumerate((own, other)):
                start = 0
                for piece in pieces:
                    n, _ = piece.shape
                    moves.append((len(sources), everything, 0, w2_at(side, start, n), piece.shape))
                    sources.append(piece)
                    start += n
            return move_kernel(ids, moves, sources, [sds((2 * w2_rows, d_model), BF16)])

        def w2_at(side, start, n):
            return lambda t: (pl.ds(pl.multiple_of((t[SP] ^ side) * w2_rows + start, BLK), n), ALL)

        (w2,) = ordered_w2([w_down], [send("s", w_down)])
        w2_near = [send("y", w_down[:BLK]), send("y", w_down[BLK:])]
        w2_next = ordered_w2(w2_near, [send("s", w2_near[0]), send("s", w2_near[1])])[0]

        inv_freq = ROPE_BASE ** (-(jnp.arange(HALF_HEAD, dtype=F32) * (1.0 / HALF_HEAD)))
        angles = pos.astype(F32)[:, None] * inv_freq
        cos_t = jnp.tile(jnp.cos(angles), (1, 4))
        sin_t = jnp.tile(jnp.sin(angles), (1, 4))
        u_rel, u_far = norm_kernel(ids, after(act, cos_t, sin_t), gain1_rel)
        u_near = send("x", u_far)
        qkv_pieces = both_cores(gather_weight(w_qkv))

        def quarter_at(r):
            return lambda t: (ALL, part(t[DP] ^ r, quarter))

        tile_shape = (BLK, quarter)
        moves = [(i, quarter_at(r), r, row_at(i, BLK), tile_shape) for r in (2, 0, 3, 1) for i in range(2)]
        q0, q1, q2, q3 = move_kernel(ids, moves, [w_gate, w_up], [sds((2 * BLK, quarter), BF16)] * CHIPS)
        from_y, from_y_next = send("y", q2), send("y", q0)
        from_x_next, from_x = send("x", q3), send("x", q1)
        from_d, from_d_next = send("y", from_x_next), send("y", from_x)

        def ffn_weights(pieces):
            moves = [(i, row_at(o, BLK), o, row_at(i, BLK), tile_shape) for i in range(PLACES) for o in range(2)]
            return move_kernel(ids, moves, pieces, [sds((d_model, quarter), BF16)] * 2)

        w1, w3 = ffn_weights(both_cores([q0, from_x, from_y, from_d]))
        w1_next, w3_next = ffn_weights(both_cores([q2, from_x_next, from_y_next, from_d_next]))

        qkv_far, qkv_keep, wqkv_full = qkv_kernel(ids, u_rel, qkv_pieces, cos_t, sin_t)
        qkv_got = send("s", qkv_far)
        o_keep, o_far = attn_fwd_kernel(ids, qkv_keep, qkv_got)
        o_got = send("s", o_far)
        attn_rel, hidden, normed, wo_full, attn_far = out_proj_kernel(ids, o_keep, o_got, wo_pieces, act, gain2_rel)

        attn_near = send("y", attn_far)

        w_rows = list(enumerate(gather_rows(normed)))
        dy_rows = gather_rows(dy)
        fwd = ffn_fwd_kernel(ids, 0, w_rows[:1], w1, w3, (), HALF_TOKENS)
        bwd = ffn_bwd_kernel(ids, 0, dy_rows[:1], fwd[2], fwd[3], w2, (), HALF_TOKENS)
        fwd = ffn_fwd_kernel(ids, 1, w_rows[1:2], w1, w3, fwd, HALF_TOKENS)
        mixed_next, act_next, slope_next = ffn_fwd_kernel(ids, 0, None, w1_next, w3_next, fwd[:1], TOKENS)
        bwd = ffn_bwd_kernel(ids, 1, dy_rows[1:2], fwd[2], fwd[3], w2, bwd, HALF_TOKENS)
        dw = ffn_dw_kernel(ids, bwd[1], bwd[2], w1, w3, ())
        dgate_next, dup_next = ffn_bwd_kernel(ids, 0, None, act_next, slope_next, w2_next, bwd[:1], TOKENS)
        dw_own, dw_far = ffn_dw_kernel(ids, dgate_next, dup_next, w1_next, w3_next, dw)
        y = ffn_y_kernel(ids, fwd[1], w2, ())
        y_own, y_far = ffn_y_kernel(ids, mixed_next, w2_next, y)
        w_all, mixed, act_c, slope_c = ffn_fwd_kernel(ids, 1, w_rows[2:], w1, w3, fwd, TOKENS)
        dy_all, dgate, dup = ffn_bwd_kernel(ids, 1, dy_rows[2:], act_c, slope_c, w2, bwd, TOKENS)
        dw_got = send("x", dw_far)
        y_got = send("x", y_far)

        def both_grads(near, far, n_blocks, parts):
            (sent,) = weight_grad_kernel(ids, far, n_blocks, None, 0)
            return weight_grad_kernel(ids, near, n_blocks, send("s", sent), parts)

        def column_grad(grad_all):
            own, *rest = both_grads([(w_all, later(0), grad_all)], [(w_all, later(CHIPS), grad_all)], CHIPS, 1)
            return [own] + [send(way, v) for way, v in zip("xyd", rest)]

        def placed(pieces):
            return move_kernel(ids, [(r, everything, 0, quarter_at(r), tile_shape) for r in range(CHIPS)], pieces, [sds((BLK, f_cols), F32)])

        gate_pieces = column_grad(dgate)
        up_pieces = column_grad(dup)
        (down_grad,) = both_grads([(mixed, lambda j, t: t[SP] * CHIPS + j, dy_all)], [(mixed, lambda j, t: (1 - t[SP]) * CHIPS + j, dy_all)], CHIPS, 0)
        (gate_grad,) = placed(gate_pieces)
        (up_grad,) = placed(up_pieces)

        grad_hidden, gain2_part = hidden_grad_kernel(ids, dw_own, dw_got, hidden, gain2_rel, dy)

        def row_grad(k, way, left, left_near, right, right_near):
            blocks = here_blocks(k)
            first, second, *_ = blocks
            stride = second - first
            half = len(blocks) // 2
            near = [(left, later(0, stride), right), (left_near, later(0), right_near)]
            far = [(left, later(CHIPS, stride), right), (left_near, later(half), right_near)]
            own, sent = both_grads(near, far, half, 1)
            return own, send(way, sent)

        do_far, do_keep = attn_grad_kernel(ids, grad_hidden, wo_full)
        do_got = send("s", do_far)
        d_keep, d_far = attn_bwd_kernel(ids, qkv_keep, qkv_got, do_keep, do_got)
        d_got = send("s", d_far)
        hidden_near = send("y", grad_hidden)
        wo_terms = row_grad(2, "x", attn_rel, attn_near, grad_hidden, hidden_near)
        grad_qkv = unrope_kernel(ids, d_keep, d_got, cos_t, sin_t)
        qkv_near = send("x", grad_qkv)
        qkv_terms = row_grad(1, "y", u_rel, u_near, grad_qkv, qkv_near)
        q_grad, k_grad, v_grad = sum_kernel(ids, qkv_terms, (q_cols, kv_cols, kv_cols))
        query_grad = q_grad.reshape(w_query.shape)
        key_grad = k_grad.reshape(w_key.shape)
        value_grad = v_grad.reshape(w_value.shape)
        (act_out,) = sum_kernel(ids, (hidden, y_own, y_got), (d_model,), BF16)
        wo_own, wo_got = wo_terms
        wo_own = after(wo_own, query_grad, key_grad, value_grad)
        (wout_grad,) = sum_kernel(ids, (wo_own, wo_got), (d_model,))
        in_grad, gain1_part = input_grad_kernel(ids, grad_qkv, wqkv_full, act, gain1_rel, grad_hidden)

        gain_part = jnp.concatenate([gain1_part, gain2_part], axis=0)
        gain_half = gain_part[:, :half_d] + send("s", gain_part[:, half_d:])
        own, to_x, to_y, to_d = [gain_half[:, cols_of(r)] for r in range(CHIPS)]
        gain1_grad, gain2_grad = own + send("x", to_x) + send("y", to_y) + send("d", to_d)
        return (act_out[None], in_grad[None], gain1_grad, gain2_grad, query_grad, key_grad, value_grad, wout_grad, gate_grad, up_grad, down_grad)

    return jax.shard_map(layer, mesh=mesh, in_specs=(row_spec, pos_spec, row_spec, vec_spec, vec_spec, cube_spec, cube_spec, cube_spec, mat_spec, mat_spec, mat_spec, mat_spec), out_specs=(row_spec, row_spec, vec_spec, vec_spec, cube_spec, cube_spec, cube_spec, mat_spec, mat_spec, mat_spec, mat_spec), check_vma=False)
```

```python
import jax
import jax.numpy as jnp
from jax import lax
from jax.experimental import pallas as pl
from jax.experimental.pallas import tpu as pltpu
from jax.sharding import PartitionSpec as P

INTERPRET = False

EPS = 1e-5
ROPE_BASE = 10000.0
NEG_BIG = -1e30
F32 = jnp.float32
BF16 = jnp.bfloat16
CHIPS = 4
PLACES = 8
BLK = 256
HALF_BLK = BLK // 2
TOKENS = 512
HEAD = 64
HALF_HEAD = HEAD // 2
PAIR = 2 * HEAD
ATTN_SCALE = HEAD ** -0.5
GROUPS = 4
GROUP_HEADS = 4
Q_PAIRS = 8
KV_PAIRS = 2
K_SLAB = Q_PAIRS
V_SLAB = K_SLAB + KV_PAIRS
SLABS = V_SLAB + KV_PAIRS
ALL = slice(None)
MANY = pltpu.SemaphoreType.DMA


def dot(a, b):
    return lax.dot_general(a, b, (((1,), (0,)), ((), ())), preferred_element_type=F32)


def dot_nt(a, b):
    return lax.dot_general(a, b, (((1,), (1,)), ((), ())), preferred_element_type=F32)


def dot_tn(a, b):
    return lax.dot_general(a, b, (((0,), (0,)), ((), ())), preferred_element_type=F32)


def after(value, *deps):
    first, *_ = lax.optimization_barrier((value,) + deps)
    return first


def sds(shape, dtype):
    return jax.ShapeDtypeStruct(shape, dtype)


def like(v):
    return sds(v.shape, v.dtype)


def fixed(j, t):
    return 0


def moving(j, t):
    return j


def until(n):
    return lambda j, t: jnp.minimum(j, n - 1)


def since(n):
    return lambda j, t: jnp.maximum(j - n, 0)


def always(n):
    return lambda j, t: n


def spec(shape, *index):
    return pl.BlockSpec(shape, lambda j, t: tuple(f(j, t) for f in index))


def whole(v):
    return spec(v.shape, *[fixed] * len(v.shape))


def anywhere(n):
    return [pl.BlockSpec(memory_space=pl.ANY)] * n


def call(body, ids, args, grid, in_specs, out_specs, out_shape, scratch=(), gflop=1.0, aliases=None):
    return pl.pallas_call(
        body,
        out_shape=out_shape,
        grid_spec=pltpu.PrefetchScalarGridSpec(num_scalar_prefetch=1, grid=(grid,), in_specs=in_specs, out_specs=out_specs, scratch_shapes=list(scratch)),
        cost_estimate=pl.CostEstimate(flops=int(gflop * 1e9), bytes_accessed=int(1e7), transcendentals=0),
        compiler_params=pltpu.CompilerParams(dimension_semantics=("arbitrary",)),
        input_output_aliases=aliases or {},
        interpret=INTERPRET,
    )(ids, *args)


def step_id():
    return pl.program_id(0)


def loop(count, body):
    def one(i, carry):
        body(i)
        return carry

    lax.fori_loop(0, count, one, 0)


SP = 2 * PLACES
DP = SP + 1


def part(index, size):
    return pl.ds(pl.multiple_of(index * size, size), size)


def cols_of(p):
    return slice(p * BLK, (p + 1) * BLK)


def row_sum(v):
    return jnp.sum(v, axis=-1, keepdims=True)


def row_scale(x):
    return lax.rsqrt(row_sum(x * x) * (1.0 / x.shape[-1]) + EPS)


def write_normed(t, src, rows, gain, out, out_rows):
    scale = row_scale(src[rows, :].astype(F32))
    for p in range(PLACES):
        blk = src[rows, part(t[p], BLK)].astype(F32)
        out[out_rows, cols_of(p)] = (blk * scale * gain[:, cols_of(p)]).astype(BF16)


def to_neighbour(k):
    return [p for p in range(PLACES) if p & k]


def here_blocks(k):
    return [p for p in range(PLACES) if not p & k]


def copy_blocks(dst, src, places):
    for i, p in enumerate(places):
        dst[:, cols_of(i)] = src[:, cols_of(p)]


def norm_kernel(ids, act, gain_rel):
    rows, cols = act.shape
    tile = HALF_BLK

    def body(t, x_ref, g_ref, o_ref, send_ref):
        write_normed(t, x_ref, ALL, g_ref, o_ref, ALL)
        copy_blocks(send_ref, o_ref, to_neighbour(1))

    io = spec((tile, cols), moving, fixed)
    return call(body, ids, (act, gain_rel), rows // tile, [io, whole(gain_rel)],
                [io, spec((tile, cols // 2), moving, fixed)], [like(act), sds((rows, cols // 2), BF16)])


def rope_lanes(values, cos_t, sin_t, sign):
    width = values.shape[-1]
    reps = width // PAIR
    if reps > 1:
        cos_t = jnp.concatenate([cos_t] * reps, axis=1)
        sin_t = jnp.concatenate([sin_t] * reps, axis=1)
    lane = lax.broadcasted_iota(jnp.int32, values.shape, 1)
    up_roll = pltpu.roll(values, width - HALF_HEAD, 1)
    down_roll = pltpu.roll(values, HALF_HEAD, 1)
    other = jnp.where((lane & (HEAD - 1)) < HALF_HEAD, -up_roll, down_roll)
    return values * cos_t + (other * sin_t if sign > 0 else -(other * sin_t))


def fill(scratch, refs):
    start = 0
    for ref in refs:
        n, _ = ref.shape
        scratch[start:start + n, :] = ref[:]
        start += n


def qkv_kernel(ids, u_rel, pieces, cos_t, sin_t):
    rows, d_model = u_rel.shape
    cols = pieces[0].shape[1]
    n_pieces = len(pieces)
    tiles = SLABS // 2
    q_tiles = Q_PAIRS // 2

    def column(j, t):
        far = (j < tiles).astype(jnp.int32)
        half = t[SP] ^ far
        tile = j - tiles * (1 - far)
        return jnp.where(tile < q_tiles, half * q_tiles + tile, 2 * tile + half)

    def body(t, u_ref, cos_ref, sin_ref, *refs):
        far_ref, keep_ref, w_ref = refs[n_pieces:]
        j = step_id()
        fill(w_ref, refs[:n_pieces])
        acc = dot(u_ref[:], w_ref[:])
        roped = rope_lanes(acc, cos_ref[:], sin_ref[:], 1)
        is_value = (j == tiles - 1) | (j == 2 * tiles - 1)
        out = jnp.where(is_value, acc, roped).astype(BF16)
        for cond, ref in ((j < tiles, far_ref), (j >= tiles, keep_ref)):
            @pl.when(cond)
            def _():
                for e in range(2):
                    ref[e] = out[:, e * PAIR:(e + 1) * PAIR]

    w_specs = [spec((p.shape[0], BLK), fixed, column) for p in pieces]
    slab = (2, rows, PAIR)
    return call(body, ids, (u_rel, cos_t, sin_t) + tuple(pieces), 2 * tiles,
                [whole(u_rel), whole(cos_t), whole(sin_t)] + w_specs,
                [spec(slab, until(tiles), fixed, fixed), spec(slab, since(tiles), fixed, fixed), spec((d_model, BLK), fixed, column)],
                [sds((SLABS, rows, PAIR), BF16)] * 2 + [sds((d_model, cols), BF16)], gflop=6.5)


def core_rows(t, rows):
    return part(t[SP], rows), part(1 - t[SP], rows)


def in_order(t, ref, own, other):
    for here, v in zip(core_rows(t, own.shape[0]), (own, other)):
        ref[here, :] = v


def one_head(pair, odd):
    return jnp.where(odd == 1, pair[:, HEAD:], pair[:, :HEAD])


def softmax_rows(q_tile, keys, first_row, span):
    scores = dot_nt(q_tile, keys) * ATTN_SCALE
    edge = span - BLK
    shape = (q_tile.shape[0], BLK)
    row = lax.broadcasted_iota(jnp.int32, shape, 0) + first_row
    col = lax.broadcasted_iota(jnp.int32, shape, 1)
    last = jnp.where(row >= col, scores[:, edge:], NEG_BIG)
    scores = jnp.concatenate([scores[:, :edge], last], axis=1) if edge else last
    expo = jnp.exp(scores - jnp.max(scores, axis=-1, keepdims=True))
    return expo * (1.0 / row_sum(expo))


def head_specs(rows):
    slabs = (2, rows, PAIR)
    one = (1, rows, PAIR)
    q_spec = spec(slabs, moving, fixed, fixed)
    return q_spec, [q_spec] + [spec(one, lambda j, t, base=base: base + j // 2, fixed, fixed) for base in (K_SLAB, V_SLAB)]


def attn_fwd_kernel(ids, keep, got):
    _, rows, _ = keep.shape
    seq = 2 * rows

    def body(t, qk_ref, kk_ref, vk_ref, qg_ref, kg_ref, vg_ref, keep_ref, send_ref, ks, vs, qs, os):
        odd = step_id() & 1
        in_order(t, ks, one_head(kk_ref[0], odd), one_head(kg_ref[0], odd))
        in_order(t, vs, one_head(vk_ref[0], odd), one_head(vg_ref[0], odd))

        def head(h):
            in_order(t, qs, one_head(qk_ref[h // 2], h & 1), one_head(qg_ref[h // 2], h & 1))
            for span in range(BLK, seq + BLK, BLK):
                prob = softmax_rows(qs[span - BLK:span, :], ks[:span, :], 0, span).astype(BF16)
                os[h, span - BLK:span, :] = dot(prob, vs[:span, :]).astype(BF16)

        loop(GROUP_HEADS, head)
        for here, ref in zip(core_rows(t, rows), (keep_ref, send_ref)):
            for p in range(2):
                ref[p] = jnp.concatenate([os[2 * p, here, :], os[2 * p + 1, here, :]], axis=1)

    q_spec, specs = head_specs(rows)
    return call(body, ids, (keep,) * 3 + (got,) * 3, GROUPS, specs * 2,
                [q_spec] * 2, [sds((Q_PAIRS, rows, PAIR), BF16)] * 2,
                [pltpu.VMEM((seq, HEAD), BF16)] * 3 + [pltpu.VMEM((GROUP_HEADS, seq, HEAD), BF16)], gflop=20)


def attn_bwd_kernel(ids, keep, got, do_keep, do_got):
    _, rows, _ = keep.shape
    seq = 2 * rows
    strip_rows = BLK

    def body(t, qk_ref, kk_ref, vk_ref, dk_ref, qg_ref, kg_ref, vg_ref, dg_ref, keep_ref, send_ref, ks, vs, qs, ds, dqs, dks, dvs):
        g = step_id()
        odd = g & 1
        in_order(t, ks, one_head(kk_ref[0], odd), one_head(kg_ref[0], odd))
        in_order(t, vs, one_head(vk_ref[0], odd), one_head(vg_ref[0], odd))
        dks[odd] = jnp.zeros_like(ks, F32)
        dvs[odd] = jnp.zeros_like(vs, F32)

        def head(h):
            in_order(t, qs, one_head(qk_ref[h // 2], h & 1), one_head(qg_ref[h // 2], h & 1))
            in_order(t, ds, one_head(dk_ref[h // 2], h & 1), one_head(dg_ref[h // 2], h & 1))
            for span in range(BLK, seq + BLK, BLK):
                def strip(n):
                    here = part((span - BLK) // strip_rows + n, strip_rows)
                    q_tile = qs[here, :]
                    do_tile = ds[here, :]
                    prob = softmax_rows(q_tile, ks[:span, :], n * strip_rows, span)
                    grad_prob = dot_nt(do_tile, vs[:span, :])
                    inner = row_sum(prob * grad_prob)
                    grad_scores = (prob * (grad_prob - inner) * ATTN_SCALE).astype(BF16)
                    dqs[h, here, :] = dot(grad_scores, ks[:span, :]).astype(BF16)
                    dks[odd, :span, :] += dot_tn(grad_scores, q_tile)
                    dvs[odd, :span, :] += dot_tn(prob.astype(BF16), do_tile)

                loop(BLK // strip_rows, strip)

        loop(GROUP_HEADS, head)
        for here, ref in zip(core_rows(t, rows), (keep_ref, send_ref)):
            for p in range(2):
                ref[2 * g + p] = jnp.concatenate([dqs[2 * p, here, :], dqs[2 * p + 1, here, :]], axis=1)

            @pl.when(odd == 1)
            def _():
                for base, acc in ((K_SLAB, dks), (V_SLAB, dvs)):
                    ref[base + g // 2] = jnp.concatenate([acc[0, here, :], acc[1, here, :]], axis=1).astype(BF16)

    q_spec, specs = head_specs(rows)
    return call(body, ids, (keep,) * 3 + (do_keep,) + (got,) * 3 + (do_got,), GROUPS, (specs + [q_spec]) * 2,
                [whole(keep)] * 2, [like(keep)] * 2,
                [pltpu.VMEM((seq, HEAD), BF16)] * 4 + [pltpu.VMEM((GROUP_HEADS, seq, HEAD), BF16)] + [pltpu.VMEM((2, seq, HEAD), F32)] * 2, gflop=50)


def out_proj_kernel(ids, o_keep, o_got, pieces, act, gain_rel):
    rows, d_model = act.shape
    tile = BLK
    strip_rows = HALF_HEAD
    n_pieces = len(pieces)

    def body(t, ok_ref, og_ref, x_ref, g_ref, *refs):
        a_ref, h_ref, normed_ref, w_ref, send_ref, a_abs = refs[n_pieces:]
        j = step_id()

        @pl.when(j == 0)
        def _():
            for ref, side in ((ok_ref, t[SP]), (og_ref, 1 - t[SP])):
                for p in range(Q_PAIRS):
                    a_abs[:, part(side * Q_PAIRS + p, PAIR)] = ref[p]
            for p in range(PLACES):
                a_ref[:, cols_of(p)] = a_abs[:, part(t[p], BLK)]
            copy_blocks(send_ref, a_ref, to_neighbour(2))

        fill(w_ref, refs[:n_pieces])
        acc = dot(a_ref[:], w_ref[:])
        cols = part(j, tile)
        h_ref[:, cols] = (x_ref[:, cols].astype(F32) + acc).astype(BF16)

        @pl.when(j == d_model // tile - 1)
        def _():
            def normed(i):
                here = part(i, strip_rows)
                write_normed(t, h_ref, here, g_ref, normed_ref, here)

            loop(rows // strip_rows, normed)

    w_specs = [spec((p.shape[0], tile), fixed, moving) for p in pieces]
    send = sds((rows, d_model // 2), BF16)
    return call(body, ids, (o_keep, o_got, act, gain_rel) + tuple(pieces), d_model // tile,
                [whole(o_keep), whole(o_got), whole(act), whole(gain_rel)] + w_specs,
                [whole(act)] * 3 + [spec((d_model, tile), fixed, moving), whole(send)],
                [like(act)] * 3 + [sds((d_model, d_model), BF16), send], [pltpu.VMEM((rows, d_model), BF16)], gflop=4.3)


def swapped(place, k):
    return place ^ k


def pair_spec(cols):
    return spec((2 * TOKENS, cols), fixed, fixed)


def ffn_fwd_kernel(ids, place, parts, weights, buffers):
    tile = BLK
    owners = [k for k, _ in parts] if parts else []
    arrays = [v for _, v in parts] if parts else list(buffers)
    rows = 2 * TOKENS
    total = CHIPS * TOKENS if parts else rows
    aliased = list(buffers) if parts else []
    n_in = len(arrays)
    pieces = len(weights) > 2
    f_cols = weights[0].shape[-1]
    d_model = PLACES * BLK
    n_w = 2 * len(weights) if pieces else 2

    def body(t, *refs):
        w_refs = refs[n_in:n_in + n_w]
        *own, m_ref, act_ref, slope_ref = refs[n_in + n_w + len(aliased):]
        if pieces:
            *own, w1_ref, w3_ref = own
            fill(w1_ref, w_refs[::2])
            fill(w3_ref, w_refs[1::2])
        else:
            w1_ref, w3_ref = w_refs
        wall_ref, *flipped = own if parts else refs[:1]

        if parts:
            @pl.when(step_id() == 0)
            def _():
                start = 0
                for k, ref in zip(owners, refs):
                    n, _ = ref.shape
                    for p in range(PLACES):
                        wall_ref[start:start + n, cols_of(p)] = ref[:, cols_of(swapped(p, k))]
                    start += n

        j = step_id()

        def strip(n):
            here = part(n, TOKENS)
            gate = dot(wall_ref[here, :], w1_ref[:])
            up = dot(wall_ref[here, :], w3_ref[:])
            for ref in flipped:
                ref[:, here] = wall_ref[here, part(j, tile)].T
            sig = jax.nn.sigmoid(gate)
            act = gate * sig
            act_ref[here, :] = act
            slope_ref[here, :] = up * sig * (1.0 + gate * (1.0 - sig))
            m_ref[here, :] = (act * up).astype(BF16)

        loop(rows // TOKENS, strip)

    w_spec = spec((d_model, tile), fixed, moving)
    tile_spec = spec((rows, tile), always(place), moving)
    out_specs = [tile_spec] * 3
    out_shape = [sds((total, f_cols), BF16)] + [sds((total, f_cols), F32)] * 2
    if pieces:
        out_specs = [w_spec] * 2 + out_specs
        out_shape = [sds((d_model, f_cols), BF16)] * 2 + out_shape
    if parts:
        out_specs = [spec((rows, d_model), always(place), fixed), spec((tile, rows), moving, always(place))] + out_specs
        out_shape = [sds((total, d_model), BF16), sds((d_model, total), BF16)] + out_shape
    in_specs = [whole(v) for v in arrays] if parts else [pair_spec(d_model)]
    if pieces:
        in_specs += [spec((BLK, tile), always(i), moving) for _ in weights for i in range(2)]
        w_args = tuple(v for v in weights for _ in range(2))
    else:
        in_specs += [w_spec] * 2
        w_args = tuple(weights)
    return call(body, ids, tuple(arrays) + w_args + tuple(aliased), f_cols // tile, in_specs + anywhere(len(aliased)), out_specs, out_shape,
                gflop=8.6, aliases={n_in + n_w + 1 + i: i for i in range(len(aliased))})


def ffn_bwd_kernel(ids, place, parts, act, slope, w2, buffers):
    f_cols, d_model = w2.shape
    tile = BLK
    arrays = list(parts) if parts else list(buffers)
    rows = sum(v.shape[0] for v in arrays) if parts else 2 * TOKENS
    total = CHIPS * TOKENS if parts else rows
    aliased = list(buffers) if parts else []
    n_in = len(arrays)

    def body(t, *refs):
        act_ref, slope_ref, w2_ref = refs[n_in:n_in + 3]
        *own, dg_ref, du_ref = refs[n_in + 3 + len(aliased):]
        (dyall_ref,) = own if parts else refs[:1]

        if parts:
            @pl.when(step_id() == 0)
            def _():
                fill(dyall_ref, refs[:n_in])

        def strip(n):
            here = part(n, TOKENS)
            back = dot_nt(dyall_ref[here, :], w2_ref[:]).astype(BF16).astype(F32)
            du_ref[here, :] = (back * act_ref[here, :]).astype(BF16)
            dg_ref[here, :] = (back * slope_ref[here, :]).astype(BF16)

        loop(rows // TOKENS, strip)

    tile_spec = spec((rows, tile), always(place), moving)
    out_specs = [tile_spec] * 2
    out_shape = [sds((total, f_cols), BF16)] * 2
    if parts:
        out_specs = [spec((rows, d_model), always(place), fixed)] + out_specs
        out_shape = [sds((total, d_model), BF16)] + out_shape
    in_specs = ([whole(v) for v in arrays] if parts else [pair_spec(d_model)]) + [tile_spec] * 2 + [spec((tile, d_model), moving, fixed)] + anywhere(len(aliased))
    return call(body, ids, tuple(arrays) + (act, slope, w2) + tuple(aliased), f_cols // tile, in_specs, out_specs, out_shape,
                gflop=8.6, aliases={n_in + 4 + i: i for i in range(len(aliased))})


def write_chips(outs, value, accs):
    for i, out in enumerate(outs):
        rows = value[i * TOKENS:(i + 1) * TOKENS]
        out[:] = rows + accs[i][:] if accs else rows


def ffn_dw_kernel(ids, dgate, dup, w1, w3, accs):
    d_model, f_cols = w1.shape

    def body(t, dg_ref, du_ref, w1_ref, w3_ref, *refs):
        write_chips(refs[len(accs):], dot_nt(dg_ref[:], w1_ref[:]) + dot_nt(du_ref[:], w3_ref[:]), refs[:len(accs)])

    w_spec = spec((BLK, f_cols), moving, fixed)
    out_specs = [spec((TOKENS, BLK), fixed, lambda j, t, k=k: j ^ k) for k in range(2)]
    return call(body, ids, (dgate, dup, w1, w3) + tuple(accs), d_model // BLK, [pair_spec(f_cols)] * 2 + [w_spec] * 2 + out_specs[:len(accs)],
                out_specs, [sds((TOKENS, d_model), F32)] * 2, gflop=17)


def ffn_y_kernel(ids, mixed, w2, accs):
    f_cols, d_model = w2.shape

    def body(t, m_ref, w2_ref, *refs):
        write_chips(refs[len(accs):], dot(m_ref[:], w2_ref[:]), refs[:len(accs)])

    out_specs = [spec((TOKENS, BLK), fixed, moving)] * 2
    return call(body, ids, (mixed, w2) + tuple(accs), d_model // BLK, [pair_spec(f_cols), spec((f_cols, BLK), fixed, moving)] + out_specs[:len(accs)],
                out_specs, [sds((TOKENS, d_model), F32)] * 2, gflop=8.6)


def flip_rows(dst, start, src, n, rows):
    def piece(i):
        here = part(i, BLK)
        dst[start:start + n, here] = src[here, :].T

    loop(rows // BLK, piece)


def weight_grad_kernel(ids, pairs, n_blocks, received, parts):
    _, cols = pairs[0][-1].shape
    out_rows = n_blocks * BLK
    strip_rows = TOKENS
    tile = BLK if n_blocks == CHIPS else TOKENS
    n_out = n_blocks if parts else 1

    def body(t, *refs):
        *refs, total = refs
        ins, outs = list(refs[:len(args)]), refs[len(args):len(args) + n_out]
        flips = list(refs[len(args) + n_out:])
        operands = []
        for (lefts, _, ready, _) in pairs:
            mine = [ins.pop(0) for _ in lefts]
            right_ref = ins.pop(0)
            if ready:
                (left_ref,) = mine
            else:
                left_ref = flips.pop(0)

                @pl.when(step_id() == 0)
                def _():
                    start = 0
                    for ref in mine:
                        rows, n = ref.shape
                        flip_rows(left_ref, start, ref, n, rows)
                        start += n
            operands.append((left_ref, right_ref))

        def strip(n):
            here = part(n, strip_rows)
            first, *rest = [dot(left_ref[here, :], right_ref[:]) for left_ref, right_ref in operands]
            total[here, :] = sum(rest, first)

        loop(out_rows // strip_rows, strip)
        size = out_rows // n_out
        for i, out in enumerate(outs):
            here = slice(i * size, (i + 1) * size)
            out[:] = total[here, :] + ins[0][here, :] if ins else total[here, :]

    in_specs, args, scratch = [], (), []
    for lefts, blocks, ready, right in pairs:
        rows, _ = right.shape
        for left, block in zip(lefts, blocks):
            if ready:
                in_specs.append(spec((out_rows, rows), block, fixed))
            else:
                in_specs.append(spec((rows, out_rows // len(lefts)), fixed, block))
            args += (left,)
        in_specs.append(spec((rows, tile), fixed, moving))
        args += (right,)
        if not ready:
            scratch.append(pltpu.VMEM((out_rows, rows), BF16))
    if received is not None:
        in_specs.append(spec((out_rows, tile), fixed, moving))
        args += (received,)
    size = out_rows // n_out
    return call(body, ids, args, cols // tile, in_specs, [spec((size, tile), fixed, moving)] * n_out, [sds((size, cols), F32)] * n_out,
                scratch + [pltpu.VMEM((out_rows, tile), F32)], gflop=8.6)


def sum_kernel(ids, terms, widths, dtype=F32):
    n = len(terms)
    rows, cols = terms[0].shape
    tile = rows // CHIPS

    def body(t, *refs):
        start = 0
        for width, out in zip(widths, refs[n:]):
            cut = slice(start, start + width)
            first, *rest = [ref[:, cut].astype(F32) for ref in refs[:n]]
            out[:] = sum(rest, first).astype(dtype)
            start += width

    return call(body, ids, tuple(terms), CHIPS, [spec((tile, cols), moving, fixed)] * n,
                [spec((tile, w), moving, fixed) for w in widths], [sds((rows, w), dtype) for w in widths])


def move_kernel(ids, moves, sources, out_shapes):
    n_src, n_out, n = len(sources), len(out_shapes), len(moves)

    def body(t, *refs):
        srcs, outs = refs[:n_src], refs[n_src:n_src + n_out]
        *bufs, in_sem, out_sem = refs[n_src + n_out:]
        loads, stores = [], []
        for i, (src, src_at, out, out_at, _) in enumerate(moves):
            loads.append(pltpu.make_async_copy(srcs[src].at[src_at(t)], bufs[i], in_sem.at[i]))
            stores.append(pltpu.make_async_copy(bufs[i], outs[out].at[out_at(t)], out_sem.at[i]))
        for load in loads:
            load.start()
        for load, store in zip(loads, stores):
            load.wait()
            store.start()
        for store in stores:
            store.wait()

    shapes = [pltpu.VMEM(shape, sources[src].dtype) for src, _, _, _, shape in moves]
    return call(body, ids, tuple(sources), 1, anywhere(n_src), anywhere(n_out), list(out_shapes), shapes + [MANY((n,))] * 2)


def everything(t):
    return ALL, ALL


def row_at(index, size):
    return lambda t: (slice(index * size, (index + 1) * size), ALL)


def norm_back(t, grad_ref, rows, src_ref, gain_ref, base_ref, out_ref, gain_out_ref):
    src = src_ref[rows, :].astype(F32)
    scale = row_scale(src)
    inner = jnp.zeros_like(scale)
    for p in range(PLACES):
        cols = cols_of(p)
        unit = src_ref[rows, part(t[p], BLK)].astype(F32) * scale
        grad = grad_ref[rows, cols].astype(F32)
        gain_out_ref[:, cols] += jnp.sum(grad * unit, axis=0, keepdims=True)
        inner += row_sum(grad * gain_ref[:, cols] * unit)
    inner = inner * (1.0 / src.shape[-1])
    for p in range(PLACES):
        cols = cols_of(p)
        place = part(t[p], BLK)
        unit = src_ref[rows, place].astype(F32) * scale
        grad_rows = scale * (grad_ref[rows, cols].astype(F32) * gain_ref[:, cols] - unit * inner)
        out_ref[rows, place] = (base_ref[rows, place].astype(F32) + grad_rows).astype(BF16)


def hidden_grad_kernel(ids, own, got, hidden, gain_rel, dy):
    rows, d_model = hidden.shape
    tile = HEAD

    def body(t, own_ref, got_ref, h_ref, g_ref, dy_ref, out_ref, gain_ref, grad):
        @pl.when(step_id() == 0)
        def _():
            gain_ref[:] = jnp.zeros_like(gain_ref)

        grad[:] = (own_ref[:] + got_ref[:]).astype(BF16)
        norm_back(t, grad, ALL, h_ref, g_ref, dy_ref, out_ref, gain_ref)

    shape = (tile, d_model)
    row_spec = spec(shape, moving, fixed)
    return call(body, ids, (own, got, hidden, gain_rel, dy), rows // tile, [row_spec] * 3 + [whole(gain_rel), row_spec],
                [row_spec, whole(gain_rel)], [like(hidden), like(gain_rel)], [pltpu.VMEM(shape, BF16)], gflop=5)


def attn_grad_kernel(ids, grad_hidden, w_full):
    rows, d_model = grad_hidden.shape
    half = CHIPS // 2

    def block_row(j, t):
        side = t[SP] ^ (j < half).astype(jnp.int32)
        return (side * half + (j & 1)) ^ t[DP]

    def body(t, g_ref, w_ref, far_ref, keep_ref):
        j = step_id()

        def one_core(s):
            grad = dot_nt(g_ref[:], w_ref[s]).astype(BF16)
            for cond, ref in ((j < half, far_ref), (j >= half, keep_ref)):
                @pl.when(cond)
                def _():
                    for e in range(2):
                        ref[(t[SP] ^ s) * 2 + e] = grad[:, e * PAIR:(e + 1) * PAIR]

        loop(2, one_core)

    slabs = (CHIPS, rows, PAIR)
    return call(body, ids, (grad_hidden, w_full.reshape(2, CHIPS * BLK, d_model)), CHIPS,
                [whole(grad_hidden), spec((2, BLK, d_model), fixed, block_row, fixed)],
                [spec(slabs, until(half), fixed, fixed), spec(slabs, since(half), fixed, fixed)],
                [sds((Q_PAIRS, rows, PAIR), BF16)] * 2, gflop=4.3)


def unrope_kernel(ids, keep, got, cos_t, sin_t):
    _, rows, _ = keep.shape
    tile = HALF_BLK
    cols = 2 * SLABS * PAIR

    def body(t, k_ref, g_ref, cos_ref, sin_ref, o_ref):
        for ref, side in ((k_ref, t[SP]), (g_ref, 1 - t[SP])):
            for first, count, roped in ((0, Q_PAIRS, True), (K_SLAB, KV_PAIRS, True), (V_SLAB, KV_PAIRS, False)):
                def move(p):
                    pair = ref[first + p]
                    if roped:
                        pair = rope_lanes(pair.astype(F32), cos_ref[:], sin_ref[:], -1).astype(BF16)
                    o_ref[:, part(2 * first + side * count + p, PAIR)] = pair

                loop(count, move)

    h_spec = spec((SLABS, tile, PAIR), fixed, moving, fixed)
    t_spec = spec((tile, PAIR), moving, fixed)
    return call(body, ids, (keep, got, cos_t, sin_t), rows // tile, [h_spec, h_spec, t_spec, t_spec],
                spec((tile, cols), moving, fixed), sds((rows, cols), BF16))


def input_grad_kernel(ids, grad_qkv, w_full, act, gain_rel, grad_hidden):
    rows, d_model = act.shape
    _, cols = grad_qkv.shape
    strip_rows = HALF_HEAD

    def body(t, g_ref, w_ref, x_ref, gain_ref, gh_ref, out_ref, gain_out_ref, grad):
        j = step_id()
        grad[:, part(j, BLK)] = dot_nt(g_ref[:], w_ref[:]).astype(BF16)

        @pl.when(j == PLACES - 1)
        def _():
            gain_out_ref[:] = jnp.zeros_like(gain_out_ref)
            loop(rows // strip_rows, lambda i: norm_back(t, grad, part(i, strip_rows), x_ref, gain_ref, gh_ref, out_ref, gain_out_ref))

    return call(body, ids, (grad_qkv, w_full, act, gain_rel, grad_hidden), PLACES,
                [whole(grad_qkv), spec((BLK, cols), moving, fixed), whole(act), whole(gain_rel), whole(grad_hidden)],
                [whole(act), whole(gain_rel)], [like(act), like(gain_rel)], [pltpu.VMEM((rows, d_model), BF16)], gflop=10)


def solution(mesh):
    flat_axes = ("dp", "sp")
    row_spec = P("dp", "sp", None)
    pos_spec = P("dp", "sp")
    vec_spec = P(flat_axes)
    mat_spec = P(flat_axes, None)
    cube_spec = P(flat_axes, None, None)
    hops = {"x": 1, "y": 2, "d": 3}

    def send(way, v):
        if way == "s":
            return lax.ppermute(v, "sp", [(0, 1), (1, 0)])
        return lax.ppermute(v, "dp", [(i, i ^ hops[way]) for i in range(CHIPS)])

    def gather_weight(own, *deps):
        from_x = send("x", own)
        from_y = send("y", own)
        return [own, from_x, from_y, send("x", after(from_y, *deps) if deps else from_y)]

    def both_cores(pieces):
        return pieces + [send("s", p) for p in pieces]

    def gather_rows(own):
        from_x = send("x", own)
        from_y = send("y", own)
        return [own, from_x, from_y, send("y", from_x)]

    def layer(act_in, positions, out_grad, norm1_gain, norm2_gain, w_query, w_key, w_value, w_out, w_gate, w_up, w_down):
        dp = lax.axis_index("dp")
        sp = lax.axis_index("sp")
        _, n_q, hd = w_query.shape
        _, n_kv, _ = w_key.shape
        q_cols, kv_cols = n_q * hd, n_kv * hd
        (act,), (pos,), (dy,) = act_in, positions, out_grad
        _, d_model = act.shape
        half_d = d_model // 2
        _, f_cols = w_gate.shape
        quarter = f_cols // CHIPS
        place = jnp.arange(PLACES, dtype=jnp.int32)
        rel_table = ((place % CHIPS) ^ dp) * 2 + ((place // CHIPS) ^ sp)
        abs_table = ((place % 2) ^ sp) * CHIPS + ((place // 2) ^ dp)
        ids = jnp.concatenate([rel_table, abs_table, jnp.stack([sp, dp])]).astype(jnp.int32)

        wo_pieces = both_cores(gather_weight(w_out, ids))
        w_qkv = jnp.concatenate([w.reshape(BLK, -1) for w in (w_query, w_key, w_value)], axis=1)
        gains = jnp.stack([norm1_gain, norm2_gain])
        gain_mine = jnp.concatenate([gains, send("x", gains), send("y", gains), send("d", gains)], axis=1)
        gain_rel = jnp.concatenate([gain_mine, send("s", gain_mine)], axis=1).astype(F32)
        gain1_rel, gain2_rel = gain_rel[:1], gain_rel[1:]
        w2_rows, _ = w_down.shape

        def ordered_w2(own, other):
            moves, sources = [], []
            for side, pieces in enumerate((own, other)):
                start = 0
                for piece in pieces:
                    n, _ = piece.shape
                    moves.append((len(sources), everything, 0, w2_at(side, start, n), piece.shape))
                    sources.append(piece)
                    start += n
            return move_kernel(ids, moves, sources, [sds((2 * w2_rows, d_model), BF16)])

        def w2_at(side, start, n):
            return lambda t: (pl.ds(pl.multiple_of((t[SP] ^ side) * w2_rows + start, BLK), n), ALL)

        (w2,) = ordered_w2([w_down], [send("s", w_down)])
        w2_near = [send("y", w_down[:BLK]), send("y", w_down[BLK:])]
        w2_next = ordered_w2(w2_near, [send("s", w2_near[0]), send("s", w2_near[1])])[0]

        inv_freq = ROPE_BASE ** (-(jnp.arange(HALF_HEAD, dtype=F32) * (1.0 / HALF_HEAD)))
        angles = pos.astype(F32)[:, None] * inv_freq
        cos_t = jnp.tile(jnp.cos(angles), (1, 4))
        sin_t = jnp.tile(jnp.sin(angles), (1, 4))
        u_rel, u_far = norm_kernel(ids, after(act, cos_t, sin_t), gain1_rel)
        u_near = send("x", u_far)
        qkv_pieces = both_cores(gather_weight(w_qkv))

        def quarter_at(r):
            return lambda t: (ALL, part(t[DP] ^ r, quarter))

        tile_shape = (BLK, quarter)
        moves = [(i, quarter_at(r), r, row_at(i, BLK), tile_shape) for r in (2, 0, 3, 1) for i in range(2)]
        q0, q1, q2, q3 = move_kernel(ids, moves, [w_gate, w_up], [sds((2 * BLK, quarter), BF16)] * CHIPS)
        from_y, from_y_next = send("y", q2), send("y", q0)
        from_x_next, from_x = send("x", q3), send("x", q1)
        from_d, from_d_next = send("y", from_x_next), send("y", from_x)

        w_pieces = both_cores([q0, from_x, from_y, from_d])
        w_next = both_cores([q2, from_x_next, from_y_next, from_d_next])

        qkv_far, qkv_keep, wqkv_full = qkv_kernel(ids, u_rel, qkv_pieces, cos_t, sin_t)
        qkv_got = send("s", qkv_far)
        o_keep, o_far = attn_fwd_kernel(ids, qkv_keep, qkv_got)
        o_got = send("s", o_far)
        attn_rel, hidden, normed, wo_full, attn_far = out_proj_kernel(ids, o_keep, o_got, wo_pieces, act, gain2_rel)

        attn_near = send("y", attn_far)

        w_rows = list(enumerate(gather_rows(normed)))
        dy_rows = gather_rows(dy)
        w_all, w_flip, w1, w3, *fwd = ffn_fwd_kernel(ids, 0, w_rows[:2], w_pieces, ())
        w1_next, w3_next, mixed_next, act_next, slope_next = ffn_fwd_kernel(ids, 0, None, w_next, (w_all,))
        bwd = ffn_bwd_kernel(ids, 0, dy_rows[:2], fwd[1], fwd[2], w2, ())
        dw = ffn_dw_kernel(ids, bwd[1], bwd[2], w1, w3, ())
        dgate_next, dup_next = ffn_bwd_kernel(ids, 0, None, act_next, slope_next, w2_next, bwd[:1])
        dw_own, dw_far = ffn_dw_kernel(ids, dgate_next, dup_next, w1_next, w3_next, dw)
        y = ffn_y_kernel(ids, fwd[0], w2, ())
        y_own, y_far = ffn_y_kernel(ids, mixed_next, w2_next, y)
        w_all, w_flip, mixed, act_c, slope_c = ffn_fwd_kernel(ids, 1, w_rows[2:], (w1, w3), [w_all, w_flip] + fwd)
        dy_all, dgate, dup = ffn_bwd_kernel(ids, 1, dy_rows[2:], act_c, slope_c, w2, bwd)
        dw_got = send("x", dw_far)
        y_got = send("x", y_far)

        def both_grads(near, far, n_blocks, parts):
            (sent,) = weight_grad_kernel(ids, far, n_blocks, None, False)
            return weight_grad_kernel(ids, near, n_blocks, send("s", sent), parts)

        def column_grad(grad_all):
            own, *rest = both_grads(*[[([w_flip], [always(i)], True, grad_all)] for i in range(2)], CHIPS, True)
            return [own] + [send(way, v) for way, v in zip("xyd", rest)]

        def placed(pieces):
            return move_kernel(ids, [(r, everything, 0, quarter_at(r), tile_shape) for r in range(CHIPS)], pieces, [sds((BLK, f_cols), F32)])

        gate_pieces = column_grad(dgate)
        up_pieces = column_grad(dup)
        (down_grad,) = both_grads(*[[([mixed], [lambda j, t, i=i: t[SP] ^ i], False, dy_all)] for i in range(2)], CHIPS, False)
        (gate_grad,) = placed(gate_pieces)
        (up_grad,) = placed(up_pieces)

        grad_hidden, gain2_part = hidden_grad_kernel(ids, dw_own, dw_got, hidden, gain2_rel, dy)

        def row_grad(k, way, left, left_near, right, right_near):
            blocks = here_blocks(k)
            half = len(blocks) // 2

            def operands(side):
                mine = [always(p) for p in blocks[side * half:(side + 1) * half]]
                return [([left] * half, mine, False, right), ([left_near], [always(side)], False, right_near)]

            own, sent = both_grads(operands(0), operands(1), half, True)
            return own, send(way, sent)

        do_far, do_keep = attn_grad_kernel(ids, grad_hidden, wo_full)
        do_got = send("s", do_far)
        d_keep, d_far = attn_bwd_kernel(ids, qkv_keep, qkv_got, do_keep, do_got)
        d_got = send("s", d_far)
        hidden_near = send("y", grad_hidden)
        wo_terms = row_grad(2, "x", attn_rel, attn_near, grad_hidden, hidden_near)
        grad_qkv = unrope_kernel(ids, d_keep, d_got, cos_t, sin_t)
        qkv_near = send("x", grad_qkv)
        qkv_terms = row_grad(1, "y", u_rel, u_near, grad_qkv, qkv_near)
        q_grad, k_grad, v_grad = sum_kernel(ids, qkv_terms, (q_cols, kv_cols, kv_cols))
        query_grad = q_grad.reshape(w_query.shape)
        key_grad = k_grad.reshape(w_key.shape)
        value_grad = v_grad.reshape(w_value.shape)
        (act_out,) = sum_kernel(ids, (hidden, y_own, y_got), (d_model,), BF16)
        wo_own, wo_got = wo_terms
        wo_own = after(wo_own, query_grad, key_grad, value_grad)
        (wout_grad,) = sum_kernel(ids, (wo_own, wo_got), (d_model,))
        in_grad, gain1_part = input_grad_kernel(ids, grad_qkv, wqkv_full, act, gain1_rel, grad_hidden)

        gain_part = jnp.concatenate([gain1_part, gain2_part], axis=0)
        gain_half = gain_part[:, :half_d] + send("s", gain_part[:, half_d:])
        own, to_x, to_y, to_d = [gain_half[:, cols_of(r)] for r in range(CHIPS)]
        gain1_grad, gain2_grad = own + send("x", to_x) + send("y", to_y) + send("d", to_d)
        return (act_out[None], in_grad[None], gain1_grad, gain2_grad, query_grad, key_grad, value_grad, wout_grad, gate_grad, up_grad, down_grad)

    return jax.shard_map(layer, mesh=mesh, in_specs=(row_spec, pos_spec, row_spec, vec_spec, vec_spec, cube_spec, cube_spec, cube_spec, mat_spec, mat_spec, mat_spec, mat_spec), out_specs=(row_spec, row_spec, vec_spec, vec_spec, cube_spec, cube_spec, cube_spec, mat_spec, mat_spec, mat_spec, mat_spec), check_vma=False)
```
